256 devices in a mesh: seq: 128 (over z, x, y), tp: 2 (over core).
Axes of the slice: x: 4, y: 4, z: 8, core: 2. Of those that a mesh axis runs over, the one named last changes fastest.
Arguments:
- img_qkv: bfloat16 [1, 4096, 3, 2048], P(None, 'seq', None, 'tp'), may hold values from -7 to 7
- txt_qkv: bfloat16 [1, 256, 3, 2048], P(None, None, None, 'tp'), may hold values from -7 to 7
- frame_index: int32 [1, 4096], P(None, 'seq'), may hold values from 0 to 32
- row_index: int32 [1, 4096], P(None, 'seq'), may hold values from 0 to 44
- column_index: int32 [1, 4096], P(None, 'seq'), may hold values from 0 to 79
- txt_len: int32 [1], replicated, may hold values from 64 to 256
- residual: bfloat16 [1, 4096, 3072], P(None, ('seq', 'tp')), may hold values from -6 to 6
- w_proj: bfloat16 [2048, 3072], P('tp'), may hold values from -0.125 to 0.125
- proj_bias: float32 [3072], replicated, may hold values from -3 to 3
- gate: float32 [3072], replicated, may hold values from -4 to 4
Outputs:
- img_out: bfloat16 [1, 4096, 3072], P(None, ('seq', 'tp'))
- txt_out: bfloat16 [1, 256, 2048], P(None, None, 'tp')
The draws below stay inside these ranges and needn't reach their ends.
All inputs are finite; a program needn't handle non-finite values.
Results may differ from the reference program's by a relative error of at most 0.0082.
Values may be sent and summed in bfloat16 or wider, within the bound.
No kernel may reach another device: no remote copies, remote signals or barrier semaphores. Data moves between devices by JAX's collectives and lax.ppermute only.
A program may use at most 64 MiB of HBM per device.

```python
import math
import jax
import jax.numpy as jnp
from jax import lax

D = 3072
HD = 128
HEADS = 16
TXT = 256
LAT_T = 33
LAT_H = 45
LAT_W = 80
CLIPS = 1
IMG = 4096
QW = 2048


def draw_img_qkv(key, part):
    width_all = HEADS * HD
    total_rows = CLIPS * IMG
    subkeys = jax.random.split(jax.random.fold_in(key, 11), 4)
    query_part = jnp.clip(1.8 * jax.random.normal(subkeys[0], (total_rows, width_all), jnp.float32), -7.0, 7.0)
    key_part = jnp.clip(1.8 * jax.random.normal(subkeys[1], (total_rows, width_all), jnp.float32), -7.0, 7.0)
    value_part = jnp.clip(jax.random.normal(subkeys[3], (total_rows, width_all), jnp.float32), -6.0, 6.0)
    stacked = jnp.stack([query_part, key_part, value_part], axis=1)
    return stacked.reshape(CLIPS, IMG, 3, width_all).astype(jnp.bfloat16)


def draw_txt_qkv(key, part):
    width_all = HEADS * HD
    subkeys = jax.random.split(jax.random.fold_in(key, 23), 4)
    query_part = jnp.clip(1.8 * jax.random.normal(subkeys[0], (CLIPS, TXT, width_all), jnp.float32), -7.0, 7.0)
    key_part = jnp.clip(1.8 * jax.random.normal(subkeys[1], (CLIPS, TXT, width_all), jnp.float32), -7.0, 7.0)
    value_part = jnp.clip(jax.random.normal(subkeys[3], (CLIPS, TXT, width_all), jnp.float32), -6.0, 6.0)
    return jnp.stack([query_part, key_part, value_part], axis=2).astype(jnp.bfloat16)


def plant(values, own_key, low, high):
    extent = values.shape
    index_at = [jax.random.randint(jax.random.fold_in(own_key, axis), (), 0, extent[axis]) for axis in range(len(extent))]
    values = values.at[tuple(index_at)].set(low)
    longest = extent.index(max(extent))
    index_at[longest] = (index_at[longest] + 1) % extent[longest]
    return values.at[tuple(index_at)].set(high)


def steps_of(key, dims, cuts, least, high):
    def one(dim, parts):
        steps = jax.random.uniform(jax.random.fold_in(jax.random.fold_in(key, 6), dim), (parts,), jnp.float32, least / len(cuts), high / len(cuts))
        return jnp.repeat(jnp.exp(steps), dims[dim] // parts).reshape((-1,) + (1,) * (len(dims) - dim - 1))

    factor_of = one(*cuts[0])
    for cut in cuts[1:]:
        factor_of = factor_of * one(*cut)
    return factor_of


def normal_values(rng, shape, scale, limit, cuts=(), held_as=jnp.bfloat16):
    values = scale * jax.random.normal(rng, shape, jnp.float32)
    if cuts:
        values = values * steps_of(rng, shape, cuts, -0.22, 0.18)
    return jnp.clip(values, -limit, limit).astype(held_as)


def setup_inputs(seed: int = 0) -> dict:
    seeds = jax.random.split(jax.random.key(seed), 11)
    img_qkv = draw_img_qkv(jax.random.fold_in(seeds[10], 71), 0)
    txt_qkv = draw_txt_qkv(jax.random.fold_in(seeds[10], 71), 0)
    frame_index = plant(jax.random.randint(seeds[2], (CLIPS, IMG), 0, LAT_T), jax.random.fold_in(seeds[2], 1), 0, LAT_T - 1).astype(jnp.int32)
    row_index = plant(jax.random.randint(seeds[3], (CLIPS, IMG), 0, LAT_H), jax.random.fold_in(seeds[3], 1), 0, LAT_H - 1).astype(jnp.int32)
    column_index = plant(jax.random.randint(seeds[4], (CLIPS, IMG), 0, LAT_W), jax.random.fold_in(seeds[4], 1), 0, LAT_W - 1).astype(jnp.int32)
    txt_len = jax.random.randint(seeds[5], (CLIPS,), TXT // 4, TXT + 1).astype(jnp.int32)
    residual = normal_values(seeds[6], (CLIPS, IMG, D), 1.0, 6.0, ((1, 256),))
    w_proj = normal_values(seeds[7], (QW, D), QW ** -0.5, 0.125, ((0, 2),))
    proj_bias = normal_values(seeds[8], (D,), 0.5, 3.0, (), jnp.float32)
    gate = normal_values(seeds[9], (D,), 1.0, 4.0, (), jnp.float32)
    return {"img_qkv": img_qkv, "txt_qkv": txt_qkv, "frame_index": frame_index, "row_index": row_index, "column_index": column_index, "txt_len": txt_len, "residual": residual, "w_proj": w_proj, "proj_bias": proj_bias, "gate": gate}


rope_base = 256.0
neg_large = -1e+30

def rope_tables(frame_index, row_index, column_index, head_dim):
    frame_part = head_dim // 8
    second = (head_dim - frame_part) // 2
    pieces = []
    for places, part_width in ((frame_index, frame_part), (row_index, second), (column_index, second)):
        pair_ids = jnp.arange(part_width // 2).astype(jnp.float32)
        pair_rates = rope_base ** (-2.0 * pair_ids / part_width)
        pieces.append(places.astype(jnp.float32)[:, None] * pair_rates[None, :])
    angles = jnp.repeat(jnp.concatenate(pieces, axis=1), 2, axis=1)
    parity = jnp.arange(head_dim) % 2
    signed = jnp.where(parity == 0, -1.0, 1.0).astype(jnp.float32)
    return (jnp.cos(angles), jnp.sin(angles) * signed[None, :])

def rotate(block_in, cosine, sine_table):
    values = block_in.astype(jnp.float32)
    parity = jnp.arange(values.shape[-1]) % 2
    partner = jnp.where(parity == 0, jnp.roll(values, -1, axis=-1), jnp.roll(values, 1, axis=-1))
    return (values * cosine[:, None, :] + partner * sine_table[:, None, :]).astype(jnp.bfloat16)

def attend_head(query_head, key_head, value_head, live_keys):
    row_count = query_head.shape[0]
    row_block = 1
    for candidate in range(1, 1025):
        if row_count % candidate == 0:
            row_block = candidate
    blocks = query_head.reshape(row_count // row_block, row_block, query_head.shape[1])
    score_scale = 1.0 / math.sqrt(query_head.shape[1])

    def one_block(query_block):
        scores = jnp.dot(query_block, key_head.T, preferred_element_type=jnp.float32) * score_scale
        scores = jnp.where(live_keys[None, :], scores, neg_large)
        peak = lax.optimization_barrier(jnp.max(scores, axis=1, keepdims=True))
        weights = jnp.where(live_keys[None, :], jnp.exp(scores - peak), 0.0)
        weight_sum = lax.optimization_barrier(jnp.sum(weights, axis=1, keepdims=True))
        blended = jnp.dot(weights.astype(jnp.bfloat16), value_head, preferred_element_type=jnp.float32)
        return (blended / weight_sum).astype(jnp.bfloat16)
    return lax.map(one_block, blocks).reshape(row_count, query_head.shape[1])

def clip_attention(clip_qkv, clip_txt, frames, rows_at, columns_at, length):
    cosine, sine_table = rope_tables(frames, rows_at, columns_at, HD)
    img_query = rotate(clip_qkv[:, 0].reshape(IMG, HEADS, HD), cosine, sine_table)
    img_key = rotate(clip_qkv[:, 1].reshape(IMG, HEADS, HD), cosine, sine_table)
    img_value = clip_qkv[:, 2].reshape(IMG, HEADS, HD)
    queries = jnp.concatenate([img_query, clip_txt[:, 0].reshape(TXT, HEADS, HD)], axis=0)
    all_keys = jnp.concatenate([img_key, clip_txt[:, 1].reshape(TXT, HEADS, HD)], axis=0)
    all_values = jnp.concatenate([img_value, clip_txt[:, 2].reshape(TXT, HEADS, HD)], axis=0)
    live_keys = jnp.arange(IMG + TXT) < IMG + length

    def head_work(operands):
        return attend_head(operands[0], operands[1], operands[2], live_keys)
    attended = lax.map(head_work, (queries.transpose(1, 0, 2), all_keys.transpose(1, 0, 2), all_values.transpose(1, 0, 2)))
    joined = attended.transpose(1, 0, 2).reshape(IMG + TXT, HEADS * HD)
    img_rows = joined[:IMG]
    txt_rows = joined[IMG:]
    txt_live = jnp.arange(TXT) < length
    txt_rows = jnp.where(txt_live[:, None], txt_rows, jnp.zeros_like(txt_rows))
    return (img_rows, txt_rows)

def reference(img_qkv, txt_qkv, frame_index, row_index, column_index, txt_len, residual, w_proj, proj_bias, gate):
    img_outs = []
    txt_outs = []
    for clip in range(CLIPS):
        img_rows, txt_rows = clip_attention(img_qkv[clip], txt_qkv[clip], frame_index[clip], row_index[clip], column_index[clip], txt_len[clip])
        projected = jnp.dot(img_rows, w_proj, preferred_element_type=jnp.float32)
        mixed = residual[clip].astype(jnp.float32) + gate[None, :] * (projected + proj_bias[None, :])
        img_outs.append(mixed.astype(jnp.bfloat16))
        txt_outs.append(txt_rows)
    return (jnp.stack(img_outs, axis=0), jnp.stack(txt_outs, axis=0))
```

```python
import math

import jax
import jax.numpy as jnp
import numpy as np
from jax import lax
from jax.experimental import pallas as pl
from jax.experimental.pallas import tpu as pltpu
from jax.sharding import Mesh
from jax.sharding import PartitionSpec as P

HD = 128
SEQ = ("zh", "zl", "x", "y")
CUBE = ("zl", "x", "y")
rope_base = 256.0
neg_large = -1e30
LOG2E = 1.4426950408889634
bf16 = jnp.bfloat16
f32 = jnp.float32


def vmem_spec():
    return pl.BlockSpec(memory_space=pltpu.VMEM)


def smem_spec():
    return pl.BlockSpec(memory_space=pltpu.SMEM)


def call(body, out_shape, n_in, smem=(), limit=40 * 1024 * 1024, scratch=(), name=None):
    single = not isinstance(out_shape, (tuple, list))
    outs = out_shape if not single else [out_shape]
    specs = [vmem_spec() for _ in outs]
    return pl.pallas_call(
        body,
        out_shape=out_shape,
        in_specs=[smem_spec() if i in smem else vmem_spec() for i in range(n_in)],
        out_specs=specs[0] if single else specs,
        scratch_shapes=list(scratch),
        compiler_params=pltpu.CompilerParams(vmem_limit_bytes=limit),
        name=name,
    )


def rate_table():
    table = np.zeros((8, HD), np.float32)
    frame_part = HD // 8
    second = (HD - frame_part) // 2
    at = 0
    for p, width in enumerate((frame_part, second, second)):
        ids = np.arange(width // 2, dtype=np.float32)
        rates = np.float32(rope_base) ** (np.float32(-2.0) * ids / np.float32(width))
        table[p, at : at + width] = np.repeat(rates.astype(np.float32), 2)
        at += width
    return table


def prep_body(qkv_ref, frame_ref, row_ref, col_ref, rate_ref, out_ref):
    tokens = qkv_ref.shape[1]
    sub = lax.broadcasted_iota(jnp.int32, (8, tokens), 0)
    pos = jnp.where(
        sub == 0, frame_ref[...], jnp.where(sub == 1, row_ref[...], jnp.where(sub == 2, col_ref[...], 0))
    ).astype(f32)
    angles = lax.dot_general(
        pos, rate_ref[...], (((0,), (0,)), ((), ())), precision=lax.Precision.HIGHEST,
        preferred_element_type=f32,
    )
    lane = lax.broadcasted_iota(jnp.int32, (tokens, HD), 1)
    even = (lane % 2) == 0
    cosine = jnp.cos(angles)
    sine = jnp.sin(angles)
    sine = jnp.where(even, -sine, sine)

    def rotate(v):
        v = v.astype(f32)
        partner = jnp.where(even, pltpu.roll(v, HD - 1, 1), pltpu.roll(v, 1, 1))
        return v * cosine + partner * sine

    for head in range(8):
        cols = slice(head * HD, (head + 1) * HD)
        query = rotate(qkv_ref[0, :, cols]).astype(bf16)
        key = rotate(qkv_ref[1, :, cols])
        value = qkv_ref[2, :, cols].astype(f32)
        for j in range(4):
            d = head * 4 + j
            out_ref[d, 0:32, :] = query
            pair = jnp.concatenate([key[8 * j : 8 * j + 8], value[8 * j : 8 * j + 8]], axis=0)
            out_ref[d, 32:48, :] = pair.astype(bf16)


def softmax_block(q, keys, values, live):
    scale = LOG2E / math.sqrt(HD)
    scores = lax.dot_general(q, keys, (((1,), (1,)), ((), ())), preferred_element_type=f32)
    n_img = keys.shape[0] - 128
    s_img = scores[:, :n_img]
    s_txt = jnp.where(live, scores[:, n_img:], neg_large)
    peak = jnp.maximum(
        jnp.max(s_img, axis=1, keepdims=True), jnp.max(s_txt, axis=1, keepdims=True)
    )
    w_img = jnp.exp2((s_img - peak) * scale)
    w_txt = jnp.exp2((s_txt - peak) * scale)
    total = jnp.sum(w_img, axis=1, keepdims=True) + jnp.sum(w_txt, axis=1, keepdims=True)
    weights = jnp.concatenate([w_img.astype(bf16), w_txt.astype(bf16)], axis=1)
    out = jnp.dot(weights, values, preferred_element_type=f32)
    return out / total, peak * scale + jnp.log2(total)


def three_parts(v):
    high = v.astype(bf16).astype(f32)
    rest = v - high
    mid = rest.astype(bf16).astype(f32)
    return high, mid, rest - mid


def live_mask(j, length):
    lane = lax.broadcasted_iota(jnp.int32, (1, 128), 1)
    index = lane + (j // 2) * 128
    return jnp.logical_and(index // 64 == j, index < length)


def text_body(
    where_ref, len_ref, kv0_ref, kv1_ref, kv2_ref, kv3_ref, txt_ref,
    p0_ref, p1_ref, p2_ref, p3_ref, keys_ref, values_ref,
):
    j = where_ref[0]
    length = len_ref[0]
    for b, ref in enumerate((kv0_ref, kv1_ref, kv2_ref, kv3_ref)):
        pair = ref[...].astype(f32)
        keys_ref[256 * b : 256 * b + 256, :] = pair[:, 0:8, :].reshape(256, HD).astype(bf16)
        values_ref[256 * b : 256 * b + 256, :] = pair[:, 8:16, :].reshape(256, HD).astype(bf16)
    start = pl.multiple_of((j // 2) * 128, 128)
    keys_ref[1024:1152, :] = txt_ref[1, pl.ds(start, 128), :]
    values_ref[1024:1152, :] = txt_ref[2, pl.ds(start, 128), :]
    keys = keys_ref[...]
    values = values_ref[...]
    live = live_mask(j, length)
    q = jnp.concatenate(
        [txt_ref[0, pl.ds(pl.multiple_of((j ^ s) * 64, 64), 64), :] for s in range(4)], axis=0
    )
    out, lse = softmax_block(q, keys, values, live)
    out = out.astype(bf16)
    row = lax.broadcasted_iota(jnp.int32, (64, 128), 0)
    lane = lax.broadcasted_iota(jnp.int32, (64, 128), 1)
    for s, ref in enumerate((p0_ref, p1_ref, p2_ref, p3_ref)):
        ref[0:64, :] = out[64 * s : 64 * s + 64]
        high, mid, low = three_parts(jnp.broadcast_to(lse[64 * s : 64 * s + 64], (64, 128)))
        first = jnp.where(row == lane % 64, jnp.where(lane < 64, high, mid), 0.0)
        second = jnp.where(row == lane, low, 0.0)
        first = jnp.broadcast_to(jnp.sum(first, axis=0, keepdims=True), (8, 128))
        second = jnp.broadcast_to(jnp.sum(second, axis=0, keepdims=True), (8, 128))
        ref[64:80, :] = jnp.concatenate([first, second], axis=0).astype(bf16)


def image_body(where_ref, len_ref, recv_ref, keys_ref, values_ref, out_ref):
    live = live_mask(where_ref[0], len_ref[0])
    keys = keys_ref[...]
    values = values_ref[...]
    row = lax.broadcasted_iota(jnp.int32, (8, 32, 128), 1)
    lane = lax.broadcasted_iota(jnp.int32, (8, 32, 128), 2)
    for b in range(4):
        q = recv_ref[8 * b : 8 * b + 8, 0:32, :].reshape(256, HD)
        out, lse = softmax_block(q, keys, values, live)
        out_ref[8 * b : 8 * b + 8, 0:32, :] = out.astype(bf16).reshape(8, 32, HD)
        high, mid, low = three_parts(jnp.broadcast_to(lse, (256, 128)).reshape(8, 32, 128))
        parts = jnp.where(lane < 32, high, jnp.where(lane < 64, mid, low))
        packed = jnp.where(jnp.logical_and(row == lane % 32, lane < 96), parts, 0.0)
        packed = jnp.sum(packed, axis=1, keepdims=True)
        out_ref[8 * b : 8 * b + 8, 32:48, :] = jnp.broadcast_to(packed, (8, 16, 128)).astype(bf16)


def blend(outs, lses):
    peak = lses[0]
    for v in lses[1:]:
        peak = jnp.maximum(peak, v)
    weights = [jnp.exp2(v - peak) for v in lses]
    total = weights[0]
    for w in weights[1:]:
        total = total + w
    mixed = outs[0] * weights[0]
    for o, w in zip(outs[1:], weights[1:]):
        mixed = mixed + o * w
    return mixed / total


def fill_body(where_ref, len_ref, img_ref, p0_ref, p1_ref, p2_ref, p3_ref, out_ref):
    row = lax.broadcasted_iota(jnp.int32, (64, 128), 0)
    lane = lax.broadcasted_iota(jnp.int32, (64, 128), 1)
    outs, lses = [], []
    for ref in (p0_ref, p1_ref, p2_ref, p3_ref):
        outs.append(ref[0:64, :].astype(f32))
        stats = ref[64:80, :].astype(f32)
        picked = jnp.where(row == lane % 64, stats[0:1], 0.0) + jnp.where(row == lane, stats[8:9], 0.0)
        lses.append(jnp.sum(picked, axis=1, keepdims=True))
    text = blend(outs, lses)
    text = jnp.where(where_ref[0] * 64 + row < len_ref[0], text, 0.0).astype(bf16)
    for d in range(32):
        out_ref[d, 0:48, :] = img_ref[d]
        out_ref[d, 48:112, :] = text


def tail_body(core_ref, recv_ref, w_ref, mine_ref, other_ref, txt_ref):
    row = lax.broadcasted_iota(jnp.int32, (32, 128), 0)
    lane = lax.broadcasted_iota(jnp.int32, (32, 128), 1)
    pick = jnp.logical_and(row == lane % 32, lane < 96)
    heads = []
    for head in range(8):
        outs, lses = [], []
        for j in range(4):
            s = head * 4 + j
            outs.append(recv_ref[s, 0:32, :].astype(f32))
            stats = recv_ref[s, 32:48, :].astype(f32)[0:1]
            lses.append(jnp.sum(jnp.where(pick, stats, 0.0), axis=1, keepdims=True))
            txt_ref[64 * j : 64 * j + 64, head * HD : (head + 1) * HD] = recv_ref[s, 48:112, :]
        heads.append(blend(outs, lses))
    rows = jnp.concatenate(heads, axis=1)
    flipped = jnp.concatenate([rows[16:32], rows[0:16]], axis=0)
    rows = jnp.where(core_ref[0] == 0, rows, flipped).astype(bf16)
    projected = jnp.dot(rows, w_ref[...], preferred_element_type=f32)
    mine_ref[...] = projected[0:16]
    other_ref[...] = projected[16:32].astype(bf16)


def shards(
    img_qkv, txt_qkv, frame_index, row_index, column_index, txt_len, residual, w_proj, proj_bias, gate
):
    tokens = img_qkv.shape[1]
    width = img_qkv.shape[3]
    d_model = w_proj.shape[1]
    j = lax.axis_index("y").astype(jnp.int32).reshape(1)
    head = lax.axis_index("zl") * 4 + lax.axis_index("x")
    core = lax.axis_index("tp").astype(jnp.int32).reshape(1)
    qkv = img_qkv.reshape(tokens, 3, width).transpose(1, 0, 2)
    txt = lax.dynamic_slice_in_dim(txt_qkv[0], head * HD, HD, 2).transpose(1, 0, 2)

    send = call(prep_body, jax.ShapeDtypeStruct((32, 48, HD), bf16), 5, name="prep")(
        qkv, frame_index, row_index, column_index, jnp.asarray(rate_table())
    )
    recv = lax.all_to_all(send, CUBE, 0, 0, tiled=True)
    kv = recv[:, 32:48, :]
    others = [lax.ppermute(kv, "zh", [(i, i ^ s) for i in range(4)]) for s in (1, 2, 3)]

    piece = jax.ShapeDtypeStruct((80, HD), bf16)
    keyed = jax.ShapeDtypeStruct((1152, HD), bf16)
    p0, p1, p2, p3, keys, values = call(
        text_body, [piece] * 4 + [keyed] * 2, 7, smem=(0, 1), name="text"
    )(j, txt_len, kv, *others, txt)
    got = [
        lax.ppermute(p, "y", [(i, i ^ s) for i in range(4)])
        for s, p in ((1, p1), (2, p2), (3, p3))
    ]
    img = call(image_body, jax.ShapeDtypeStruct((32, 48, HD), bf16), 5, smem=(0, 1), name="image")(
        j, txt_len, recv, keys, values
    )
    back = call(fill_body, jax.ShapeDtypeStruct((32, 112, HD), bf16), 7, smem=(0, 1), name="fill")(
        j, txt_len, img, p0, *got
    )
    home = lax.all_to_all(back, CUBE, 0, 0, tiled=True)
    half = tokens // 2
    mine, other, txt_out = call(
        tail_body,
        [
            jax.ShapeDtypeStruct((half, d_model), f32),
            jax.ShapeDtypeStruct((half, d_model), bf16),
            jax.ShapeDtypeStruct((256, width), bf16),
        ],
        3, smem=(0,), name="tail",
    )(core, home, w_proj)
    theirs = lax.ppermute(other, "tp", [(0, 1), (1, 0)])
    projected = mine + theirs.astype(f32)
    img_out = residual[0].astype(f32) + gate[None, :] * (projected + proj_bias[None, :])
    return img_out.astype(bf16)[None], txt_out[None]


def solution(mesh):
    split = Mesh(
        mesh.devices.reshape(4, 2, 4, 4, mesh.shape["tp"]), ("zh", "zl", "x", "y", "tp")
    )
    placed = (
        P(None, SEQ, None, "tp"),
        P(None, None, None, "tp"),
        P(None, SEQ),
        P(None, SEQ),
        P(None, SEQ),
        P(),
        P(None, SEQ + ("tp",), None),
        P("tp", None),
        P(),
        P(),
    )
    return jax.shard_map(
        shards,
        mesh=split,
        in_specs=placed,
        out_specs=(P(None, SEQ + ("tp",), None), P(None, None, "tp")),
        check_vma=False,
    )
```

```python
import math

import jax
import jax.numpy as jnp
import numpy as np
from jax import lax
from jax.experimental import pallas as pl
from jax.experimental.pallas import tpu as pltpu
from jax.sharding import Mesh
from jax.sharding import PartitionSpec as P

HD = 128
SEQ = ("zh", "zl", "x", "y")
CUBE = ("zl", "x", "y")
HEAD = ("zl", "x")
rope_base = 256.0
neg_large = -1e30
LOG2E = 1.4426950408889634
bf16 = jnp.bfloat16
f32 = jnp.float32


def vmem_spec():
    return pl.BlockSpec(memory_space=pltpu.VMEM)


def smem_spec():
    return pl.BlockSpec(memory_space=pltpu.SMEM)


def any_spec():
    return pl.BlockSpec(memory_space=pltpu.HBM)


def call(
    body, out_shape, n_in, smem=(), hbm=(), limit=40 * 1024 * 1024, scratch=(), name=None, alias=None
):
    single = not isinstance(out_shape, (tuple, list))
    outs = out_shape if not single else [out_shape]
    specs = [vmem_spec() for _ in outs]
    kernel = pl.pallas_call(
        body,
        out_shape=out_shape,
        in_specs=[
            smem_spec() if i in smem else any_spec() if i in hbm else vmem_spec() for i in range(n_in)
        ],
        out_specs=specs[0] if single else specs,
        scratch_shapes=list(scratch),
        input_output_aliases=alias or {},
        compiler_params=pltpu.CompilerParams(vmem_limit_bytes=limit),
        name=name,
    )

    def run(*operands):
        held = [
            pltpu.with_memory_space_constraint(v, pltpu.HBM) if i in hbm else v
            for i, v in enumerate(operands)
        ]
        return kernel(*held)

    return run


def rate_table():
    table = np.zeros((8, HD), np.float32)
    frame_part = HD // 8
    second = (HD - frame_part) // 2
    at = 0
    for p, width in enumerate((frame_part, second, second)):
        ids = np.arange(width // 2, dtype=np.float32)
        rates = np.float32(rope_base) ** (np.float32(-2.0) * ids / np.float32(width))
        table[p, at : at + width] = np.repeat(rates.astype(np.float32), 2)
        at += width
    return table


def prep_body(
    qkv_hbm, frame_hbm, row_hbm, col_hbm, rate_hbm, q_out, kv_out,
    qkv_ref, frame_ref, row_ref, col_ref, rate_ref, sems,
):
    copies = [
        pltpu.make_async_copy(src, dst, sems.at[i])
        for i, (src, dst) in enumerate(
            (
                (frame_hbm, frame_ref), (row_hbm, row_ref), (col_hbm, col_ref),
                (rate_hbm, rate_ref), (qkv_hbm, qkv_ref),
            )
        )
    ]
    for c in copies:
        c.start()
    for c in copies[:4]:
        c.wait()
    tokens = qkv_ref.shape[1]
    sub = lax.broadcasted_iota(jnp.int32, (8, tokens), 0)
    pos = jnp.where(
        sub == 0, frame_ref[...], jnp.where(sub == 1, row_ref[...], jnp.where(sub == 2, col_ref[...], 0))
    ).astype(f32)
    angles = lax.dot_general(
        pos, rate_ref[...], (((0,), (0,)), ((), ())), precision=lax.Precision.HIGHEST,
        preferred_element_type=f32,
    )
    lane = lax.broadcasted_iota(jnp.int32, (tokens, HD), 1)
    even = (lane % 2) == 0
    cosine = jnp.cos(angles)
    sine = jnp.sin(angles)
    sine = jnp.where(even, -sine, sine)
    copies[4].wait()

    def rotate(v):
        v = v.astype(f32)
        partner = jnp.where(even, pltpu.roll(v, HD - 1, 1), pltpu.roll(v, 1, 1))
        return (v * cosine + partner * sine).astype(bf16)

    for head in range(8):
        cols = slice(head * HD, (head + 1) * HD)
        kv_out[head, 0:32, :] = rotate(qkv_ref[1, :, cols])
        kv_out[head, 32:64, :] = qkv_ref[2, :, cols]
        query = rotate(qkv_ref[0, :, cols])
        for j in range(4):
            q_out[head * 4 + j] = query


def softmax_block(q, keys, values, live):
    scale = LOG2E / math.sqrt(HD)
    scores = lax.dot_general(q, keys, (((1,), (1,)), ((), ())), preferred_element_type=f32)
    n_img = keys.shape[0] - 128
    s_img = scores[:, :n_img]
    s_txt = jnp.where(live, scores[:, n_img:], neg_large)
    peak = jnp.maximum(
        jnp.max(s_img, axis=1, keepdims=True), jnp.max(s_txt, axis=1, keepdims=True)
    )
    w_img = jnp.exp2((s_img - peak) * scale)
    w_txt = jnp.exp2((s_txt - peak) * scale)
    total = jnp.sum(w_img, axis=1, keepdims=True) + jnp.sum(w_txt, axis=1, keepdims=True)
    weights = jnp.concatenate([w_img.astype(bf16), w_txt.astype(bf16)], axis=1)
    out = jnp.dot(weights, values, preferred_element_type=f32)
    return out / total, peak * scale + jnp.log2(total)


def three_parts(v):
    high = v.astype(bf16).astype(f32)
    rest = v - high
    mid = rest.astype(bf16).astype(f32)
    return high, mid, rest - mid


def live_mask(j, length):
    lane = lax.broadcasted_iota(jnp.int32, (1, 128), 1)
    index = lane + (j // 2) * 128
    return jnp.logical_and(index // 64 == j, index < length)


def text_body(
    where_ref, len_ref, kv0_ref, kv1_ref, kv2_ref, kv3_ref, txt_ref,
    p0_ref, p1_ref, p2_ref, p3_ref, keys_ref, values_ref,
):
    j = where_ref[0]
    length = len_ref[0]
    for b, ref in enumerate((kv0_ref, kv1_ref, kv2_ref, kv3_ref)):
        keys_ref[256 * b : 256 * b + 256, :] = ref[:, 0:32, :].reshape(256, HD)
        values_ref[256 * b : 256 * b + 256, :] = ref[:, 32:64, :].reshape(256, HD)
    start = pl.multiple_of((j // 2) * 128, 128)
    keys_ref[1024:1152, :] = txt_ref[1, pl.ds(start, 128), :]
    values_ref[1024:1152, :] = txt_ref[2, pl.ds(start, 128), :]
    keys = keys_ref[...]
    values = values_ref[...]
    live = live_mask(j, length)
    q = jnp.concatenate(
        [txt_ref[0, pl.ds(pl.multiple_of((j ^ s) * 64, 64), 64), :] for s in range(4)], axis=0
    )
    out, lse = softmax_block(q, keys, values, live)
    out = out.astype(bf16)
    row = lax.broadcasted_iota(jnp.int32, (64, 128), 0)
    lane = lax.broadcasted_iota(jnp.int32, (64, 128), 1)
    for s, ref in enumerate((p0_ref, p1_ref, p2_ref, p3_ref)):
        ref[0:64, :] = out[64 * s : 64 * s + 64]
        high, mid, low = three_parts(jnp.broadcast_to(lse[64 * s : 64 * s + 64], (64, 128)))
        first = jnp.where(row == lane % 64, jnp.where(lane < 64, high, mid), 0.0)
        second = jnp.where(row == lane, low, 0.0)
        first = jnp.broadcast_to(jnp.sum(first, axis=0, keepdims=True), (8, 128))
        second = jnp.broadcast_to(jnp.sum(second, axis=0, keepdims=True), (8, 128))
        ref[64:80, :] = jnp.concatenate([first, second], axis=0).astype(bf16)


def image_body(where_ref, len_ref, recv_ref, keys_ref, values_ref, out_ref):
    live = live_mask(where_ref[0], len_ref[0])
    keys = keys_ref[...]
    values = values_ref[...]
    row = lax.broadcasted_iota(jnp.int32, (8, 32, 128), 1)
    lane = lax.broadcasted_iota(jnp.int32, (8, 32, 128), 2)
    for b in range(4):
        q = recv_ref[8 * b : 8 * b + 8].reshape(256, HD)
        out, lse = softmax_block(q, keys, values, live)
        out_ref[8 * b : 8 * b + 8, 0:32, :] = out.astype(bf16).reshape(8, 32, HD)
        high, mid, low = three_parts(jnp.broadcast_to(lse, (256, 128)).reshape(8, 32, 128))
        parts = jnp.where(lane < 32, high, jnp.where(lane < 64, mid, low))
        packed = jnp.where(jnp.logical_and(row == lane % 32, lane < 96), parts, 0.0)
        packed = jnp.sum(packed, axis=1, keepdims=True)
        out_ref[8 * b : 8 * b + 8, 32:40, :] = jnp.broadcast_to(packed, (8, 8, 128)).astype(bf16)


def blend(outs, lses):
    peak = lses[0]
    for v in lses[1:]:
        peak = jnp.maximum(peak, v)
    weights = [jnp.exp2(v - peak) for v in lses]
    total = weights[0]
    for w in weights[1:]:
        total = total + w
    mixed = outs[0] * weights[0]
    for o, w in zip(outs[1:], weights[1:]):
        mixed = mixed + o * w
    return mixed / total


def fill_body(where_ref, len_ref, img_ref, p0_ref, p1_ref, p2_ref, p3_ref, out_ref):
    row = lax.broadcasted_iota(jnp.int32, (64, 128), 0)
    lane = lax.broadcasted_iota(jnp.int32, (64, 128), 1)
    outs, lses = [], []
    for ref in (p0_ref, p1_ref, p2_ref, p3_ref):
        outs.append(ref[0:64, :].astype(f32))
        stats = ref[64:80, :].astype(f32)
        picked = jnp.where(row == lane % 64, stats[0:1], 0.0) + jnp.where(row == lane, stats[8:9], 0.0)
        lses.append(jnp.sum(picked, axis=1, keepdims=True))
    text = blend(outs, lses)
    text = jnp.where(where_ref[0] * 64 + row < len_ref[0], text, 0.0).astype(bf16)
    for d in range(32):
        out_ref[d, 0:32, :] = img_ref[d, 0:32]
        out_ref[d, 32:96, :] = text
        out_ref[d, 96:104, :] = img_ref[d, 32:40]


def tail_body(core_ref, recv_ref, w_hbm, mine_ref, other_ref, txt_ref, w_ref, sems):
    fetches = [
        pltpu.make_async_copy(
            w_hbm.at[pl.ds(256 * i, 256)], w_ref.at[pl.ds(256 * i, 256)], sems.at[i]
        )
        for i in range(4)
    ]
    for c in fetches:
        c.start()
    row = lax.broadcasted_iota(jnp.int32, (32, 128), 0)
    lane = lax.broadcasted_iota(jnp.int32, (32, 128), 1)
    pick = jnp.logical_and(row == lane % 32, lane < 96)
    heads = []
    for head in range(8):
        outs, lses = [], []
        for j in range(4):
            s = head * 4 + j
            outs.append(recv_ref[s, 0:32, :].astype(f32))
            stats = recv_ref[s, 96:104, :].astype(f32)[0:1]
            lses.append(jnp.sum(jnp.where(pick, stats, 0.0), axis=1, keepdims=True))
            txt_ref[64 * j : 64 * j + 64, head * HD : (head + 1) * HD] = recv_ref[s, 32:96, :]
        heads.append(blend(outs, lses))
    rows = jnp.concatenate(heads, axis=1)
    flipped = jnp.concatenate([rows[16:32], rows[0:16]], axis=0)
    rows = jnp.where(core_ref[0] == 0, rows, flipped).astype(bf16)
    projected = None
    for i in range(4):
        fetches[i].wait()
        part = jnp.dot(
            rows[:, 256 * i : 256 * i + 256], w_ref[256 * i : 256 * i + 256, :],
            preferred_element_type=f32,
        )
        projected = part if projected is None else projected + part
    mine_ref[...] = projected[0:16]
    other_ref[...] = projected[16:32].astype(bf16)


def shards(
    img_qkv, txt_qkv, frame_index, row_index, column_index, txt_len, residual, w_proj, proj_bias, gate
):
    tokens = img_qkv.shape[1]
    width = img_qkv.shape[3]
    d_model = w_proj.shape[1]
    j = lax.axis_index("y").astype(jnp.int32).reshape(1)
    head = lax.axis_index("zl") * 4 + lax.axis_index("x")
    core = lax.axis_index("tp").astype(jnp.int32).reshape(1)
    qkv = img_qkv.reshape(tokens, 3, width).transpose(1, 0, 2)
    txt = lax.dynamic_slice_in_dim(txt_qkv[0], head * HD, HD, 2).transpose(1, 0, 2)

    q_send, kv_send = call(
        prep_body,
        [jax.ShapeDtypeStruct((32, 32, HD), bf16), jax.ShapeDtypeStruct((8, 64, HD), bf16)],
        5, hbm=(0, 1, 2, 3, 4), name="prep",
        scratch=(
            pltpu.VMEM((3, tokens, width), bf16),
            pltpu.VMEM((1, tokens), jnp.int32),
            pltpu.VMEM((1, tokens), jnp.int32),
            pltpu.VMEM((1, tokens), jnp.int32),
            pltpu.VMEM((8, HD), f32),
            pltpu.SemaphoreType.DMA((5,)),
        ),
    )(qkv, frame_index, row_index, column_index, jnp.asarray(rate_table()))
    kv = lax.all_to_all(kv_send, HEAD, 0, 0, tiled=True)
    others = [lax.ppermute(kv, "zh", [(i, i ^ s) for i in range(4)]) for s in (1, 2, 3)]
    q_send, _ = lax.optimization_barrier((q_send, kv))
    recv = lax.all_to_all(q_send, CUBE, 0, 0, tiled=True)

    piece = jax.ShapeDtypeStruct((80, HD), bf16)
    keyed = jax.ShapeDtypeStruct((1152, HD), bf16)
    p0, p1, p2, p3, keys, values = call(
        text_body, [piece] * 4 + [keyed] * 2, 7, smem=(0, 1), name="text"
    )(j, txt_len, kv, *others, txt)
    got = [
        lax.ppermute(p, "y", [(i, i ^ s) for i in range(4)])
        for s, p in ((1, p1), (2, p2), (3, p3))
    ]
    img = call(
        image_body, jax.ShapeDtypeStruct((32, 40, HD), bf16), 5, smem=(0, 1), name="image"
    )(j, txt_len, recv, keys, values)
    back = call(
        fill_body, jax.ShapeDtypeStruct((32, 104, HD), bf16), 7, smem=(0, 1), name="fill"
    )(j, txt_len, img, p0, *got)
    home = lax.all_to_all(back, CUBE, 0, 0, tiled=True)
    half = tokens // 2
    mine, other, txt_out = call(
        tail_body,
        [
            jax.ShapeDtypeStruct((half, d_model), f32),
            jax.ShapeDtypeStruct((half, d_model), bf16),
            jax.ShapeDtypeStruct((256, width), bf16),
        ],
        3, smem=(0,), hbm=(2,), name="tail",
        scratch=(pltpu.VMEM(w_proj.shape, bf16), pltpu.SemaphoreType.DMA((4,))),
    )(core, home, w_proj)
    theirs = lax.ppermute(other, "tp", [(0, 1), (1, 0)])
    projected = mine + theirs.astype(f32)
    img_out = residual[0].astype(f32) + gate[None, :] * (projected + proj_bias[None, :])
    return img_out.astype(bf16)[None], txt_out[None]


def solution(mesh):
    split = Mesh(
        mesh.devices.reshape(4, 2, 4, 4, mesh.shape["tp"]), ("zh", "zl", "x", "y", "tp")
    )
    placed = (
        P(None, SEQ, None, "tp"),
        P(None, None, None, "tp"),
        P(None, SEQ),
        P(None, SEQ),
        P(None, SEQ),
        P(),
        P(None, SEQ + ("tp",), None),
        P("tp", None),
        P(),
        P(),
    )
    return jax.shard_map(
        shards,
        mesh=split,
        in_specs=placed,
        out_specs=(P(None, SEQ + ("tp",), None), P(None, None, "tp")),
        check_vma=False,
    )
```

```python
import math

import jax
import jax.numpy as jnp
import numpy as np
from jax import lax
from jax.experimental import pallas as pl
from jax.experimental.pallas import tpu as pltpu
from jax.sharding import Mesh
from jax.sharding import PartitionSpec as P


HD = 128
SEQ = ("zh", "zl", "x", "y")
CUBE = ("zl", "x", "y")
HEAD = ("zl", "x")
rope_base = 256.0
neg_large = -1e30
LOG2E = 1.4426950408889634
bf16 = jnp.bfloat16
f32 = jnp.float32


def vmem_spec():
    return pl.BlockSpec(memory_space=pltpu.VMEM)


def smem_spec():
    return pl.BlockSpec(memory_space=pltpu.SMEM)


def any_spec():
    return pl.BlockSpec(memory_space=pltpu.HBM)


def call(
    body, out_shape, n_in, smem=(), hbm=(), near=(), limit=40 * 1024 * 1024, scratch=(), alias=None
):
    single = not isinstance(out_shape, (tuple, list))
    outs = out_shape if not single else [out_shape]
    specs = [vmem_spec() for _ in outs]
    kernel = pl.pallas_call(
        body,
        out_shape=out_shape,
        in_specs=[
            smem_spec() if i in smem else any_spec() if i in hbm else vmem_spec() for i in range(n_in)
        ],
        out_specs=specs[0] if single else specs,
        scratch_shapes=list(scratch),
        input_output_aliases=alias or {},
        compiler_params=pltpu.CompilerParams(vmem_limit_bytes=limit),
    )

    def run(*operands):
        held = [
            pltpu.with_memory_space_constraint(v, pltpu.HBM if i in hbm else pltpu.VMEM)
            if i in hbm or i in near
            else v
            for i, v in enumerate(operands)
        ]
        return kernel(*held)

    return run


def rate_table():
    table = np.zeros((8, HD), np.float32)
    frame_part = HD // 8
    second = (HD - frame_part) // 2
    at = 0
    for p, width in enumerate((frame_part, second, second)):
        ids = np.arange(width // 2, dtype=np.float32)
        rates = np.float32(rope_base) ** (np.float32(-2.0) * ids / np.float32(width))
        table[p, at : at + width] = np.repeat(rates.astype(np.float32), 2)
        at += width
    return table


def prep_body(
    qkv_hbm, frame_hbm, row_hbm, col_hbm, rate_hbm, q_out, kv_out,
    qkv_ref, frame_ref, row_ref, col_ref, rate_ref, sems,
):
    copies = [
        pltpu.make_async_copy(src, dst, sems.at[i])
        for i, (src, dst) in enumerate(
            (
                (frame_hbm, frame_ref), (row_hbm, row_ref), (col_hbm, col_ref),
                (rate_hbm, rate_ref), (qkv_hbm, qkv_ref),
            )
        )
    ]
    for c in copies:
        c.start()
    for c in copies[:4]:
        c.wait()
    tokens = qkv_ref.shape[1]
    sub = lax.broadcasted_iota(jnp.int32, (8, tokens), 0)
    pos = jnp.where(
        sub == 0, frame_ref[...], jnp.where(sub == 1, row_ref[...], jnp.where(sub == 2, col_ref[...], 0))
    ).astype(f32)
    angles = lax.dot_general(
        pos, rate_ref[...], (((0,), (0,)), ((), ())), precision=lax.Precision.HIGHEST,
        preferred_element_type=f32,
    )
    lane = lax.broadcasted_iota(jnp.int32, (tokens, HD), 1)
    even = (lane % 2) == 0
    cosine = jnp.cos(angles)
    sine = jnp.sin(angles)
    sine = jnp.where(even, -sine, sine)
    copies[4].wait()

    def rotate(v):
        v = v.astype(f32)
        partner = jnp.where(even, pltpu.roll(v, HD - 1, 1), pltpu.roll(v, 1, 1))
        return (v * cosine + partner * sine).astype(bf16)

    for head in range(8):
        cols = slice(head * HD, (head + 1) * HD)
        kv_out[head, 0:32, :] = rotate(qkv_ref[1, :, cols])
        kv_out[head, 32:64, :] = qkv_ref[2, :, cols]
        query = rotate(qkv_ref[0, :, cols])
        for j in range(4):
            q_out[head * 4 + j] = query


def softmax_block(q, keys, values, live):
    scale = LOG2E / math.sqrt(HD)
    scores = lax.dot_general(q, keys, (((1,), (1,)), ((), ())), preferred_element_type=f32)
    n_img = keys.shape[0] - 128
    s_img = scores[:, :n_img]
    s_txt = jnp.where(live, scores[:, n_img:], neg_large)
    peak = jnp.maximum(
        jnp.max(s_img, axis=1, keepdims=True), jnp.max(s_txt, axis=1, keepdims=True)
    )
    w_img = jnp.exp2((s_img - peak) * scale)
    w_txt = jnp.exp2((s_txt - peak) * scale)
    total = jnp.sum(w_img, axis=1, keepdims=True) + jnp.sum(w_txt, axis=1, keepdims=True)
    weights = jnp.concatenate([w_img.astype(bf16), w_txt.astype(bf16)], axis=1)
    out = jnp.dot(weights, values, preferred_element_type=f32)
    return out / total, peak * scale + jnp.log2(total)


def three_parts(v):
    high = v.astype(bf16).astype(f32)
    rest = v - high
    mid = rest.astype(bf16).astype(f32)
    return high, mid, rest - mid


def live_mask(j, length):
    lane = lax.broadcasted_iota(jnp.int32, (1, 128), 1)
    index = lane + (j // 2) * 128
    return jnp.logical_and(index // 64 == j, index < length)


def text_body(
    where_ref, len_ref, kv0_ref, kv1_ref, kv2_ref, kv3_ref, txt_ref,
    p0_ref, p1_ref, p2_ref, p3_ref, keys_ref, values_ref,
):
    j = where_ref[0]
    length = len_ref[0]
    for b, ref in enumerate((kv0_ref, kv1_ref, kv2_ref, kv3_ref)):
        keys_ref[256 * b : 256 * b + 256, :] = ref[:, 0:32, :].reshape(256, HD)
        values_ref[256 * b : 256 * b + 256, :] = ref[:, 32:64, :].reshape(256, HD)
    start = pl.multiple_of((j // 2) * 128, 128)
    keys_ref[1024:1152, :] = txt_ref[1, pl.ds(start, 128), :]
    values_ref[1024:1152, :] = txt_ref[2, pl.ds(start, 128), :]
    keys = keys_ref[...]
    values = values_ref[...]
    live = live_mask(j, length)
    q = jnp.concatenate(
        [txt_ref[0, pl.ds(pl.multiple_of((j ^ s) * 64, 64), 64), :] for s in range(4)], axis=0
    )
    out, lse = softmax_block(q, keys, values, live)
    out = out.astype(bf16)
    row = lax.broadcasted_iota(jnp.int32, (64, 128), 0)
    lane = lax.broadcasted_iota(jnp.int32, (64, 128), 1)
    for s, ref in enumerate((p0_ref, p1_ref, p2_ref, p3_ref)):
        ref[0:64, :] = out[64 * s : 64 * s + 64]
        high, mid, low = three_parts(jnp.broadcast_to(lse[64 * s : 64 * s + 64], (64, 128)))
        first = jnp.where(row == lane % 64, jnp.where(lane < 64, high, mid), 0.0)
        second = jnp.where(row == lane, low, 0.0)
        first = jnp.broadcast_to(jnp.sum(first, axis=0, keepdims=True), (8, 128))
        second = jnp.broadcast_to(jnp.sum(second, axis=0, keepdims=True), (8, 128))
        ref[64:80, :] = jnp.concatenate([first, second], axis=0).astype(bf16)


def image_body(
    where_ref, len_ref, recv_ref, keys_ref, values_ref, w_hbm, out_ref, w_out, sem
):
    fetch = pltpu.make_async_copy(w_hbm, w_out, sem)
    fetch.start()
    live = live_mask(where_ref[0], len_ref[0])
    keys = keys_ref[...]
    values = values_ref[...]
    row = lax.broadcasted_iota(jnp.int32, (8, 32, 128), 1)
    lane = lax.broadcasted_iota(jnp.int32, (8, 32, 128), 2)
    for b in range(4):
        q = recv_ref[8 * b : 8 * b + 8].reshape(256, HD)
        out, lse = softmax_block(q, keys, values, live)
        out_ref[8 * b : 8 * b + 8, 0:32, :] = out.astype(bf16).reshape(8, 32, HD)
        high, mid, low = three_parts(jnp.broadcast_to(lse, (256, 128)).reshape(8, 32, 128))
        parts = jnp.where(lane < 32, high, jnp.where(lane < 64, mid, low))
        packed = jnp.where(jnp.logical_and(row == lane % 32, lane < 96), parts, 0.0)
        packed = jnp.sum(packed, axis=1, keepdims=True)
        out_ref[8 * b : 8 * b + 8, 32:40, :] = jnp.broadcast_to(packed, (8, 8, 128)).astype(bf16)
    fetch.wait()


def blend(outs, lses):
    peak = lses[0]
    for v in lses[1:]:
        peak = jnp.maximum(peak, v)
    weights = [jnp.exp2(v - peak) for v in lses]
    total = weights[0]
    for w in weights[1:]:
        total = total + w
    mixed = outs[0] * weights[0]
    for o, w in zip(outs[1:], weights[1:]):
        mixed = mixed + o * w
    return mixed / total


def fill_body(where_ref, len_ref, img_ref, p0_ref, p1_ref, p2_ref, p3_ref, out_ref):
    row = lax.broadcasted_iota(jnp.int32, (64, 128), 0)
    lane = lax.broadcasted_iota(jnp.int32, (64, 128), 1)
    outs, lses = [], []
    for ref in (p0_ref, p1_ref, p2_ref, p3_ref):
        outs.append(ref[0:64, :].astype(f32))
        stats = ref[64:80, :].astype(f32)
        picked = jnp.where(row == lane % 64, stats[0:1], 0.0) + jnp.where(row == lane, stats[8:9], 0.0)
        lses.append(jnp.sum(picked, axis=1, keepdims=True))
    text = blend(outs, lses)
    text = jnp.where(where_ref[0] * 64 + row < len_ref[0], text, 0.0).astype(bf16)
    for d in range(32):
        out_ref[d, 0:32, :] = img_ref[d, 0:32]
        out_ref[d, 32:96, :] = text
        out_ref[d, 96:104, :] = img_ref[d, 32:40]


def tail_body(core_ref, recv_ref, w_ref, mine_ref, other_ref, txt_ref):
    row = lax.broadcasted_iota(jnp.int32, (32, 128), 0)
    lane = lax.broadcasted_iota(jnp.int32, (32, 128), 1)
    pick = jnp.logical_and(row == lane % 32, lane < 96)
    heads = []
    for head in range(8):
        outs, lses = [], []
        for j in range(4):
            s = head * 4 + j
            outs.append(recv_ref[s, 0:32, :].astype(f32))
            stats = recv_ref[s, 96:104, :].astype(f32)[0:1]
            lses.append(jnp.sum(jnp.where(pick, stats, 0.0), axis=1, keepdims=True))
            txt_ref[64 * j : 64 * j + 64, head * HD : (head + 1) * HD] = recv_ref[s, 32:96, :]
        heads.append(blend(outs, lses))
    rows = jnp.concatenate(heads, axis=1)
    flipped = jnp.concatenate([rows[16:32], rows[0:16]], axis=0)
    rows = jnp.where(core_ref[0] == 0, rows, flipped).astype(bf16)
    projected = jnp.dot(rows, w_ref[...], preferred_element_type=f32)
    mine_ref[...] = projected[0:16]
    other_ref[...] = projected[16:32].astype(bf16)


def shards(
    img_qkv, txt_qkv, frame_index, row_index, column_index, txt_len, residual, w_proj, proj_bias, gate
):
    tokens = img_qkv.shape[1]
    width = img_qkv.shape[3]
    d_model = w_proj.shape[1]
    j = lax.axis_index("y").astype(jnp.int32).reshape(1)
    head = lax.axis_index("zl") * 4 + lax.axis_index("x")
    core = lax.axis_index("tp").astype(jnp.int32).reshape(1)
    j, core, frame_index = lax.optimization_barrier((j, core, frame_index))
    qkv = img_qkv.reshape(tokens, 3, width).transpose(1, 0, 2)
    txt = lax.dynamic_slice_in_dim(txt_qkv[0], head * HD, HD, 2).transpose(1, 0, 2)

    q_send, kv_send = call(
        prep_body,
        [jax.ShapeDtypeStruct((32, 32, HD), bf16), jax.ShapeDtypeStruct((8, 64, HD), bf16)],
        5, hbm=(0, 1, 2, 3, 4),
        scratch=(
            pltpu.VMEM((3, tokens, width), bf16),
            pltpu.VMEM((1, tokens), jnp.int32),
            pltpu.VMEM((1, tokens), jnp.int32),
            pltpu.VMEM((1, tokens), jnp.int32),
            pltpu.VMEM((8, HD), f32),
            pltpu.SemaphoreType.DMA((5,)),
        ),
    )(qkv, frame_index, row_index, column_index, jnp.asarray(rate_table()))
    kv = lax.all_to_all(kv_send, HEAD, 0, 0, tiled=True)
    others = [lax.ppermute(kv, "zh", [(i, i ^ s) for i in range(4)]) for s in (1, 2, 3)]
    q_send, _ = lax.optimization_barrier((q_send, kv))
    recv = lax.all_to_all(q_send, CUBE, 0, 0, tiled=True)

    piece = jax.ShapeDtypeStruct((80, HD), bf16)
    keyed = jax.ShapeDtypeStruct((1152, HD), bf16)
    p0, p1, p2, p3, keys, values = call(
        text_body, [piece] * 4 + [keyed] * 2, 7, smem=(0, 1)
    )(j, txt_len, kv, *others, txt)
    got = [
        lax.ppermute(p, "y", [(i, i ^ s) for i in range(4)])
        for s, p in ((1, p1), (2, p2), (3, p3))
    ]
    img, w_near = call(
        image_body,
        [jax.ShapeDtypeStruct((32, 40, HD), bf16), pltpu.VMEM(w_proj.shape, bf16)],
        6, smem=(0, 1), hbm=(5,), scratch=(pltpu.SemaphoreType.DMA,),
    )(j, txt_len, recv, keys, values, w_proj)
    back = call(
        fill_body, jax.ShapeDtypeStruct((32, 104, HD), bf16), 7, smem=(0, 1)
    )(j, txt_len, img, p0, *got)
    home = lax.all_to_all(back, CUBE, 0, 0, tiled=True)
    half = tokens // 2
    mine, other, txt_out = call(
        tail_body,
        [
            jax.ShapeDtypeStruct((half, d_model), f32),
            jax.ShapeDtypeStruct((half, d_model), bf16),
            jax.ShapeDtypeStruct((256, width), bf16),
        ],
        3, smem=(0,), near=(2,),
    )(core, home, w_near)
    theirs = lax.ppermute(other, "tp", [(0, 1), (1, 0)])
    projected = mine + theirs.astype(f32)
    img_out = residual[0].astype(f32) + gate[None, :] * (projected + proj_bias[None, :])
    return img_out.astype(bf16)[None], txt_out[None]


def solution(mesh):
    split = Mesh(
        mesh.devices.reshape(4, 2, 4, 4, mesh.shape["tp"]), ("zh", "zl", "x", "y", "tp")
    )
    placed = (
        P(None, SEQ, None, "tp"),
        P(None, None, None, "tp"),
        P(None, SEQ),
        P(None, SEQ),
        P(None, SEQ),
        P(),
        P(None, SEQ + ("tp",), None),
        P("tp", None),
        P(),
        P(),
    )
    return jax.shard_map(
        shards,
        mesh=split,
        in_specs=placed,
        out_specs=(P(None, SEQ + ("tp",), None), P(None, None, "tp")),
        check_vma=False,
    )
```

```python
import math

import jax
import jax.numpy as jnp
import numpy as np
from jax import lax
from jax.experimental import pallas as pl
from jax.experimental.pallas import tpu as pltpu
from jax.sharding import Mesh
from jax.sharding import PartitionSpec as P


HD = 128
SEQ = ("zq", "zm", "zl", "x", "y")
CUBE = ("zl", "x", "y")
NEAR = ("zm", "zl", "x")
rope_base = 256.0
neg_large = -1e30
LOG2E = 1.4426950408889634
bf16 = jnp.bfloat16
f32 = jnp.float32


def vmem_spec():
    return pl.BlockSpec(memory_space=pltpu.VMEM)


def smem_spec():
    return pl.BlockSpec(memory_space=pltpu.SMEM)


def any_spec():
    return pl.BlockSpec(memory_space=pltpu.HBM)


def call(
    body, out_shape, n_in, smem=(), hbm=(), near=(), limit=40 * 1024 * 1024, scratch=(), alias=None
):
    single = not isinstance(out_shape, (tuple, list))
    outs = out_shape if not single else [out_shape]
    specs = [vmem_spec() for _ in outs]
    kernel = pl.pallas_call(
        body,
        out_shape=out_shape,
        in_specs=[
            smem_spec() if i in smem else any_spec() if i in hbm else vmem_spec() for i in range(n_in)
        ],
        out_specs=specs[0] if single else specs,
        scratch_shapes=list(scratch),
        input_output_aliases=alias or {},
        compiler_params=pltpu.CompilerParams(vmem_limit_bytes=limit),
    )

    def run(*operands):
        held = [
            pltpu.with_memory_space_constraint(v, pltpu.HBM if i in hbm else pltpu.VMEM)
            if i in hbm or i in near
            else v
            for i, v in enumerate(operands)
        ]
        return kernel(*held)

    return run


def rate_table():
    table = np.zeros((8, HD), np.float32)
    frame_part = HD // 8
    second = (HD - frame_part) // 2
    at = 0
    for p, width in enumerate((frame_part, second, second)):
        ids = np.arange(width // 2, dtype=np.float32)
        rates = np.float32(rope_base) ** (np.float32(-2.0) * ids / np.float32(width))
        table[p, at : at + width] = np.repeat(rates.astype(np.float32), 2)
        at += width
    return table


def prep_body(
    qkv_hbm, frame_hbm, row_hbm, col_hbm, rate_hbm, q_out, kv_out,
    qkv_ref, frame_ref, row_ref, col_ref, rate_ref, sems,
):
    copies = [
        pltpu.make_async_copy(src, dst, sems.at[i])
        for i, (src, dst) in enumerate(
            (
                (frame_hbm, frame_ref), (row_hbm, row_ref), (col_hbm, col_ref),
                (rate_hbm, rate_ref), (qkv_hbm, qkv_ref),
            )
        )
    ]
    for c in copies:
        c.start()
    for c in copies[:4]:
        c.wait()
    tokens = qkv_ref.shape[1]
    sub = lax.broadcasted_iota(jnp.int32, (8, tokens), 0)
    pos = jnp.where(
        sub == 0, frame_ref[...], jnp.where(sub == 1, row_ref[...], jnp.where(sub == 2, col_ref[...], 0))
    ).astype(f32)
    angles = lax.dot_general(
        pos, rate_ref[...], (((0,), (0,)), ((), ())), precision=lax.Precision.HIGHEST,
        preferred_element_type=f32,
    )
    lane = lax.broadcasted_iota(jnp.int32, (tokens, HD), 1)
    even = (lane % 2) == 0
    cosine = jnp.cos(angles)
    sine = jnp.sin(angles)
    sine = jnp.where(even, -sine, sine)
    copies[4].wait()

    def rotate(v):
        v = v.astype(f32)
        partner = jnp.where(even, pltpu.roll(v, HD - 1, 1), pltpu.roll(v, 1, 1))
        return (v * cosine + partner * sine).astype(bf16)

    for head in range(8):
        cols = slice(head * HD, (head + 1) * HD)
        key = rotate(qkv_ref[1, :, cols])
        value = qkv_ref[2, :, cols]
        for d in (head, head + 8):
            kv_out[d, 0:32, :] = key
            kv_out[d, 32:64, :] = value
        q_out[head] = rotate(qkv_ref[0, :, cols])


def softmax_block(q, keys, values, live):
    scale = LOG2E / math.sqrt(HD)
    scores = lax.dot_general(q, keys, (((1,), (1,)), ((), ())), preferred_element_type=f32)
    n_img = keys.shape[0] - 128
    s_img = scores[:, :n_img]
    s_txt = jnp.where(live, scores[:, n_img:], neg_large)
    peak = jnp.maximum(
        jnp.max(s_img, axis=1, keepdims=True), jnp.max(s_txt, axis=1, keepdims=True)
    )
    w_img = jnp.exp2((s_img - peak) * scale)
    w_txt = jnp.exp2((s_txt - peak) * scale)
    total = jnp.sum(w_img, axis=1, keepdims=True) + jnp.sum(w_txt, axis=1, keepdims=True)
    weights = jnp.concatenate([w_img.astype(bf16), w_txt.astype(bf16)], axis=1)
    out = jnp.dot(weights, values, preferred_element_type=f32)
    return out / total, peak * scale + jnp.log2(total)


def three_parts(v):
    high = v.astype(bf16).astype(f32)
    rest = v - high
    mid = rest.astype(bf16).astype(f32)
    return high, mid, rest - mid


def live_mask(j, length):
    lane = lax.broadcasted_iota(jnp.int32, (1, 128), 1)
    index = lane + (j // 2) * 128
    return jnp.logical_and(index // 64 == j, index < length)


def text_body(
    where_ref, len_ref, kv0_ref, kv1_ref, txt_ref,
    p0_ref, p1_ref, p2_ref, p3_ref, keys_ref, values_ref,
):
    j = where_ref[0]
    length = len_ref[0]
    for b, ref in enumerate((kv0_ref, kv1_ref)):
        keys_ref[512 * b : 512 * b + 512, :] = ref[:, 0:32, :].reshape(512, HD)
        values_ref[512 * b : 512 * b + 512, :] = ref[:, 32:64, :].reshape(512, HD)
    start = pl.multiple_of((j // 2) * 128, 128)
    keys_ref[1024:1152, :] = txt_ref[1, pl.ds(start, 128), :]
    values_ref[1024:1152, :] = txt_ref[2, pl.ds(start, 128), :]
    keys = keys_ref[...]
    values = values_ref[...]
    live = live_mask(j, length)
    q = jnp.concatenate(
        [txt_ref[0, pl.ds(pl.multiple_of((j ^ s) * 64, 64), 64), :] for s in range(4)], axis=0
    )
    out, lse = softmax_block(q, keys, values, live)
    out = out.astype(bf16)
    row = lax.broadcasted_iota(jnp.int32, (64, 128), 0)
    lane = lax.broadcasted_iota(jnp.int32, (64, 128), 1)
    for s, ref in enumerate((p0_ref, p1_ref, p2_ref, p3_ref)):
        ref[0:64, :] = out[64 * s : 64 * s + 64]
        high, mid, low = three_parts(jnp.broadcast_to(lse[64 * s : 64 * s + 64], (64, 128)))
        first = jnp.where(row == lane % 64, jnp.where(lane < 64, high, mid), 0.0)
        second = jnp.where(row == lane, low, 0.0)
        first = jnp.broadcast_to(jnp.sum(first, axis=0, keepdims=True), (8, 128))
        second = jnp.broadcast_to(jnp.sum(second, axis=0, keepdims=True), (8, 128))
        ref[64:80, :] = jnp.concatenate([first, second], axis=0).astype(bf16)


def image_body(
    where_ref, len_ref, recv_ref, keys_ref, values_ref, w_hbm, out_ref, w_out, sem
):
    fetch = pltpu.make_async_copy(w_hbm, w_out, sem)
    fetch.start()
    live = live_mask(where_ref[0], len_ref[0])
    keys = keys_ref[...]
    values = values_ref[...]
    row = lax.broadcasted_iota(jnp.int32, (8, 32, 128), 1)
    lane = lax.broadcasted_iota(jnp.int32, (8, 32, 128), 2)
    for b in range(4):
        q = recv_ref[8 * b : 8 * b + 8].reshape(256, HD)
        out, lse = softmax_block(q, keys, values, live)
        out_ref[8 * b : 8 * b + 8, 0:32, :] = out.astype(bf16).reshape(8, 32, HD)
        high, mid, low = three_parts(jnp.broadcast_to(lse, (256, 128)).reshape(8, 32, 128))
        parts = jnp.where(lane < 32, high, jnp.where(lane < 64, mid, low))
        packed = jnp.where(jnp.logical_and(row == lane % 32, lane < 96), parts, 0.0)
        packed = jnp.sum(packed, axis=1, keepdims=True)
        out_ref[8 * b : 8 * b + 8, 32:40, :] = jnp.broadcast_to(packed, (8, 8, 128)).astype(bf16)
    fetch.wait()


def blend(outs, lses):
    peak = lses[0]
    for v in lses[1:]:
        peak = jnp.maximum(peak, v)
    weights = [jnp.exp2(v - peak) for v in lses]
    total = weights[0]
    for w in weights[1:]:
        total = total + w
    mixed = outs[0] * weights[0]
    for o, w in zip(outs[1:], weights[1:]):
        mixed = mixed + o * w
    return mixed / total


def fill_body(where_ref, len_ref, img_ref, p0_ref, p1_ref, p2_ref, p3_ref, out_ref):
    row = lax.broadcasted_iota(jnp.int32, (64, 128), 0)
    lane = lax.broadcasted_iota(jnp.int32, (64, 128), 1)
    outs, lses = [], []
    for ref in (p0_ref, p1_ref, p2_ref, p3_ref):
        outs.append(ref[0:64, :].astype(f32))
        stats = ref[64:80, :].astype(f32)
        picked = jnp.where(row == lane % 64, stats[0:1], 0.0) + jnp.where(row == lane, stats[8:9], 0.0)
        lses.append(jnp.sum(picked, axis=1, keepdims=True))
    text = blend(outs, lses)
    text = jnp.where(where_ref[0] * 64 + row < len_ref[0], text, 0.0).astype(bf16)
    for d in range(32):
        out_ref[d, 0:32, :] = img_ref[d, 0:32]
        out_ref[d, 32:96, :] = text
        out_ref[d, 96:104, :] = img_ref[d, 32:40]


def tail_body(core_ref, recv_ref, w_ref, mine_ref, other_ref, txt_ref):
    row = lax.broadcasted_iota(jnp.int32, (32, 128), 0)
    lane = lax.broadcasted_iota(jnp.int32, (32, 128), 1)
    pick = jnp.logical_and(row == lane % 32, lane < 96)
    heads = []
    for head in range(8):
        outs, lses = [], []
        for j in range(4):
            s = head * 4 + j
            outs.append(recv_ref[s, 0:32, :].astype(f32))
            stats = recv_ref[s, 96:104, :].astype(f32)[0:1]
            lses.append(jnp.sum(jnp.where(pick, stats, 0.0), axis=1, keepdims=True))
            txt_ref[64 * j : 64 * j + 64, head * HD : (head + 1) * HD] = recv_ref[s, 32:96, :]
        heads.append(blend(outs, lses))
    rows = jnp.concatenate(heads, axis=1)
    flipped = jnp.concatenate([rows[16:32], rows[0:16]], axis=0)
    rows = jnp.where(core_ref[0] == 0, rows, flipped).astype(bf16)
    projected = jnp.dot(rows, w_ref[...], preferred_element_type=f32)
    mine_ref[...] = projected[0:16]
    other_ref[...] = projected[16:32].astype(bf16)


def shards(
    img_qkv, txt_qkv, frame_index, row_index, column_index, txt_len, residual, w_proj, proj_bias, gate
):
    tokens = img_qkv.shape[1]
    width = img_qkv.shape[3]
    d_model = w_proj.shape[1]
    j = lax.axis_index("y").astype(jnp.int32).reshape(1)
    head = lax.axis_index("zl") * 4 + lax.axis_index("x")
    core = lax.axis_index("tp").astype(jnp.int32).reshape(1)
    j, core, frame_index = lax.optimization_barrier((j, core, frame_index))
    qkv = img_qkv.reshape(tokens, 3, width).transpose(1, 0, 2)
    txt = lax.dynamic_slice_in_dim(txt_qkv[0], head * HD, HD, 2).transpose(1, 0, 2)

    q_mine, kv_send = call(
        prep_body,
        [jax.ShapeDtypeStruct((8, tokens, HD), bf16), jax.ShapeDtypeStruct((16, 64, HD), bf16)],
        5, hbm=(0, 1, 2, 3, 4),
        scratch=(
            pltpu.VMEM((3, tokens, width), bf16),
            pltpu.VMEM((1, tokens), jnp.int32),
            pltpu.VMEM((1, tokens), jnp.int32),
            pltpu.VMEM((1, tokens), jnp.int32),
            pltpu.VMEM((8, HD), f32),
            pltpu.SemaphoreType.DMA((5,)),
        ),
    )(qkv, frame_index, row_index, column_index, jnp.asarray(rate_table()))
    kv = lax.all_to_all(kv_send, NEAR, 0, 0, tiled=True)
    other = lax.ppermute(kv, "zq", [(0, 1), (1, 0)])
    q_mine, _ = lax.optimization_barrier((q_mine, kv))
    q_send = jnp.broadcast_to(q_mine[:, None], (8, 4, tokens, HD)).reshape(32, tokens, HD)
    recv = lax.all_to_all(q_send, CUBE, 0, 0, tiled=True)

    piece = jax.ShapeDtypeStruct((80, HD), bf16)
    keyed = jax.ShapeDtypeStruct((1152, HD), bf16)
    p0, p1, p2, p3, keys, values = call(
        text_body, [piece] * 4 + [keyed] * 2, 5, smem=(0, 1)
    )(j, txt_len, kv, other, txt)
    got = [
        lax.ppermute(p, "y", [(i, i ^ s) for i in range(4)])
        for s, p in ((1, p1), (2, p2), (3, p3))
    ]
    img, w_near = call(
        image_body,
        [jax.ShapeDtypeStruct((32, 40, HD), bf16), pltpu.VMEM(w_proj.shape, bf16)],
        6, smem=(0, 1), hbm=(5,), scratch=(pltpu.SemaphoreType.DMA,),
    )(j, txt_len, recv, keys, values, w_proj)
    back = call(
        fill_body, jax.ShapeDtypeStruct((32, 104, HD), bf16), 7, smem=(0, 1)
    )(j, txt_len, img, p0, *got)
    home = lax.all_to_all(back, CUBE, 0, 0, tiled=True)
    half = tokens // 2
    mine, given, txt_out = call(
        tail_body,
        [
            jax.ShapeDtypeStruct((half, d_model), f32),
            jax.ShapeDtypeStruct((half, d_model), bf16),
            jax.ShapeDtypeStruct((256, width), bf16),
        ],
        3, smem=(0,), near=(2,),
    )(core, home, w_near)
    theirs = lax.ppermute(given, "tp", [(0, 1), (1, 0)])
    projected = mine + theirs.astype(f32)
    img_out = residual[0].astype(f32) + gate[None, :] * (projected + proj_bias[None, :])
    return img_out.astype(bf16)[None], txt_out[None]


def solution(mesh):
    split = Mesh(
        mesh.devices.reshape(2, 2, 2, 4, 4, mesh.shape["tp"]), ("zq", "zm", "zl", "x", "y", "tp")
    )
    placed = (
        P(None, SEQ, None, "tp"),
        P(None, None, None, "tp"),
        P(None, SEQ),
        P(None, SEQ),
        P(None, SEQ),
        P(),
        P(None, SEQ + ("tp",), None),
        P("tp", None),
        P(),
        P(),
    )
    return jax.shard_map(
        shards,
        mesh=split,
        in_specs=placed,
        out_specs=(P(None, SEQ + ("tp",), None), P(None, None, "tp")),
        check_vma=False,
    )
```

```python
import functools
import math

import jax
import jax.numpy as jnp
import numpy as np
from jax import lax
from jax.experimental import pallas as pl
from jax.experimental.pallas import tpu as pltpu
from jax.sharding import Mesh
from jax.sharding import PartitionSpec as P


HD = 128
SEQ = ("zh", "zl", "x", "y")
CUBE = ("zl", "x", "y")
HEAD = ("zl", "x")
rope_base = 256.0
neg_large = -1e30
LOG2E = 1.4426950408889634
bf16 = jnp.bfloat16
f32 = jnp.float32


def vmem_spec():
    return pl.BlockSpec(memory_space=pltpu.VMEM)


def smem_spec():
    return pl.BlockSpec(memory_space=pltpu.SMEM)


def any_spec():
    return pl.BlockSpec(memory_space=pltpu.HBM)


def call(
    body, out_shape, n_in, smem=(), hbm=(), near=(), limit=40 * 1024 * 1024, scratch=(), alias=None
):
    single = not isinstance(out_shape, (tuple, list))
    outs = out_shape if not single else [out_shape]
    specs = [vmem_spec() for _ in outs]
    kernel = pl.pallas_call(
        body,
        out_shape=out_shape,
        in_specs=[
            smem_spec() if i in smem else any_spec() if i in hbm else vmem_spec() for i in range(n_in)
        ],
        out_specs=specs[0] if single else specs,
        scratch_shapes=list(scratch),
        input_output_aliases=alias or {},
        compiler_params=pltpu.CompilerParams(vmem_limit_bytes=limit),
    )

    def run(*operands):
        held = [
            pltpu.with_memory_space_constraint(v, pltpu.HBM if i in hbm else pltpu.VMEM)
            if i in hbm or i in near
            else v
            for i, v in enumerate(operands)
        ]
        return kernel(*held)

    return run


def rate_table():
    table = np.zeros((8, HD), np.float32)
    frame_part = HD // 8
    second = (HD - frame_part) // 2
    at = 0
    for p, width in enumerate((frame_part, second, second)):
        ids = np.arange(width // 2, dtype=np.float32)
        rates = np.float32(rope_base) ** (np.float32(-2.0) * ids / np.float32(width))
        table[p, at : at + width] = np.repeat(rates.astype(np.float32), 2)
        at += width
    return table


def prep_body(
    qkv_hbm, frame_hbm, row_hbm, col_hbm, rate_hbm, q_out, kv_out,
    qkv_ref, frame_ref, row_ref, col_ref, rate_ref, sems,
):
    copies = [
        pltpu.make_async_copy(src, dst, sems.at[i])
        for i, (src, dst) in enumerate(
            (
                (frame_hbm, frame_ref), (row_hbm, row_ref), (col_hbm, col_ref),
                (rate_hbm, rate_ref), (qkv_hbm, qkv_ref),
            )
        )
    ]
    for c in copies:
        c.start()
    for c in copies[:4]:
        c.wait()
    tokens = qkv_ref.shape[1]
    sub = lax.broadcasted_iota(jnp.int32, (8, tokens), 0)
    pos = jnp.where(
        sub == 0, frame_ref[...], jnp.where(sub == 1, row_ref[...], jnp.where(sub == 2, col_ref[...], 0))
    ).astype(f32)
    angles = lax.dot_general(
        pos, rate_ref[...], (((0,), (0,)), ((), ())), precision=lax.Precision.HIGHEST,
        preferred_element_type=f32,
    )
    lane = lax.broadcasted_iota(jnp.int32, (tokens, HD), 1)
    even = (lane % 2) == 0
    cosine = jnp.cos(angles)
    sine = jnp.sin(angles)
    sine = jnp.where(even, -sine, sine)
    copies[4].wait()

    def rotate(v):
        v = v.astype(f32)
        partner = jnp.where(even, pltpu.roll(v, HD - 1, 1), pltpu.roll(v, 1, 1))
        return (v * cosine + partner * sine).astype(bf16)

    for head in range(8):
        cols = slice(head * HD, (head + 1) * HD)
        kv_out[head, 0:32, :] = rotate(qkv_ref[1, :, cols])
        kv_out[head, 32:64, :] = qkv_ref[2, :, cols]
        q_out[head] = rotate(qkv_ref[0, :, cols])


def softmax_block(q, keys, values, live):
    scale = LOG2E / math.sqrt(HD)
    scores = lax.dot_general(q, keys, (((1,), (1,)), ((), ())), preferred_element_type=f32)
    n_img = keys.shape[0] - 128
    s_img = scores[:, :n_img]
    s_txt = jnp.where(live, scores[:, n_img:], neg_large)
    peak = jnp.maximum(
        jnp.max(s_img, axis=1, keepdims=True), jnp.max(s_txt, axis=1, keepdims=True)
    )
    w_img = jnp.exp2((s_img - peak) * scale)
    w_txt = jnp.exp2((s_txt - peak) * scale)
    total = jnp.sum(w_img, axis=1, keepdims=True) + jnp.sum(w_txt, axis=1, keepdims=True)
    weights = jnp.concatenate([w_img.astype(bf16), w_txt.astype(bf16)], axis=1)
    out = jnp.dot(weights, values, preferred_element_type=f32)
    return out / total, peak * scale + jnp.log2(total)


def three_parts(v):
    high = v.astype(bf16).astype(f32)
    rest = v - high
    mid = rest.astype(bf16).astype(f32)
    return high, mid, rest - mid


def live_mask(j, length):
    lane = lax.broadcasted_iota(jnp.int32, (1, 128), 1)
    index = lane + (j // 2) * 128
    return jnp.logical_and(index // 64 == j, index < length)


def text_body(
    where_ref, len_ref, kv0_ref, kv1_ref, kv2_ref, kv3_ref, txt_ref,
    send_ref, keep_ref, keys_ref, values_ref,
):
    j = where_ref[0]
    length = len_ref[0]
    for b, ref in enumerate((kv0_ref, kv1_ref, kv2_ref, kv3_ref)):
        keys_ref[256 * b : 256 * b + 256, :] = ref[:, 0:32, :].reshape(256, HD)
        values_ref[256 * b : 256 * b + 256, :] = ref[:, 32:64, :].reshape(256, HD)
    start = pl.multiple_of((j // 2) * 128, 128)
    keys_ref[1024:1152, :] = txt_ref[1, pl.ds(start, 128), :]
    values_ref[1024:1152, :] = txt_ref[2, pl.ds(start, 128), :]
    keys = keys_ref[...]
    values = values_ref[...]
    live = live_mask(j, length)
    q = jnp.concatenate(
        [txt_ref[0, pl.ds(pl.multiple_of((j ^ s) * 64, 64), 64), :] for s in (2, 3, 0, 1)], axis=0
    )
    out, lse = softmax_block(q, keys, values, live)
    send_ref[0:128, :] = out[0:128].astype(bf16)
    send_ref[128:136, :] = stat_rows(lse[0:128]).astype(bf16)
    keep_ref[0] = out[128:256]
    keep_ref[1] = jnp.broadcast_to(lse[128:256], (128, 128))


def stat_rows(lse):
    rows = lse.shape[0]
    row = lax.broadcasted_iota(jnp.int32, (rows, 128), 0)
    lane = lax.broadcasted_iota(jnp.int32, (rows, 128), 1)
    sub = lax.broadcasted_iota(jnp.int32, (8, 128), 0)
    packed = jnp.zeros((8, 128), f32)
    for p, part in enumerate(three_parts(jnp.broadcast_to(lse, (rows, 128)))):
        line = jnp.sum(jnp.where(row == lane, part, 0.0), axis=0, keepdims=True)
        packed = jnp.where(sub == p, line, packed)
    return packed


def stat_column(packed, rows):
    row = lax.broadcasted_iota(jnp.int32, (rows, 128), 0)
    lane = lax.broadcasted_iota(jnp.int32, (rows, 128), 1)
    line = packed[0:1] + packed[1:2] + packed[2:3]
    return jnp.sum(jnp.where(row == lane, line, 0.0), axis=1, keepdims=True)


def middle_body(keep_ref, got_ref, send_ref, out_ref):
    outs = (keep_ref[0], got_ref[0:128, :].astype(f32))
    lses = (keep_ref[1], stat_column(got_ref[128:136, :].astype(f32), 128))
    mixed, lse = blend_pair(outs, lses)
    out_ref[0] = mixed[0:64]
    out_ref[1] = lse[0:64]
    send_ref[0:64, :] = mixed[64:128].astype(bf16)
    send_ref[64:72, :] = stat_rows(lse[64:128, 0:1]).astype(bf16)


def blend_pair(outs, lses):
    peak = jnp.maximum(lses[0], lses[1])
    first = jnp.exp2(lses[0] - peak)
    second = jnp.exp2(lses[1] - peak)
    total = first + second
    return (outs[0] * first + outs[1] * second) / total, peak + jnp.log2(total)


def image_body(
    half, where_ref, len_ref, recv_ref, keys_ref, values_ref, w_hbm, out_ref, w_out, sem
):
    fetch = pltpu.make_async_copy(w_hbm.at[pl.ds(512 * half, 512)], w_out, sem)
    fetch.start()
    live = live_mask(where_ref[0], len_ref[0])
    keys = keys_ref[...]
    values = values_ref[...]
    row = lax.broadcasted_iota(jnp.int32, (8, 32, 128), 1)
    lane = lax.broadcasted_iota(jnp.int32, (8, 32, 128), 2)
    for b in range(2):
        at = 16 * half + 8 * b
        q = recv_ref[at : at + 8].reshape(256, HD)
        out, lse = softmax_block(q, keys, values, live)
        out_ref[8 * b : 8 * b + 8, 0:32, :] = out.astype(bf16).reshape(8, 32, HD)
        high, mid, low = three_parts(jnp.broadcast_to(lse, (256, 128)).reshape(8, 32, 128))
        parts = jnp.where(lane < 32, high, jnp.where(lane < 64, mid, low))
        packed = jnp.where(jnp.logical_and(row == lane % 32, lane < 96), parts, 0.0)
        packed = jnp.sum(packed, axis=1, keepdims=True)
        out_ref[8 * b : 8 * b + 8, 32:40, :] = jnp.broadcast_to(packed, (8, 8, 128)).astype(bf16)
    fetch.wait()


def blend(outs, lses):
    peak = lses[0]
    for v in lses[1:]:
        peak = jnp.maximum(peak, v)
    weights = [jnp.exp2(v - peak) for v in lses]
    total = weights[0]
    for w in weights[1:]:
        total = total + w
    mixed = outs[0] * weights[0]
    for o, w in zip(outs[1:], weights[1:]):
        mixed = mixed + o * w
    return mixed / total


def fill_body(where_ref, len_ref, img0_ref, img1_ref, keep_ref, got_ref, out_ref):
    row = lax.broadcasted_iota(jnp.int32, (64, 128), 0)
    outs = (keep_ref[0], got_ref[0:64, :].astype(f32))
    lses = (keep_ref[1], stat_column(got_ref[64:72, :].astype(f32), 64))
    text, _ = blend_pair(outs, lses)
    text = jnp.where(where_ref[0] * 64 + row < len_ref[0], text, 0.0).astype(bf16)
    for d in range(32):
        src = (img0_ref, img1_ref)[d // 16]
        out_ref[d, 0:32, :] = src[d % 16, 0:32]
        out_ref[d, 32:96, :] = text
        out_ref[d, 96:104, :] = src[d % 16, 32:40]


def tail_body(core_ref, recv_ref, w0_ref, w1_ref, mine_ref, other_ref, txt_ref):
    row = lax.broadcasted_iota(jnp.int32, (32, 128), 0)
    lane = lax.broadcasted_iota(jnp.int32, (32, 128), 1)
    pick = jnp.logical_and(row == lane % 32, lane < 96)
    heads = []
    for head in range(8):
        outs, lses = [], []
        for j in range(4):
            s = head * 4 + j
            outs.append(recv_ref[s, 0:32, :].astype(f32))
            stats = recv_ref[s, 96:104, :].astype(f32)[0:1]
            lses.append(jnp.sum(jnp.where(pick, stats, 0.0), axis=1, keepdims=True))
            txt_ref[64 * j : 64 * j + 64, head * HD : (head + 1) * HD] = recv_ref[s, 32:96, :]
        heads.append(blend(outs, lses))
    rows = jnp.concatenate(heads, axis=1)
    flipped = jnp.concatenate([rows[16:32], rows[0:16]], axis=0)
    rows = jnp.where(core_ref[0] == 0, rows, flipped).astype(bf16)
    projected = jnp.dot(rows[:, 0:512], w0_ref[...], preferred_element_type=f32) + jnp.dot(
        rows[:, 512:1024], w1_ref[...], preferred_element_type=f32
    )
    mine_ref[...] = projected[0:16]
    other_ref[...] = projected[16:32].astype(bf16)


def shards(
    img_qkv, txt_qkv, frame_index, row_index, column_index, txt_len, residual, w_proj, proj_bias, gate
):
    tokens = img_qkv.shape[1]
    width = img_qkv.shape[3]
    d_model = w_proj.shape[1]
    j = lax.axis_index("y").astype(jnp.int32).reshape(1)
    head = lax.axis_index("zl") * 4 + lax.axis_index("x")
    core = lax.axis_index("tp").astype(jnp.int32).reshape(1)
    j, core, frame_index = lax.optimization_barrier((j, core, frame_index))
    qkv = img_qkv.reshape(tokens, 3, width).transpose(1, 0, 2)
    txt = lax.dynamic_slice_in_dim(txt_qkv[0], head * HD, HD, 2).transpose(1, 0, 2)

    q_mine, kv_send = call(
        prep_body,
        [jax.ShapeDtypeStruct((8, tokens, HD), bf16), jax.ShapeDtypeStruct((8, 64, HD), bf16)],
        5, hbm=(0, 1, 2, 3, 4),
        scratch=(
            pltpu.VMEM((3, tokens, width), bf16),
            pltpu.VMEM((1, tokens), jnp.int32),
            pltpu.VMEM((1, tokens), jnp.int32),
            pltpu.VMEM((1, tokens), jnp.int32),
            pltpu.VMEM((8, HD), f32),
            pltpu.SemaphoreType.DMA((5,)),
        ),
    )(qkv, frame_index, row_index, column_index, jnp.asarray(rate_table()))
    kv = lax.all_to_all(kv_send, HEAD, 0, 0, tiled=True)
    others = [lax.ppermute(kv, "zh", [(i, i ^ s) for i in range(4)]) for s in (1, 2, 3)]
    q_mine, _ = lax.optimization_barrier((q_mine, kv))
    q_send = jnp.broadcast_to(q_mine[:, None], (8, 4, tokens, HD)).reshape(32, tokens, HD)
    recv = lax.all_to_all(q_send, CUBE, 0, 0, tiled=True)

    keyed = jax.ShapeDtypeStruct((1152, HD), bf16)
    send, keep, keys, values = call(
        text_body,
        [jax.ShapeDtypeStruct((136, HD), bf16), jax.ShapeDtypeStruct((2, 128, HD), f32)] + [keyed] * 2,
        7, smem=(0, 1),
    )(j, txt_len, kv, *others, txt)

    def image_half(half):
        return call(
            functools.partial(image_body, half),
            [
                jax.ShapeDtypeStruct((16, 40, HD), bf16),
                pltpu.VMEM((w_proj.shape[0] // 2, d_model), bf16),
            ],
            6, smem=(0, 1), hbm=(5,), scratch=(pltpu.SemaphoreType.DMA,),
        )(j, txt_len, recv, keys, values, w_proj)

    got = lax.ppermute(send, "y", [(i, i ^ 2) for i in range(4)])
    img0, w0 = image_half(0)
    send, keep = call(
        middle_body,
        [jax.ShapeDtypeStruct((72, HD), bf16), jax.ShapeDtypeStruct((2, 64, HD), f32)],
        2,
    )(keep, got)
    got = lax.ppermute(send, "y", [(i, i ^ 1) for i in range(4)])
    img1, w1 = image_half(1)
    back = call(fill_body, jax.ShapeDtypeStruct((32, 104, HD), bf16), 6, smem=(0, 1))(
        j, txt_len, img0, img1, keep, got
    )
    home = lax.all_to_all(back, CUBE, 0, 0, tiled=True)
    half = tokens // 2
    mine, other, txt_out = call(
        tail_body,
        [
            jax.ShapeDtypeStruct((half, d_model), f32),
            jax.ShapeDtypeStruct((half, d_model), bf16),
            jax.ShapeDtypeStruct((256, width), bf16),
        ],
        4, smem=(0,), near=(2, 3),
    )(core, home, w0, w1)
    theirs = lax.ppermute(other, "tp", [(0, 1), (1, 0)])
    projected = mine + theirs.astype(f32)
    img_out = residual[0].astype(f32) + gate[None, :] * (projected + proj_bias[None, :])
    return img_out.astype(bf16)[None], txt_out[None]


def solution(mesh):
    split = Mesh(
        mesh.devices.reshape(4, 2, 4, 4, mesh.shape["tp"]), ("zh", "zl", "x", "y", "tp")
    )
    placed = (
        P(None, SEQ, None, "tp"),
        P(None, None, None, "tp"),
        P(None, SEQ),
        P(None, SEQ),
        P(None, SEQ),
        P(),
        P(None, SEQ + ("tp",), None),
        P("tp", None),
        P(),
        P(),
    )
    return jax.shard_map(
        shards,
        mesh=split,
        in_specs=placed,
        out_specs=(P(None, SEQ + ("tp",), None), P(None, None, "tp")),
        check_vma=False,
    )
```

```python
import math

import jax
import jax.numpy as jnp
import numpy as np
from jax import lax
from jax.experimental import pallas as pl
from jax.experimental.pallas import tpu as pltpu
from jax.sharding import Mesh
from jax.sharding import PartitionSpec as P


HD = 128
SEQ = ("zh", "zl", "x", "y")
CUBE = ("zl", "x", "y")
HEAD = ("zl", "x")
rope_base = 256.0
neg_large = -1e30
LOG2E = 1.4426950408889634
bf16 = jnp.bfloat16
f32 = jnp.float32


def vmem_spec():
    return pl.BlockSpec(memory_space=pltpu.VMEM)


def smem_spec():
    return pl.BlockSpec(memory_space=pltpu.SMEM)


def any_spec():
    return pl.BlockSpec(memory_space=pltpu.HBM)


def call(
    body, out_shape, n_in, smem=(), hbm=(), near=(), limit=40 * 1024 * 1024, scratch=(), alias=None
):
    single = not isinstance(out_shape, (tuple, list))
    outs = out_shape if not single else [out_shape]
    specs = [vmem_spec() for _ in outs]
    kernel = pl.pallas_call(
        body,
        out_shape=out_shape,
        in_specs=[
            smem_spec() if i in smem else any_spec() if i in hbm else vmem_spec() for i in range(n_in)
        ],
        out_specs=specs[0] if single else specs,
        scratch_shapes=list(scratch),
        input_output_aliases=alias or {},
        compiler_params=pltpu.CompilerParams(vmem_limit_bytes=limit),
    )

    def run(*operands):
        held = [
            pltpu.with_memory_space_constraint(v, pltpu.HBM if i in hbm else pltpu.VMEM)
            if i in hbm or i in near
            else v
            for i, v in enumerate(operands)
        ]
        return kernel(*held)

    return run


def rate_table():
    table = np.zeros((8, HD), np.float32)
    frame_part = HD // 8
    second = (HD - frame_part) // 2
    at = 0
    for p, width in enumerate((frame_part, second, second)):
        ids = np.arange(width // 2, dtype=np.float32)
        rates = np.float32(rope_base) ** (np.float32(-2.0) * ids / np.float32(width))
        table[p, at : at + width] = np.repeat(rates.astype(np.float32), 2)
        at += width
    return table


def prep_body(
    qkv_hbm, frame_hbm, row_hbm, col_hbm, rate_hbm, out_ref,
    qkv_ref, frame_ref, row_ref, col_ref, rate_ref, sems,
):
    copies = [
        pltpu.make_async_copy(src, dst, sems.at[i])
        for i, (src, dst) in enumerate(
            (
                (frame_hbm, frame_ref), (row_hbm, row_ref), (col_hbm, col_ref),
                (rate_hbm, rate_ref), (qkv_hbm, qkv_ref),
            )
        )
    ]
    for c in copies:
        c.start()
    for c in copies[:4]:
        c.wait()
    tokens = qkv_ref.shape[1]
    sub = lax.broadcasted_iota(jnp.int32, (8, tokens), 0)
    pos = jnp.where(
        sub == 0, frame_ref[...], jnp.where(sub == 1, row_ref[...], jnp.where(sub == 2, col_ref[...], 0))
    ).astype(f32)
    angles = lax.dot_general(
        pos, rate_ref[...], (((0,), (0,)), ((), ())), precision=lax.Precision.HIGHEST,
        preferred_element_type=f32,
    )
    lane = lax.broadcasted_iota(jnp.int32, (tokens, HD), 1)
    even = (lane % 2) == 0
    cosine = jnp.cos(angles)
    sine = jnp.sin(angles)
    sine = jnp.where(even, -sine, sine)
    copies[4].wait()

    def rotate(v):
        v = v.astype(f32)
        partner = jnp.where(even, pltpu.roll(v, HD - 1, 1), pltpu.roll(v, 1, 1))
        return (v * cosine + partner * sine).astype(bf16)

    for head in range(8):
        cols = slice(head * HD, (head + 1) * HD)
        out_ref[head, 0:32, :] = rotate(qkv_ref[0, :, cols])
        out_ref[head, 32:64, :] = rotate(qkv_ref[1, :, cols])
        out_ref[head, 64:96, :] = qkv_ref[2, :, cols]


def softmax_block(q, keys, values, live):
    scale = LOG2E / math.sqrt(HD)
    scores = lax.dot_general(q, keys, (((1,), (1,)), ((), ())), preferred_element_type=f32)
    n_img = keys.shape[0] - 128
    s_img = scores[:, :n_img]
    s_txt = jnp.where(live, scores[:, n_img:], neg_large)
    peak = jnp.maximum(
        jnp.max(s_img, axis=1, keepdims=True), jnp.max(s_txt, axis=1, keepdims=True)
    )
    w_img = jnp.exp2((s_img - peak) * scale)
    w_txt = jnp.exp2((s_txt - peak) * scale)
    total = jnp.sum(w_img, axis=1, keepdims=True) + jnp.sum(w_txt, axis=1, keepdims=True)
    weights = jnp.concatenate([w_img.astype(bf16), w_txt.astype(bf16)], axis=1)
    out = jnp.dot(weights, values, preferred_element_type=f32)
    return out / total, peak * scale + jnp.log2(total)


def three_parts(v):
    high = v.astype(bf16).astype(f32)
    rest = v - high
    mid = rest.astype(bf16).astype(f32)
    return high, mid, rest - mid


def live_mask(j, length):
    lane = lax.broadcasted_iota(jnp.int32, (1, 128), 1)
    index = lane + (j // 2) * 128
    return jnp.logical_and(index // 64 == j, index < length)


def text_body(
    where_ref, len_ref, kv0_ref, kv1_ref, kv2_ref, kv3_ref, txt_ref,
    send_ref, keep_ref, keys_ref, values_ref,
):
    j = where_ref[0]
    length = len_ref[0]
    for b, ref in enumerate((kv0_ref, kv1_ref, kv2_ref, kv3_ref)):
        keys_ref[256 * b : 256 * b + 256, :] = ref[:, 0:32, :].reshape(256, HD)
        values_ref[256 * b : 256 * b + 256, :] = ref[:, 32:64, :].reshape(256, HD)
    start = pl.multiple_of((j // 2) * 128, 128)
    keys_ref[1024:1152, :] = txt_ref[1, pl.ds(start, 128), :]
    values_ref[1024:1152, :] = txt_ref[2, pl.ds(start, 128), :]
    keys = keys_ref[...]
    values = values_ref[...]
    live = live_mask(j, length)
    q = jnp.concatenate(
        [txt_ref[0, pl.ds(pl.multiple_of((j ^ s) * 64, 64), 64), :] for s in (2, 3, 0, 1)], axis=0
    )
    out, lse = softmax_block(q, keys, values, live)
    send_ref[0:128, :] = out[0:128].astype(bf16)
    send_ref[128:136, :] = stat_rows(lse[0:128]).astype(bf16)
    keep_ref[0] = out[128:256]
    keep_ref[1] = jnp.broadcast_to(lse[128:256], (128, 128))


def stat_rows(lse):
    rows = lse.shape[0]
    row = lax.broadcasted_iota(jnp.int32, (rows, 128), 0)
    lane = lax.broadcasted_iota(jnp.int32, (rows, 128), 1)
    sub = lax.broadcasted_iota(jnp.int32, (8, 128), 0)
    packed = jnp.zeros((8, 128), f32)
    for p, part in enumerate(three_parts(jnp.broadcast_to(lse, (rows, 128)))):
        line = jnp.sum(jnp.where(row == lane, part, 0.0), axis=0, keepdims=True)
        packed = jnp.where(sub == p, line, packed)
    return packed


def stat_column(packed, rows):
    row = lax.broadcasted_iota(jnp.int32, (rows, 128), 0)
    lane = lax.broadcasted_iota(jnp.int32, (rows, 128), 1)
    line = packed[0:1] + packed[1:2] + packed[2:3]
    return jnp.sum(jnp.where(row == lane, line, 0.0), axis=1, keepdims=True)


def middle_body(keep_ref, got_ref, send_ref, out_ref):
    outs = (keep_ref[0], got_ref[0:128, :].astype(f32))
    lses = (keep_ref[1], stat_column(got_ref[128:136, :].astype(f32), 128))
    mixed, lse = blend_pair(outs, lses)
    out_ref[0] = mixed[0:64]
    out_ref[1] = lse[0:64]
    send_ref[0:64, :] = mixed[64:128].astype(bf16)
    send_ref[64:72, :] = stat_rows(lse[64:128, 0:1]).astype(bf16)


def blend_pair(outs, lses):
    peak = jnp.maximum(lses[0], lses[1])
    first = jnp.exp2(lses[0] - peak)
    second = jnp.exp2(lses[1] - peak)
    total = first + second
    return (outs[0] * first + outs[1] * second) / total, peak + jnp.log2(total)


def image_body(where_ref, len_ref, q0_ref, q1_ref, keys_ref, values_ref, out0_ref, out1_ref):
    live = live_mask(where_ref[0], len_ref[0])
    keys = keys_ref[...]
    values = values_ref[...]
    row = lax.broadcasted_iota(jnp.int32, (8, 32, 128), 1)
    lane = lax.broadcasted_iota(jnp.int32, (8, 32, 128), 2)
    for q_ref, out_ref in ((q0_ref, out0_ref), (q1_ref, out1_ref)):
        out, lse = softmax_block(q_ref[...].reshape(256, HD), keys, values, live)
        out_ref[:, 0:32, :] = out.astype(bf16).reshape(8, 32, HD)
        high, mid, low = three_parts(jnp.broadcast_to(lse, (256, 128)).reshape(8, 32, 128))
        parts = jnp.where(lane < 32, high, jnp.where(lane < 64, mid, low))
        packed = jnp.where(jnp.logical_and(row == lane % 32, lane < 96), parts, 0.0)
        packed = jnp.sum(packed, axis=1, keepdims=True)
        out_ref[:, 32:40, :] = jnp.broadcast_to(packed, (8, 8, 128)).astype(bf16)


def weights_body(w_hbm, w_out, sems):
    share = w_hbm.shape[0] // 8
    copies = [
        pltpu.make_async_copy(
            w_hbm.at[pl.ds(share * i, share)], w_out.at[pl.ds(share * i, share)], sems.at[i]
        )
        for i in range(8)
    ]
    for c in copies:
        c.start()
    for c in copies:
        c.wait()


def blend(outs, lses):
    peak = lses[0]
    for v in lses[1:]:
        peak = jnp.maximum(peak, v)
    weights = [jnp.exp2(v - peak) for v in lses]
    total = weights[0]
    for w in weights[1:]:
        total = total + w
    mixed = outs[0] * weights[0]
    for o, w in zip(outs[1:], weights[1:]):
        mixed = mixed + o * w
    return mixed / total


def fill_body(
    where_ref, len_ref, img0_ref, img1_ref, img2_ref, img3_ref, keep_ref, got_ref, out_ref
):
    row = lax.broadcasted_iota(jnp.int32, (64, 128), 0)
    outs = (keep_ref[0], got_ref[0:64, :].astype(f32))
    lses = (keep_ref[1], stat_column(got_ref[64:72, :].astype(f32), 64))
    text, _ = blend_pair(outs, lses)
    text = jnp.where(where_ref[0] * 64 + row < len_ref[0], text, 0.0).astype(bf16)
    for s, src in enumerate((img0_ref, img1_ref, img2_ref, img3_ref)):
        for i in range(8):
            d = 4 * i + (where_ref[0] ^ s)
            out_ref[d, 0:32, :] = src[i, 0:32]
            out_ref[d, 32:96, :] = text
            out_ref[d, 96:104, :] = src[i, 32:40]


def tail_body(core_ref, recv_ref, w_ref, mine_ref, other_ref, txt_ref):
    row = lax.broadcasted_iota(jnp.int32, (32, 128), 0)
    lane = lax.broadcasted_iota(jnp.int32, (32, 128), 1)
    pick = jnp.logical_and(row == lane % 32, lane < 96)
    heads = []
    for head in range(8):
        outs, lses = [], []
        for j in range(4):
            s = head * 4 + j
            outs.append(recv_ref[s, 0:32, :].astype(f32))
            stats = recv_ref[s, 96:104, :].astype(f32)[0:1]
            lses.append(jnp.sum(jnp.where(pick, stats, 0.0), axis=1, keepdims=True))
            txt_ref[64 * j : 64 * j + 64, head * HD : (head + 1) * HD] = recv_ref[s, 32:96, :]
        heads.append(blend(outs, lses))
    rows = jnp.concatenate(heads, axis=1)
    flipped = jnp.concatenate([rows[16:32], rows[0:16]], axis=0)
    rows = jnp.where(core_ref[0] == 0, rows, flipped).astype(bf16)
    projected = jnp.dot(rows, w_ref[...], preferred_element_type=f32)
    mine_ref[...] = projected[0:16]
    other_ref[...] = projected[16:32].astype(bf16)


def shards(
    img_qkv, txt_qkv, frame_index, row_index, column_index, txt_len, residual, w_proj, proj_bias, gate
):
    tokens = img_qkv.shape[1]
    width = img_qkv.shape[3]
    d_model = w_proj.shape[1]
    j = lax.axis_index("y").astype(jnp.int32).reshape(1)
    head = lax.axis_index("zl") * 4 + lax.axis_index("x")
    core = lax.axis_index("tp").astype(jnp.int32).reshape(1)
    j, core, frame_index = lax.optimization_barrier((j, core, frame_index))
    qkv = img_qkv.reshape(tokens, 3, width).transpose(1, 0, 2)
    txt = lax.dynamic_slice_in_dim(txt_qkv[0], head * HD, HD, 2).transpose(1, 0, 2)

    send = call(
        prep_body,
        jax.ShapeDtypeStruct((8, 96, HD), bf16),
        5, hbm=(0, 1, 2, 3, 4),
        scratch=(
            pltpu.VMEM((3, tokens, width), bf16),
            pltpu.VMEM((1, tokens), jnp.int32),
            pltpu.VMEM((1, tokens), jnp.int32),
            pltpu.VMEM((1, tokens), jnp.int32),
            pltpu.VMEM((8, HD), f32),
            pltpu.SemaphoreType.DMA((5,)),
        ),
    )(qkv, frame_index, row_index, column_index, jnp.asarray(rate_table()))
    recv = lax.all_to_all(send, HEAD, 0, 0, tiled=True)
    kv = recv[:, 32:96]
    q = recv[:, 0:32]
    others = [lax.ppermute(kv, "zh", [(i, i ^ s) for i in range(4)]) for s in (1, 2, 3)]
    queries = [q] + [lax.ppermute(q, "y", [(i, i ^ s) for i in range(4)]) for s in (1, 2, 3)]
    w_near = call(
        weights_body, pltpu.VMEM(w_proj.shape, bf16), 1, hbm=(0,),
        scratch=(pltpu.SemaphoreType.DMA((8,)),),
    )(w_proj)
    keyed = jax.ShapeDtypeStruct((1152, HD), bf16)
    send, keep, keys, values = call(
        text_body,
        [jax.ShapeDtypeStruct((136, HD), bf16), jax.ShapeDtypeStruct((2, 128, HD), f32)] + [keyed] * 2,
        7, smem=(0, 1),
    )(j, txt_len, kv, *others, txt)

    def image_half(q0, q1):
        return call(
            image_body, [jax.ShapeDtypeStruct((8, 40, HD), bf16)] * 2, 6, smem=(0, 1)
        )(j, txt_len, q0, q1, keys, values)

    got = lax.ppermute(send, "y", [(i, i ^ 2) for i in range(4)])
    img0, img1 = image_half(queries[0], queries[1])
    send, keep = call(
        middle_body,
        [jax.ShapeDtypeStruct((72, HD), bf16), jax.ShapeDtypeStruct((2, 64, HD), f32)],
        2,
    )(keep, got)
    got = lax.ppermute(send, "y", [(i, i ^ 1) for i in range(4)])
    img2, img3 = image_half(queries[2], queries[3])
    back = call(fill_body, jax.ShapeDtypeStruct((32, 104, HD), bf16), 8, smem=(0, 1))(
        j, txt_len, img0, img1, img2, img3, keep, got
    )
    home = lax.all_to_all(back, CUBE, 0, 0, tiled=True)
    half = tokens // 2
    mine, other, txt_out = call(
        tail_body,
        [
            jax.ShapeDtypeStruct((half, d_model), f32),
            jax.ShapeDtypeStruct((half, d_model), bf16),
            jax.ShapeDtypeStruct((256, width), bf16),
        ],
        3, smem=(0,), near=(2,),
    )(core, home, w_near)
    theirs = lax.ppermute(other, "tp", [(0, 1), (1, 0)])
    projected = mine + theirs.astype(f32)
    img_out = residual[0].astype(f32) + gate[None, :] * (projected + proj_bias[None, :])
    return img_out.astype(bf16)[None], txt_out[None]


def solution(mesh):
    split = Mesh(
        mesh.devices.reshape(4, 2, 4, 4, mesh.shape["tp"]), ("zh", "zl", "x", "y", "tp")
    )
    placed = (
        P(None, SEQ, None, "tp"),
        P(None, None, None, "tp"),
        P(None, SEQ),
        P(None, SEQ),
        P(None, SEQ),
        P(),
        P(None, SEQ + ("tp",), None),
        P("tp", None),
        P(),
        P(),
    )
    return jax.shard_map(
        shards,
        mesh=split,
        in_specs=placed,
        out_specs=(P(None, SEQ + ("tp",), None), P(None, None, "tp")),
        check_vma=False,
    )
```

```python
import math

import jax
import jax.numpy as jnp
import numpy as np
from jax import lax
from jax.experimental import pallas as pl
from jax.experimental.pallas import tpu as pltpu
from jax.sharding import Mesh
from jax.sharding import PartitionSpec as P


HD = 128
SEQ = ("zh", "zl", "x", "y")
CUBE = ("zl", "x", "y")
HEAD = ("zl", "x")
rope_base = 256.0
neg_large = -1e30
LOG2E = 1.4426950408889634
bf16 = jnp.bfloat16
f32 = jnp.float32


def vmem_spec():
    return pl.BlockSpec(memory_space=pltpu.VMEM)


def smem_spec():
    return pl.BlockSpec(memory_space=pltpu.SMEM)


def any_spec():
    return pl.BlockSpec(memory_space=pltpu.HBM)


def call(
    body, out_shape, n_in, smem=(), hbm=(), near=(), limit=40 * 1024 * 1024, scratch=(), alias=None
):
    single = not isinstance(out_shape, (tuple, list))
    outs = out_shape if not single else [out_shape]
    specs = [vmem_spec() for _ in outs]
    kernel = pl.pallas_call(
        body,
        out_shape=out_shape,
        in_specs=[
            smem_spec() if i in smem else any_spec() if i in hbm else vmem_spec() for i in range(n_in)
        ],
        out_specs=specs[0] if single else specs,
        scratch_shapes=list(scratch),
        input_output_aliases=alias or {},
        compiler_params=pltpu.CompilerParams(vmem_limit_bytes=limit),
    )

    def run(*operands):
        held = [
            pltpu.with_memory_space_constraint(v, pltpu.HBM if i in hbm else pltpu.VMEM)
            if i in hbm or i in near
            else v
            for i, v in enumerate(operands)
        ]
        return kernel(*held)

    return run


def rate_table():
    table = np.zeros((8, HD), np.float32)
    frame_part = HD // 8
    second = (HD - frame_part) // 2
    at = 0
    for p, width in enumerate((frame_part, second, second)):
        ids = np.arange(width // 2, dtype=np.float32)
        rates = np.float32(rope_base) ** (np.float32(-2.0) * ids / np.float32(width))
        table[p, at : at + width] = np.repeat(rates.astype(np.float32), 2)
        at += width
    return table


def prep_body(
    qkv_hbm, frame_hbm, row_hbm, col_hbm, rate_hbm, out_ref,
    qkv_ref, frame_ref, row_ref, col_ref, rate_ref, sems,
):
    copies = [
        pltpu.make_async_copy(src, dst, sems.at[i])
        for i, (src, dst) in enumerate(
            (
                (frame_hbm, frame_ref), (row_hbm, row_ref), (col_hbm, col_ref),
                (rate_hbm, rate_ref), (qkv_hbm, qkv_ref),
            )
        )
    ]
    for c in copies:
        c.start()
    for c in copies[:4]:
        c.wait()
    tokens = qkv_ref.shape[1]
    sub = lax.broadcasted_iota(jnp.int32, (8, tokens), 0)
    pos = jnp.where(
        sub == 0, frame_ref[...], jnp.where(sub == 1, row_ref[...], jnp.where(sub == 2, col_ref[...], 0))
    ).astype(f32)
    angles = lax.dot_general(
        pos, rate_ref[...], (((0,), (0,)), ((), ())), precision=lax.Precision.HIGHEST,
        preferred_element_type=f32,
    )
    lane = lax.broadcasted_iota(jnp.int32, (tokens, HD), 1)
    even = (lane % 2) == 0
    cosine = jnp.cos(angles)
    sine = jnp.sin(angles)
    sine = jnp.where(even, -sine, sine)
    copies[4].wait()

    def rotate(v):
        v = v.astype(f32)
        partner = jnp.where(even, pltpu.roll(v, HD - 1, 1), pltpu.roll(v, 1, 1))
        return (v * cosine + partner * sine).astype(bf16)

    for head in range(8):
        cols = slice(head * HD, (head + 1) * HD)
        out_ref[head, 0:32, :] = rotate(qkv_ref[0, :, cols])
        out_ref[head, 32:64, :] = rotate(qkv_ref[1, :, cols])
        out_ref[head, 64:96, :] = qkv_ref[2, :, cols]


def softmax_block(q, keys, values, live):
    scale = LOG2E / math.sqrt(HD)
    scores = lax.dot_general(q, keys, (((1,), (1,)), ((), ())), preferred_element_type=f32)
    n_img = keys.shape[0] - 128
    s_img = scores[:, :n_img]
    s_txt = jnp.where(live, scores[:, n_img:], neg_large)
    peak = jnp.maximum(
        jnp.max(s_img, axis=1, keepdims=True), jnp.max(s_txt, axis=1, keepdims=True)
    )
    w_img = jnp.exp2((s_img - peak) * scale)
    w_txt = jnp.exp2((s_txt - peak) * scale)
    total = jnp.sum(w_img, axis=1, keepdims=True) + jnp.sum(w_txt, axis=1, keepdims=True)
    weights = jnp.concatenate([w_img.astype(bf16), w_txt.astype(bf16)], axis=1)
    out = jnp.dot(weights, values, preferred_element_type=f32)
    return out / total, peak * scale + jnp.log2(total)


def three_parts(v):
    high = v.astype(bf16).astype(f32)
    rest = v - high
    mid = rest.astype(bf16).astype(f32)
    return high, mid, rest - mid


def live_mask(j, length):
    lane = lax.broadcasted_iota(jnp.int32, (1, 128), 1)
    index = lane + (j // 2) * 128
    return jnp.logical_and(index // 64 == j, index < length)


def text_body(
    where_ref, len_ref, kv0_ref, kv1_ref, kv2_ref, kv3_ref, txt_ref,
    p0_ref, p1_ref, p2_ref, p3_ref, keys_ref, values_ref,
):
    j = where_ref[0]
    length = len_ref[0]
    for b, ref in enumerate((kv0_ref, kv1_ref, kv2_ref, kv3_ref)):
        keys_ref[256 * b : 256 * b + 256, :] = ref[:, 0:32, :].reshape(256, HD)
        values_ref[256 * b : 256 * b + 256, :] = ref[:, 32:64, :].reshape(256, HD)
    start = pl.multiple_of((j // 2) * 128, 128)
    keys_ref[1024:1152, :] = txt_ref[1, pl.ds(start, 128), :]
    values_ref[1024:1152, :] = txt_ref[2, pl.ds(start, 128), :]
    keys = keys_ref[...]
    values = values_ref[...]
    live = live_mask(j, length)
    q = jnp.concatenate(
        [txt_ref[0, pl.ds(pl.multiple_of((j ^ s) * 64, 64), 64), :] for s in range(4)], axis=0
    )
    out, lse = softmax_block(q, keys, values, live)
    out = out.astype(bf16)
    row = lax.broadcasted_iota(jnp.int32, (64, 128), 0)
    lane = lax.broadcasted_iota(jnp.int32, (64, 128), 1)
    for s, ref in enumerate((p0_ref, p1_ref, p2_ref, p3_ref)):
        ref[0:64, :] = out[64 * s : 64 * s + 64]
        high, mid, low = three_parts(jnp.broadcast_to(lse[64 * s : 64 * s + 64], (64, 128)))
        first = jnp.where(row == lane % 64, jnp.where(lane < 64, high, mid), 0.0)
        second = jnp.where(row == lane, low, 0.0)
        first = jnp.broadcast_to(jnp.sum(first, axis=0, keepdims=True), (8, 128))
        second = jnp.broadcast_to(jnp.sum(second, axis=0, keepdims=True), (8, 128))
        ref[64:80, :] = jnp.concatenate([first, second], axis=0).astype(bf16)


def image_body(
    where_ref, len_ref, q0_ref, q1_ref, q2_ref, q3_ref, keys_ref, values_ref, out_ref
):
    live = live_mask(where_ref[0], len_ref[0])
    keys = keys_ref[...]
    values = values_ref[...]
    row = lax.broadcasted_iota(jnp.int32, (8, 32, 128), 1)
    lane = lax.broadcasted_iota(jnp.int32, (8, 32, 128), 2)
    for s, q_ref in enumerate((q0_ref, q1_ref, q2_ref, q3_ref)):
        out, lse = softmax_block(q_ref[...].reshape(256, HD), keys, values, live)
        at = slice(8 * s, 8 * s + 8)
        out_ref[at, 0:32, :] = out.astype(bf16).reshape(8, 32, HD)
        high, mid, low = three_parts(jnp.broadcast_to(lse, (256, 128)).reshape(8, 32, 128))
        parts = jnp.where(lane < 32, high, jnp.where(lane < 64, mid, low))
        packed = jnp.where(jnp.logical_and(row == lane % 32, lane < 96), parts, 0.0)
        packed = jnp.sum(packed, axis=1, keepdims=True)
        out_ref[at, 32:40, :] = jnp.broadcast_to(packed, (8, 8, 128)).astype(bf16)


def weights_body(w_hbm, w_out, sems):
    share = w_hbm.shape[0] // 8
    copies = [
        pltpu.make_async_copy(
            w_hbm.at[pl.ds(share * i, share)], w_out.at[pl.ds(share * i, share)], sems.at[i]
        )
        for i in range(8)
    ]
    for c in copies:
        c.start()
    for c in copies:
        c.wait()


def blend(outs, lses):
    peak = lses[0]
    for v in lses[1:]:
        peak = jnp.maximum(peak, v)
    weights = [jnp.exp2(v - peak) for v in lses]
    total = weights[0]
    for w in weights[1:]:
        total = total + w
    mixed = outs[0] * weights[0]
    for o, w in zip(outs[1:], weights[1:]):
        mixed = mixed + o * w
    return mixed / total


def fill_body(where_ref, len_ref, img_ref, p0_ref, p1_ref, p2_ref, p3_ref, out_ref):
    row = lax.broadcasted_iota(jnp.int32, (64, 128), 0)
    lane = lax.broadcasted_iota(jnp.int32, (64, 128), 1)
    outs, lses = [], []
    for ref in (p0_ref, p1_ref, p2_ref, p3_ref):
        outs.append(ref[0:64, :].astype(f32))
        stats = ref[64:80, :].astype(f32)
        picked = jnp.where(row == lane % 64, stats[0:1], 0.0) + jnp.where(row == lane, stats[8:9], 0.0)
        lses.append(jnp.sum(picked, axis=1, keepdims=True))
    text = blend(outs, lses)
    text = jnp.where(where_ref[0] * 64 + row < len_ref[0], text, 0.0).astype(bf16)
    for s in range(4):
        for i in range(8):
            d = 4 * i + (where_ref[0] ^ s)
            out_ref[d, 0:32, :] = img_ref[8 * s + i, 0:32]
            out_ref[d, 32:96, :] = text
            out_ref[d, 96:104, :] = img_ref[8 * s + i, 32:40]


def tail_body(core_ref, recv_ref, w_ref, mine_ref, other_ref, txt_ref):
    row = lax.broadcasted_iota(jnp.int32, (32, 128), 0)
    lane = lax.broadcasted_iota(jnp.int32, (32, 128), 1)
    pick = jnp.logical_and(row == lane % 32, lane < 96)
    heads = []
    for head in range(8):
        outs, lses = [], []
        for j in range(4):
            s = head * 4 + j
            outs.append(recv_ref[s, 0:32, :].astype(f32))
            stats = recv_ref[s, 96:104, :].astype(f32)[0:1]
            lses.append(jnp.sum(jnp.where(pick, stats, 0.0), axis=1, keepdims=True))
            txt_ref[64 * j : 64 * j + 64, head * HD : (head + 1) * HD] = recv_ref[s, 32:96, :]
        heads.append(blend(outs, lses))
    rows = jnp.concatenate(heads, axis=1)
    flipped = jnp.concatenate([rows[16:32], rows[0:16]], axis=0)
    rows = jnp.where(core_ref[0] == 0, rows, flipped).astype(bf16)
    projected = jnp.dot(rows, w_ref[...], preferred_element_type=f32)
    mine_ref[...] = projected[0:16]
    other_ref[...] = projected[16:32].astype(bf16)


def shards(
    img_qkv, txt_qkv, frame_index, row_index, column_index, txt_len, residual, w_proj, proj_bias, gate
):
    tokens = img_qkv.shape[1]
    width = img_qkv.shape[3]
    d_model = w_proj.shape[1]
    j = lax.axis_index("y").astype(jnp.int32).reshape(1)
    head = lax.axis_index("zl") * 4 + lax.axis_index("x")
    core = lax.axis_index("tp").astype(jnp.int32).reshape(1)
    j, core, frame_index = lax.optimization_barrier((j, core, frame_index))
    qkv = img_qkv.reshape(tokens, 3, width).transpose(1, 0, 2)
    txt = lax.dynamic_slice_in_dim(txt_qkv[0], head * HD, HD, 2).transpose(1, 0, 2)

    send = call(
        prep_body,
        jax.ShapeDtypeStruct((8, 96, HD), bf16),
        5, hbm=(0, 1, 2, 3, 4),
        scratch=(
            pltpu.VMEM((3, tokens, width), bf16),
            pltpu.VMEM((1, tokens), jnp.int32),
            pltpu.VMEM((1, tokens), jnp.int32),
            pltpu.VMEM((1, tokens), jnp.int32),
            pltpu.VMEM((8, HD), f32),
            pltpu.SemaphoreType.DMA((5,)),
        ),
    )(qkv, frame_index, row_index, column_index, jnp.asarray(rate_table()))
    recv = lax.all_to_all(send, HEAD, 0, 0, tiled=True)
    kv = recv[:, 32:96]
    q = recv[:, 0:32]
    others = [lax.ppermute(kv, "zh", [(i, i ^ s) for i in range(4)]) for s in (1, 2, 3)]
    queries = [q] + [lax.ppermute(q, "y", [(i, i ^ s) for i in range(4)]) for s in (1, 2, 3)]
    w_near = call(
        weights_body, pltpu.VMEM(w_proj.shape, bf16), 1, hbm=(0,),
        scratch=(pltpu.SemaphoreType.DMA((8,)),),
    )(w_proj)
    piece = jax.ShapeDtypeStruct((80, HD), bf16)
    keyed = jax.ShapeDtypeStruct((1152, HD), bf16)
    p0, p1, p2, p3, keys, values = call(
        text_body, [piece] * 4 + [keyed] * 2, 7, smem=(0, 1)
    )(j, txt_len, kv, *others, txt)
    got = [
        lax.ppermute(p, "y", [(i, i ^ s) for i in range(4)])
        for s, p in ((1, p1), (2, p2), (3, p3))
    ]
    img = call(
        image_body, jax.ShapeDtypeStruct((32, 40, HD), bf16), 8, smem=(0, 1)
    )(j, txt_len, *queries, keys, values)
    back = call(fill_body, jax.ShapeDtypeStruct((32, 104, HD), bf16), 7, smem=(0, 1))(
        j, txt_len, img, p0, *got
    )
    home = lax.all_to_all(back, CUBE, 0, 0, tiled=True)
    half = tokens // 2
    mine, other, txt_out = call(
        tail_body,
        [
            jax.ShapeDtypeStruct((half, d_model), f32),
            jax.ShapeDtypeStruct((half, d_model), bf16),
            jax.ShapeDtypeStruct((256, width), bf16),
        ],
        3, smem=(0,), near=(2,),
    )(core, home, w_near)
    theirs = lax.ppermute(other, "tp", [(0, 1), (1, 0)])
    projected = mine + theirs.astype(f32)
    img_out = residual[0].astype(f32) + gate[None, :] * (projected + proj_bias[None, :])
    return img_out.astype(bf16)[None], txt_out[None]


def solution(mesh):
    split = Mesh(
        mesh.devices.reshape(4, 2, 4, 4, mesh.shape["tp"]), ("zh", "zl", "x", "y", "tp")
    )
    placed = (
        P(None, SEQ, None, "tp"),
        P(None, None, None, "tp"),
        P(None, SEQ),
        P(None, SEQ),
        P(None, SEQ),
        P(),
        P(None, SEQ + ("tp",), None),
        P("tp", None),
        P(),
        P(),
    )
    return jax.shard_map(
        shards,
        mesh=split,
        in_specs=placed,
        out_specs=(P(None, SEQ + ("tp",), None), P(None, None, "tp")),
        check_vma=False,
    )
```

```python
import math

import jax
import jax.numpy as jnp
import numpy as np
from jax import lax
from jax.experimental import pallas as pl
from jax.experimental.pallas import tpu as pltpu
from jax.sharding import Mesh
from jax.sharding import PartitionSpec as P


HD = 128
SEQ = ("zh", "zl", "x", "y")
CUBE = ("zl", "x", "y")
HEAD = ("zl", "x")
rope_base = 256.0
neg_large = -1e30
LOG2E = 1.4426950408889634
bf16 = jnp.bfloat16
f32 = jnp.float32


def vmem_spec():
    return pl.BlockSpec(memory_space=pltpu.VMEM)


def smem_spec():
    return pl.BlockSpec(memory_space=pltpu.SMEM)


def any_spec():
    return pl.BlockSpec(memory_space=pltpu.HBM)


def call(
    body, out_shape, n_in, smem=(), hbm=(), near=(), limit=40 * 1024 * 1024, scratch=(), alias=None
):
    single = not isinstance(out_shape, (tuple, list))
    outs = out_shape if not single else [out_shape]
    specs = [vmem_spec() for _ in outs]
    kernel = pl.pallas_call(
        body,
        out_shape=out_shape,
        in_specs=[
            smem_spec() if i in smem else any_spec() if i in hbm else vmem_spec() for i in range(n_in)
        ],
        out_specs=specs[0] if single else specs,
        scratch_shapes=list(scratch),
        input_output_aliases=alias or {},
        compiler_params=pltpu.CompilerParams(vmem_limit_bytes=limit),
    )

    def run(*operands):
        held = [
            pltpu.with_memory_space_constraint(v, pltpu.HBM if i in hbm else pltpu.VMEM)
            if i in hbm or i in near
            else v
            for i, v in enumerate(operands)
        ]
        return kernel(*held)

    return run


def rate_table():
    table = np.zeros((8, HD), np.float32)
    frame_part = HD // 8
    second = (HD - frame_part) // 2
    at = 0
    for p, width in enumerate((frame_part, second, second)):
        ids = np.arange(width // 2, dtype=np.float32)
        rates = np.float32(rope_base) ** (np.float32(-2.0) * ids / np.float32(width))
        table[p, at : at + width] = np.repeat(rates.astype(np.float32), 2)
        at += width
    return table


def prep_body(
    qkv_hbm, frame_hbm, row_hbm, col_hbm, rate_hbm, out_ref,
    qkv_ref, frame_ref, row_ref, col_ref, rate_ref, sems,
):
    copies = [
        pltpu.make_async_copy(src, dst, sems.at[i])
        for i, (src, dst) in enumerate(
            (
                (frame_hbm, frame_ref), (row_hbm, row_ref), (col_hbm, col_ref),
                (rate_hbm, rate_ref), (qkv_hbm, qkv_ref),
            )
        )
    ]
    for c in copies:
        c.start()
    for c in copies[:4]:
        c.wait()
    tokens = qkv_ref.shape[1]
    sub = lax.broadcasted_iota(jnp.int32, (8, tokens), 0)
    pos = jnp.where(
        sub == 0, frame_ref[...], jnp.where(sub == 1, row_ref[...], jnp.where(sub == 2, col_ref[...], 0))
    ).astype(f32)
    angles = lax.dot_general(
        pos, rate_ref[...], (((0,), (0,)), ((), ())), precision=lax.Precision.HIGHEST,
        preferred_element_type=f32,
    )
    lane = lax.broadcasted_iota(jnp.int32, (tokens, HD), 1)
    even = (lane % 2) == 0
    cosine = jnp.cos(angles)
    sine = jnp.sin(angles)
    sine = jnp.where(even, -sine, sine)
    copies[4].wait()

    def rotate(v):
        v = v.astype(f32)
        partner = jnp.where(even, pltpu.roll(v, HD - 1, 1), pltpu.roll(v, 1, 1))
        return (v * cosine + partner * sine).astype(bf16)

    for head in range(8):
        cols = slice(head * HD, (head + 1) * HD)
        out_ref[head, 0:32, :] = rotate(qkv_ref[0, :, cols])
        out_ref[head, 32:64, :] = rotate(qkv_ref[1, :, cols])
        out_ref[head, 64:96, :] = qkv_ref[2, :, cols]


def softmax_block(q, keys, values, live):
    scale = LOG2E / math.sqrt(HD)
    scores = lax.dot_general(q, keys, (((1,), (1,)), ((), ())), preferred_element_type=f32)
    n_img = keys.shape[0] - 128
    s_img = scores[:, :n_img]
    s_txt = jnp.where(live, scores[:, n_img:], neg_large)
    peak = jnp.maximum(
        jnp.max(s_img, axis=1, keepdims=True), jnp.max(s_txt, axis=1, keepdims=True)
    )
    w_img = jnp.exp2((s_img - peak) * scale)
    w_txt = jnp.exp2((s_txt - peak) * scale)
    total = jnp.sum(w_img, axis=1, keepdims=True) + jnp.sum(w_txt, axis=1, keepdims=True)
    weights = jnp.concatenate([w_img.astype(bf16), w_txt.astype(bf16)], axis=1)
    out = jnp.dot(weights, values, preferred_element_type=f32)
    return out / total, peak * scale + jnp.log2(total)


def three_parts(v):
    high = v.astype(bf16).astype(f32)
    rest = v - high
    mid = rest.astype(bf16).astype(f32)
    return high, mid, rest - mid


def live_mask(block, size, length):
    lane = lax.broadcasted_iota(jnp.int32, (1, 128), 1)
    index = lane + (block * size // 128) * 128
    return jnp.logical_and(index // size == block, index < length)


def stat_rows(lse):
    rows = lse.shape[0]
    row = lax.broadcasted_iota(jnp.int32, (rows, 128), 0)
    lane = lax.broadcasted_iota(jnp.int32, (rows, 128), 1)
    sub = lax.broadcasted_iota(jnp.int32, (8, 128), 0)
    packed = jnp.zeros((8, 128), f32)
    for p, part in enumerate(three_parts(jnp.broadcast_to(lse, (rows, 128)))):
        line = jnp.sum(jnp.where(row == lane, part, 0.0), axis=0, keepdims=True)
        packed = jnp.where(sub == p, line, packed)
    return packed.astype(bf16)


def stat_column(packed, rows):
    packed = packed.astype(f32)
    row = lax.broadcasted_iota(jnp.int32, (rows, 128), 0)
    lane = lax.broadcasted_iota(jnp.int32, (rows, 128), 1)
    line = packed[0:1] + packed[1:2] + packed[2:3]
    return jnp.sum(jnp.where(row == lane, line, 0.0), axis=1, keepdims=True)


def text_body(where_ref, len_ref, recv_ref, txt_ref, m1_ref, m2_ref, m3_ref, keep_ref):
    j = where_ref[0]
    block = where_ref[1] * 4 + j
    start = pl.multiple_of((block // 8) * 128, 128)
    keys = jnp.concatenate(
        [recv_ref[:, 32:64, :].reshape(256, HD), txt_ref[1, pl.ds(start, 128), :]], axis=0
    )
    values = jnp.concatenate(
        [recv_ref[:, 64:96, :].reshape(256, HD), txt_ref[2, pl.ds(start, 128), :]], axis=0
    )
    q = jnp.concatenate(
        [txt_ref[0, pl.ds(pl.multiple_of((j ^ s) * 64, 64), 64), :] for s in range(4)], axis=0
    )
    out, lse = softmax_block(q, keys, values, live_mask(block, 16, len_ref[0]))
    keep_ref[0] = out[0:64]
    keep_ref[1] = jnp.broadcast_to(lse[0:64], (64, 128))
    for s, ref in ((1, m1_ref), (2, m2_ref), (3, m3_ref)):
        ref[0:256, :] = recv_ref[:, 0:32, :].reshape(256, HD)
        ref[256:320, :] = out[64 * s : 64 * s + 64].astype(bf16)
        ref[320:328, :] = stat_rows(lse[64 * s : 64 * s + 64])


def level_body(keep_ref, g1_ref, g2_ref, g3_ref, send_ref, out_ref):
    outs = [keep_ref[0]] + [g[256:320, :].astype(f32) for g in (g1_ref, g2_ref, g3_ref)]
    lses = [keep_ref[1]] + [stat_column(g[320:328, :], 64) for g in (g1_ref, g2_ref, g3_ref)]
    mixed, lse = blend(outs, lses)
    out_ref[0] = mixed
    out_ref[1] = lse
    send_ref[0:64, :] = mixed.astype(bf16)
    send_ref[64:72, :] = stat_rows(lse[:, 0:1])


def image_body(
    where_ref, len_ref, recv_ref, kv1_ref, kv2_ref, kv3_ref, m1_ref, m2_ref, m3_ref, txt_ref,
    out_ref, keys_ref, values_ref,
):
    j = where_ref[0]
    keys_ref[0:256, :] = recv_ref[:, 32:64, :].reshape(256, HD)
    values_ref[0:256, :] = recv_ref[:, 64:96, :].reshape(256, HD)
    for b, ref in ((1, kv1_ref), (2, kv2_ref), (3, kv3_ref)):
        keys_ref[256 * b : 256 * b + 256, :] = ref[:, 0:32, :].reshape(256, HD)
        values_ref[256 * b : 256 * b + 256, :] = ref[:, 32:64, :].reshape(256, HD)
    start = pl.multiple_of((j // 2) * 128, 128)
    keys_ref[1024:1152, :] = txt_ref[1, pl.ds(start, 128), :]
    values_ref[1024:1152, :] = txt_ref[2, pl.ds(start, 128), :]
    live = live_mask(j, 64, len_ref[0])
    keys = keys_ref[...]
    values = values_ref[...]
    row = lax.broadcasted_iota(jnp.int32, (8, 32, 128), 1)
    lane = lax.broadcasted_iota(jnp.int32, (8, 32, 128), 2)
    for s in range(4):
        if s == 0:
            q = recv_ref[:, 0:32, :].reshape(256, HD)
        else:
            q = (m1_ref, m2_ref, m3_ref)[s - 1][0:256, :]
        out, lse = softmax_block(q, keys, values, live)
        at = slice(8 * s, 8 * s + 8)
        out_ref[at, 0:32, :] = out.astype(bf16).reshape(8, 32, HD)
        high, mid, low = three_parts(jnp.broadcast_to(lse, (256, 128)).reshape(8, 32, 128))
        parts = jnp.where(lane < 32, high, jnp.where(lane < 64, mid, low))
        packed = jnp.where(jnp.logical_and(row == lane % 32, lane < 96), parts, 0.0)
        packed = jnp.sum(packed, axis=1, keepdims=True)
        out_ref[at, 32:40, :] = jnp.broadcast_to(packed, (8, 8, 128)).astype(bf16)


def weights_body(w_hbm, w_out, sems):
    share = w_hbm.shape[0] // 8
    copies = [
        pltpu.make_async_copy(
            w_hbm.at[pl.ds(share * i, share)], w_out.at[pl.ds(share * i, share)], sems.at[i]
        )
        for i in range(8)
    ]
    for c in copies:
        c.start()
    for c in copies:
        c.wait()


def blend(outs, lses):
    peak = lses[0]
    for v in lses[1:]:
        peak = jnp.maximum(peak, v)
    weights = [jnp.exp2(v - peak) for v in lses]
    total = weights[0]
    for w in weights[1:]:
        total = total + w
    mixed = outs[0] * weights[0]
    for o, w in zip(outs[1:], weights[1:]):
        mixed = mixed + o * w
    return mixed / total, peak + jnp.log2(total)


def fill_body(where_ref, len_ref, img_ref, keep_ref, g1_ref, g2_ref, g3_ref, out_ref):
    row = lax.broadcasted_iota(jnp.int32, (64, 128), 0)
    outs = [keep_ref[0]] + [g[0:64, :].astype(f32) for g in (g1_ref, g2_ref, g3_ref)]
    lses = [keep_ref[1]] + [stat_column(g[64:72, :], 64) for g in (g1_ref, g2_ref, g3_ref)]
    text, _ = blend(outs, lses)
    text = jnp.where(where_ref[0] * 64 + row < len_ref[0], text, 0.0).astype(bf16)
    for s in range(4):
        for i in range(8):
            d = 4 * i + (where_ref[0] ^ s)
            out_ref[d, 0:32, :] = img_ref[8 * s + i, 0:32]
            out_ref[d, 32:96, :] = text
            out_ref[d, 96:104, :] = img_ref[8 * s + i, 32:40]


def tail_body(core_ref, recv_ref, w_ref, mine_ref, other_ref, txt_ref):
    row = lax.broadcasted_iota(jnp.int32, (32, 128), 0)
    lane = lax.broadcasted_iota(jnp.int32, (32, 128), 1)
    pick = jnp.logical_and(row == lane % 32, lane < 96)
    heads = []
    for head in range(8):
        outs, lses = [], []
        for j in range(4):
            s = head * 4 + j
            outs.append(recv_ref[s, 0:32, :].astype(f32))
            stats = recv_ref[s, 96:104, :].astype(f32)[0:1]
            lses.append(jnp.sum(jnp.where(pick, stats, 0.0), axis=1, keepdims=True))
            txt_ref[64 * j : 64 * j + 64, head * HD : (head + 1) * HD] = recv_ref[s, 32:96, :]
        heads.append(blend(outs, lses)[0])
    rows = jnp.concatenate(heads, axis=1)
    flipped = jnp.concatenate([rows[16:32], rows[0:16]], axis=0)
    rows = jnp.where(core_ref[0] == 0, rows, flipped).astype(bf16)
    projected = jnp.dot(rows, w_ref[...], preferred_element_type=f32)
    mine_ref[...] = projected[0:16]
    other_ref[...] = projected[16:32].astype(bf16)


def shards(
    img_qkv, txt_qkv, frame_index, row_index, column_index, txt_len, residual, w_proj, proj_bias, gate
):
    tokens = img_qkv.shape[1]
    width = img_qkv.shape[3]
    d_model = w_proj.shape[1]
    where = jnp.stack([lax.axis_index("y"), lax.axis_index("zh")]).astype(jnp.int32)
    head = lax.axis_index("zl") * 4 + lax.axis_index("x")
    core = lax.axis_index("tp").astype(jnp.int32).reshape(1)
    where, core, head, frame_index = lax.optimization_barrier((where, core, head, frame_index))
    qkv = img_qkv.reshape(tokens, 3, width).transpose(1, 0, 2)
    txt = lax.dynamic_slice_in_dim(txt_qkv[0], head * HD, HD, 2).transpose(1, 0, 2)

    send = call(
        prep_body,
        jax.ShapeDtypeStruct((8, 96, HD), bf16),
        5, hbm=(0, 1, 2, 3, 4),
        scratch=(
            pltpu.VMEM((3, tokens, width), bf16),
            pltpu.VMEM((1, tokens), jnp.int32),
            pltpu.VMEM((1, tokens), jnp.int32),
            pltpu.VMEM((1, tokens), jnp.int32),
            pltpu.VMEM((8, HD), f32),
            pltpu.SemaphoreType.DMA((5,)),
        ),
    )(qkv, frame_index, row_index, column_index, jnp.asarray(rate_table()))
    recv = lax.all_to_all(send, HEAD, 0, 0, tiled=True)
    kv = recv[:, 32:96]
    rows = 8 * tokens
    others = [lax.ppermute(kv, "zh", [(i, i ^ s) for i in range(4)]) for s in (1, 2, 3)]
    m1, m2, m3, keep = call(
        text_body,
        [jax.ShapeDtypeStruct((rows + 72, HD), bf16)] * 3
        + [jax.ShapeDtypeStruct((2, 64, HD), f32)],
        4, smem=(0, 1),
    )(where, txt_len, recv, txt)
    messages = [
        lax.ppermute(m, "y", [(i, i ^ s) for i in range(4)])
        for s, m in ((1, m1), (2, m2), (3, m3))
    ]
    w_near = call(
        weights_body, pltpu.VMEM(w_proj.shape, bf16), 1, hbm=(0,),
        scratch=(pltpu.SemaphoreType.DMA((8,)),),
    )(w_proj)
    send, keep = call(
        level_body,
        [jax.ShapeDtypeStruct((72, HD), bf16), jax.ShapeDtypeStruct((2, 64, HD), f32)],
        4,
    )(keep, *messages)
    got = [lax.ppermute(send, "zh", [(i, i ^ s) for i in range(4)]) for s in (1, 2, 3)]
    img = call(
        image_body, jax.ShapeDtypeStruct((32, 40, HD), bf16), 10, smem=(0, 1),
        scratch=(pltpu.VMEM((1152, HD), bf16), pltpu.VMEM((1152, HD), bf16)),
    )(where, txt_len, recv, *others, *messages, txt)
    back = call(fill_body, jax.ShapeDtypeStruct((32, 104, HD), bf16), 7, smem=(0, 1))(
        where, txt_len, img, keep, *got
    )
    home = lax.all_to_all(back, CUBE, 0, 0, tiled=True)
    half = tokens // 2
    mine, other, txt_out = call(
        tail_body,
        [
            jax.ShapeDtypeStruct((half, d_model), f32),
            jax.ShapeDtypeStruct((half, d_model), bf16),
            jax.ShapeDtypeStruct((256, width), bf16),
        ],
        3, smem=(0,), near=(2,),
    )(core, home, w_near)
    theirs = lax.ppermute(other, "tp", [(0, 1), (1, 0)])
    projected = mine + theirs.astype(f32)
    img_out = residual[0].astype(f32) + gate[None, :] * (projected + proj_bias[None, :])
    return img_out.astype(bf16)[None], txt_out[None]


def solution(mesh):
    split = Mesh(
        mesh.devices.reshape(4, 2, 4, 4, mesh.shape["tp"]), ("zh", "zl", "x", "y", "tp")
    )
    placed = (
        P(None, SEQ, None, "tp"),
        P(None, None, None, "tp"),
        P(None, SEQ),
        P(None, SEQ),
        P(None, SEQ),
        P(),
        P(None, SEQ + ("tp",), None),
        P("tp", None),
        P(),
        P(),
    )
    return jax.shard_map(
        shards,
        mesh=split,
        in_specs=placed,
        out_specs=(P(None, SEQ + ("tp",), None), P(None, None, "tp")),
        check_vma=False,
    )
```

```python
import math

import jax
import jax.numpy as jnp
import numpy as np
from jax import lax
from jax.experimental import pallas as pl
from jax.experimental.pallas import tpu as pltpu
from jax.sharding import Mesh
from jax.sharding import PartitionSpec as P


HD = 128
SEQ = ("zh", "zl", "x", "y")
CUBE = ("zl", "x", "y")
HEAD = ("zl", "x")
rope_base = 256.0
neg_large = -1e30
LOG2E = 1.4426950408889634
bf16 = jnp.bfloat16
f32 = jnp.float32


def vmem_spec():
    return pl.BlockSpec(memory_space=pltpu.VMEM)


def smem_spec():
    return pl.BlockSpec(memory_space=pltpu.SMEM)


def any_spec():
    return pl.BlockSpec(memory_space=pltpu.HBM)


def call(
    body, out_shape, n_in, smem=(), hbm=(), near=(), far_outs=(), limit=40 * 1024 * 1024, scratch=(), alias=None
):
    single = not isinstance(out_shape, (tuple, list))
    outs = out_shape if not single else [out_shape]
    specs = [any_spec() if i in far_outs else vmem_spec() for i in range(len(outs))]
    kernel = pl.pallas_call(
        body,
        out_shape=out_shape,
        in_specs=[
            smem_spec() if i in smem else any_spec() if i in hbm else vmem_spec() for i in range(n_in)
        ],
        out_specs=specs[0] if single else specs,
        scratch_shapes=list(scratch),
        input_output_aliases=alias or {},
        compiler_params=pltpu.CompilerParams(vmem_limit_bytes=limit),
    )

    def run(*operands):
        held = [
            pltpu.with_memory_space_constraint(v, pltpu.HBM if i in hbm else pltpu.VMEM)
            if i in hbm or i in near
            else v
            for i, v in enumerate(operands)
        ]
        return kernel(*held)

    return run


def rate_table():
    table = np.zeros((8, HD), np.float32)
    frame_part = HD // 8
    second = (HD - frame_part) // 2
    at = 0
    for p, width in enumerate((frame_part, second, second)):
        ids = np.arange(width // 2, dtype=np.float32)
        rates = np.float32(rope_base) ** (np.float32(-2.0) * ids / np.float32(width))
        table[p, at : at + width] = np.repeat(rates.astype(np.float32), 2)
        at += width
    return table


def prep_body(
    qkv_hbm, frame_hbm, row_hbm, col_hbm, rate_hbm, out_ref,
    qkv_ref, frame_ref, row_ref, col_ref, rate_ref, sems,
):
    copies = [
        pltpu.make_async_copy(src, dst, sems.at[i])
        for i, (src, dst) in enumerate(
            (
                (frame_hbm, frame_ref), (row_hbm, row_ref), (col_hbm, col_ref),
                (rate_hbm, rate_ref), (qkv_hbm, qkv_ref),
            )
        )
    ]
    for c in copies:
        c.start()
    for c in copies[:4]:
        c.wait()
    tokens = qkv_ref.shape[1]
    sub = lax.broadcasted_iota(jnp.int32, (8, tokens), 0)
    pos = jnp.where(
        sub == 0, frame_ref[...], jnp.where(sub == 1, row_ref[...], jnp.where(sub == 2, col_ref[...], 0))
    ).astype(f32)
    angles = lax.dot_general(
        pos, rate_ref[...], (((0,), (0,)), ((), ())), precision=lax.Precision.HIGHEST,
        preferred_element_type=f32,
    )
    lane = lax.broadcasted_iota(jnp.int32, (tokens, HD), 1)
    even = (lane % 2) == 0
    cosine = jnp.cos(angles)
    sine = jnp.sin(angles)
    sine = jnp.where(even, -sine, sine)
    copies[4].wait()

    def rotate(v):
        v = v.astype(f32)
        partner = jnp.where(even, pltpu.roll(v, HD - 1, 1), pltpu.roll(v, 1, 1))
        return (v * cosine + partner * sine).astype(bf16)

    for head in range(8):
        cols = slice(head * HD, (head + 1) * HD)
        out_ref[head, 0:32, :] = rotate(qkv_ref[0, :, cols])
        out_ref[head, 32:64, :] = rotate(qkv_ref[1, :, cols])
        out_ref[head, 64:96, :] = qkv_ref[2, :, cols]


def softmax_block(q, keys, values, live):
    scale = LOG2E / math.sqrt(HD)
    scores = lax.dot_general(q, keys, (((1,), (1,)), ((), ())), preferred_element_type=f32)
    n_img = keys.shape[0] - 128
    s_img = scores[:, :n_img]
    s_txt = jnp.where(live, scores[:, n_img:], neg_large)
    peak = jnp.maximum(
        jnp.max(s_img, axis=1, keepdims=True), jnp.max(s_txt, axis=1, keepdims=True)
    )
    w_img = jnp.exp2((s_img - peak) * scale)
    w_txt = jnp.exp2((s_txt - peak) * scale)
    total = jnp.sum(w_img, axis=1, keepdims=True) + jnp.sum(w_txt, axis=1, keepdims=True)
    weights = jnp.concatenate([w_img.astype(bf16), w_txt.astype(bf16)], axis=1)
    out = jnp.dot(weights, values, preferred_element_type=f32)
    return out / total, peak * scale + jnp.log2(total)


def three_parts(v):
    high = v.astype(bf16).astype(f32)
    rest = v - high
    mid = rest.astype(bf16).astype(f32)
    return high, mid, rest - mid


def live_mask(j, length):
    lane = lax.broadcasted_iota(jnp.int32, (1, 128), 1)
    index = lane + (j // 2) * 128
    return jnp.logical_and(index // 64 == j, index < length)


SCALE = LOG2E / math.sqrt(HD)


def text_queries(txt_ref, j):
    return jnp.concatenate(
        [txt_ref[0, pl.ds(pl.multiple_of((j ^ s) * 64, 64), 64), :] for s in range(4)], axis=0
    )


def early_body(where_ref, len_ref, recv_ref, kv_ref, txt_ref, acc_ref, stat_ref):
    j = where_ref[0]
    start = pl.multiple_of((j // 2) * 128, 128)
    keys = jnp.concatenate(
        [
            recv_ref[:, 32:64, :].reshape(256, HD), kv_ref[:, 0:32, :].reshape(256, HD),
            txt_ref[1, pl.ds(start, 128), :],
        ],
        axis=0,
    )
    values = jnp.concatenate(
        [
            recv_ref[:, 64:96, :].reshape(256, HD), kv_ref[:, 32:64, :].reshape(256, HD),
            txt_ref[2, pl.ds(start, 128), :],
        ],
        axis=0,
    )
    q = text_queries(txt_ref, j)
    scores = lax.dot_general(q, keys, (((1,), (1,)), ((), ())), preferred_element_type=f32)
    s_txt = jnp.where(live_mask(j, len_ref[0]), scores[:, 512:], neg_large)
    peak = jnp.maximum(
        jnp.max(scores[:, :512], axis=1, keepdims=True), jnp.max(s_txt, axis=1, keepdims=True)
    )
    w_img = jnp.exp2((scores[:, :512] - peak) * SCALE)
    w_txt = jnp.exp2((s_txt - peak) * SCALE)
    total = jnp.sum(w_img, axis=1, keepdims=True) + jnp.sum(w_txt, axis=1, keepdims=True)
    weights = jnp.concatenate([w_img.astype(bf16), w_txt.astype(bf16)], axis=1)
    acc_ref[...] = jnp.dot(weights, values, preferred_element_type=f32)
    stat_ref[0] = jnp.broadcast_to(peak, (256, 128))
    stat_ref[1] = jnp.broadcast_to(total, (256, 128))


def text_body(
    where_ref, kv0_ref, kv1_ref, txt_ref, acc_ref, stat_ref, p0_ref, p1_ref, p2_ref, p3_ref
):
    keys = jnp.concatenate([r[:, 0:32, :].reshape(256, HD) for r in (kv0_ref, kv1_ref)], axis=0)
    values = jnp.concatenate([r[:, 32:64, :].reshape(256, HD) for r in (kv0_ref, kv1_ref)], axis=0)
    q = text_queries(txt_ref, where_ref[0])
    scores = lax.dot_general(q, keys, (((1,), (1,)), ((), ())), preferred_element_type=f32)
    before = stat_ref[0][:, 0:1]
    peak = jnp.maximum(before, jnp.max(scores, axis=1, keepdims=True))
    shrink = jnp.exp2((before - peak) * SCALE)
    weights = jnp.exp2((scores - peak) * SCALE)
    total = stat_ref[1][:, 0:1] * shrink + jnp.sum(weights, axis=1, keepdims=True)
    out = acc_ref[...] * shrink + jnp.dot(weights.astype(bf16), values, preferred_element_type=f32)
    out = out / total
    lse = peak * SCALE + jnp.log2(total)
    out = out.astype(bf16)
    row = lax.broadcasted_iota(jnp.int32, (64, 128), 0)
    lane = lax.broadcasted_iota(jnp.int32, (64, 128), 1)
    for s, ref in enumerate((p0_ref, p1_ref, p2_ref, p3_ref)):
        ref[0:64, :] = out[64 * s : 64 * s + 64]
        high, mid, low = three_parts(jnp.broadcast_to(lse[64 * s : 64 * s + 64], (64, 128)))
        first = jnp.where(row == lane % 64, jnp.where(lane < 64, high, mid), 0.0)
        second = jnp.where(row == lane, low, 0.0)
        first = jnp.broadcast_to(jnp.sum(first, axis=0, keepdims=True), (8, 128))
        second = jnp.broadcast_to(jnp.sum(second, axis=0, keepdims=True), (8, 128))
        ref[64:80, :] = jnp.concatenate([first, second], axis=0).astype(bf16)


def image_body(
    where_ref, len_ref, recv_ref, kv1_ref, kv2_ref, kv3_ref, q1_ref, q2_ref, q3_ref, txt_ref,
    out_ref, keys_ref, values_ref,
):
    j = where_ref[0]
    keys_ref[0:256, :] = recv_ref[:, 32:64, :].reshape(256, HD)
    values_ref[0:256, :] = recv_ref[:, 64:96, :].reshape(256, HD)
    for b, ref in ((1, kv1_ref), (2, kv2_ref), (3, kv3_ref)):
        keys_ref[256 * b : 256 * b + 256, :] = ref[:, 0:32, :].reshape(256, HD)
        values_ref[256 * b : 256 * b + 256, :] = ref[:, 32:64, :].reshape(256, HD)
    start = pl.multiple_of((j // 2) * 128, 128)
    keys_ref[1024:1152, :] = txt_ref[1, pl.ds(start, 128), :]
    values_ref[1024:1152, :] = txt_ref[2, pl.ds(start, 128), :]
    live = live_mask(j, len_ref[0])
    keys = keys_ref[...]
    values = values_ref[...]
    row = lax.broadcasted_iota(jnp.int32, (8, 32, 128), 1)
    lane = lax.broadcasted_iota(jnp.int32, (8, 32, 128), 2)
    for s in range(4):
        q = recv_ref[:, 0:32, :] if s == 0 else (q1_ref, q2_ref, q3_ref)[s - 1][...]
        out, lse = softmax_block(q.reshape(256, HD), keys, values, live)
        at = slice(8 * s, 8 * s + 8)
        out_ref[at, 0:32, :] = out.astype(bf16).reshape(8, 32, HD)
        high, mid, low = three_parts(jnp.broadcast_to(lse, (256, 128)).reshape(8, 32, 128))
        parts = jnp.where(lane < 32, high, jnp.where(lane < 64, mid, low))
        packed = jnp.where(jnp.logical_and(row == lane % 32, lane < 96), parts, 0.0)
        packed = jnp.sum(packed, axis=1, keepdims=True)
        out_ref[at, 32:40, :] = jnp.broadcast_to(packed, (8, 8, 128)).astype(bf16)


def weights_body(w_hbm, w_out, sems):
    share = w_hbm.shape[0] // 8
    copies = [
        pltpu.make_async_copy(
            w_hbm.at[pl.ds(share * i, share)], w_out.at[pl.ds(share * i, share)], sems.at[i]
        )
        for i in range(8)
    ]
    for c in copies:
        c.start()
    for c in copies:
        c.wait()


def blend(outs, lses):
    peak = lses[0]
    for v in lses[1:]:
        peak = jnp.maximum(peak, v)
    weights = [jnp.exp2(v - peak) for v in lses]
    total = weights[0]
    for w in weights[1:]:
        total = total + w
    mixed = outs[0] * weights[0]
    for o, w in zip(outs[1:], weights[1:]):
        mixed = mixed + o * w
    return mixed / total


def fill_body(where_ref, len_ref, img_ref, p0_ref, p1_ref, p2_ref, p3_ref, out_ref):
    row = lax.broadcasted_iota(jnp.int32, (64, 128), 0)
    lane = lax.broadcasted_iota(jnp.int32, (64, 128), 1)
    outs, lses = [], []
    for ref in (p0_ref, p1_ref, p2_ref, p3_ref):
        outs.append(ref[0:64, :].astype(f32))
        stats = ref[64:80, :].astype(f32)
        picked = jnp.where(row == lane % 64, stats[0:1], 0.0) + jnp.where(row == lane, stats[8:9], 0.0)
        lses.append(jnp.sum(picked, axis=1, keepdims=True))
    text = blend(outs, lses)
    text = jnp.where(where_ref[0] * 64 + row < len_ref[0], text, 0.0).astype(bf16)
    for s in range(4):
        for i in range(8):
            d = 4 * i + (where_ref[0] ^ s)
            out_ref[d, 0:32, :] = img_ref[8 * s + i, 0:32]
            out_ref[d, 32:96, :] = text
            out_ref[d, 96:104, :] = img_ref[8 * s + i, 32:40]


def tail_body(core_ref, recv_ref, w_ref, mine_ref, other_ref, txt_out, txt_ref, sem):
    row = lax.broadcasted_iota(jnp.int32, (32, 128), 0)
    lane = lax.broadcasted_iota(jnp.int32, (32, 128), 1)
    pick = jnp.logical_and(row == lane % 32, lane < 96)
    heads = []
    for head in range(8):
        outs, lses = [], []
        for j in range(4):
            s = head * 4 + j
            outs.append(recv_ref[s, 0:32, :].astype(f32))
            stats = recv_ref[s, 96:104, :].astype(f32)[0:1]
            lses.append(jnp.sum(jnp.where(pick, stats, 0.0), axis=1, keepdims=True))
            txt_ref[64 * j : 64 * j + 64, head * HD : (head + 1) * HD] = recv_ref[s, 32:96, :]
        heads.append(blend(outs, lses))
    leave = pltpu.make_async_copy(txt_ref, txt_out, sem)
    leave.start()
    rows = jnp.concatenate(heads, axis=1)
    flipped = jnp.concatenate([rows[16:32], rows[0:16]], axis=0)
    rows = jnp.where(core_ref[0] == 0, rows, flipped).astype(bf16)
    projected = jnp.dot(rows, w_ref[...], preferred_element_type=f32)
    mine_ref[...] = projected[0:16]
    other_ref[...] = projected[16:32].astype(bf16)
    leave.wait()


def shards(
    img_qkv, txt_qkv, frame_index, row_index, column_index, txt_len, residual, w_proj, proj_bias, gate
):
    tokens = img_qkv.shape[1]
    width = img_qkv.shape[3]
    d_model = w_proj.shape[1]
    j = lax.axis_index("y").astype(jnp.int32).reshape(1)
    head = lax.axis_index("zl") * 4 + lax.axis_index("x")
    core = lax.axis_index("tp").astype(jnp.int32).reshape(1)
    j, core, head, frame_index = lax.optimization_barrier((j, core, head, frame_index))
    qkv = img_qkv.reshape(tokens, 3, width).transpose(1, 0, 2)
    txt = lax.dynamic_slice_in_dim(txt_qkv[0], head * HD, HD, 2).transpose(1, 0, 2)

    send = call(
        prep_body,
        jax.ShapeDtypeStruct((8, 96, HD), bf16),
        5, hbm=(0, 1, 2, 3, 4),
        scratch=(
            pltpu.VMEM((3, tokens, width), bf16),
            pltpu.VMEM((1, tokens), jnp.int32),
            pltpu.VMEM((1, tokens), jnp.int32),
            pltpu.VMEM((1, tokens), jnp.int32),
            pltpu.VMEM((8, HD), f32),
            pltpu.SemaphoreType.DMA((5,)),
        ),
    )(qkv, frame_index, row_index, column_index, jnp.asarray(rate_table()))
    recv = lax.all_to_all(send, HEAD, 0, 0, tiled=True)
    kv = recv[:, 32:96]
    q = recv[:, 0:32]
    others = {}
    for s in (2, 3, 1):
        others[s] = lax.ppermute(kv, "zh", [(i, i ^ s) for i in range(4)])
    queries = [lax.ppermute(q, "y", [(i, i ^ s) for i in range(4)]) for s in (1, 2, 3)]
    w_near = call(
        weights_body, pltpu.VMEM(w_proj.shape, bf16), 1, hbm=(0,),
        scratch=(pltpu.SemaphoreType.DMA((8,)),),
    )(w_proj)
    piece = jax.ShapeDtypeStruct((80, HD), bf16)
    got = {}
    acc, stat = call(
        early_body,
        [jax.ShapeDtypeStruct((256, HD), f32), jax.ShapeDtypeStruct((2, 256, 128), f32)],
        5, smem=(0, 1),
    )(j, txt_len, recv, others[2], txt)
    pieces = call(text_body, [piece] * 4, 6, smem=(0,))(j, others[3], others[1], txt, acc, stat)
    for s in (2, 3, 1):
        got[s] = lax.ppermute(pieces[s], "y", [(i, i ^ s) for i in range(4)])
    img = call(
        image_body, jax.ShapeDtypeStruct((32, 40, HD), bf16), 10, smem=(0, 1),
        scratch=(pltpu.VMEM((1152, HD), bf16), pltpu.VMEM((1152, HD), bf16)),
    )(j, txt_len, recv, others[1], others[2], others[3], *queries, txt)
    back = call(fill_body, jax.ShapeDtypeStruct((32, 104, HD), bf16), 7, smem=(0, 1))(
        j, txt_len, img, pieces[0], got[1], got[2], got[3]
    )
    home = lax.all_to_all(back, CUBE, 0, 0, tiled=True)
    half = tokens // 2
    mine, other, txt_out = call(
        tail_body,
        [
            jax.ShapeDtypeStruct((half, d_model), f32),
            jax.ShapeDtypeStruct((half, d_model), bf16),
            pltpu.HBM((256, width), bf16),
        ],
        3, smem=(0,), near=(2,), far_outs=(2,),
        scratch=(pltpu.VMEM((256, width), bf16), pltpu.SemaphoreType.DMA),
    )(core, home, w_near)
    theirs = lax.ppermute(other, "tp", [(0, 1), (1, 0)])
    projected = mine + theirs.astype(f32)
    img_out = residual[0].astype(f32) + gate[None, :] * (projected + proj_bias[None, :])
    return img_out.astype(bf16)[None], txt_out[None]


def solution(mesh):
    split = Mesh(
        mesh.devices.reshape(4, 2, 4, 4, mesh.shape["tp"]), ("zh", "zl", "x", "y", "tp")
    )
    placed = (
        P(None, SEQ, None, "tp"),
        P(None, None, None, "tp"),
        P(None, SEQ),
        P(None, SEQ),
        P(None, SEQ),
        P(),
        P(None, SEQ + ("tp",), None),
        P("tp", None),
        P(),
        P(),
    )
    return jax.shard_map(
        shards,
        mesh=split,
        in_specs=placed,
        out_specs=(P(None, SEQ + ("tp",), None), P(None, None, "tp")),
        check_vma=False,
    )
```

```python
import math

import jax
import jax.numpy as jnp
import numpy as np
from jax import lax
from jax.experimental import pallas as pl
from jax.experimental.pallas import tpu as pltpu
from jax.sharding import Mesh
from jax.sharding import PartitionSpec as P


HD = 128
SEQ = ("zh", "zl", "x", "y")
CUBE = ("zl", "x", "y")
HEAD = ("zl", "x")
rope_base = 256.0
neg_large = -1e30
LOG2E = 1.4426950408889634
bf16 = jnp.bfloat16
f32 = jnp.float32


def vmem_spec():
    return pl.BlockSpec(memory_space=pltpu.VMEM)


def smem_spec():
    return pl.BlockSpec(memory_space=pltpu.SMEM)


def any_spec():
    return pl.BlockSpec(memory_space=pltpu.HBM)


def call(
    body, out_shape, n_in, smem=(), hbm=(), near=(), far_outs=(), limit=40 * 1024 * 1024, scratch=(), alias=None
):
    single = not isinstance(out_shape, (tuple, list))
    outs = out_shape if not single else [out_shape]
    specs = [any_spec() if i in far_outs else vmem_spec() for i in range(len(outs))]
    kernel = pl.pallas_call(
        body,
        out_shape=out_shape,
        in_specs=[
            smem_spec() if i in smem else any_spec() if i in hbm else vmem_spec() for i in range(n_in)
        ],
        out_specs=specs[0] if single else specs,
        scratch_shapes=list(scratch),
        input_output_aliases=alias or {},
        compiler_params=pltpu.CompilerParams(vmem_limit_bytes=limit),
    )

    def run(*operands):
        held = [
            pltpu.with_memory_space_constraint(v, pltpu.HBM if i in hbm else pltpu.VMEM)
            if i in hbm or i in near
            else v
            for i, v in enumerate(operands)
        ]
        return kernel(*held)

    return run


def rate_table():
    table = np.zeros((8, HD), np.float32)
    frame_part = HD // 8
    second = (HD - frame_part) // 2
    at = 0
    for p, width in enumerate((frame_part, second, second)):
        ids = np.arange(width // 2, dtype=np.float32)
        rates = np.float32(rope_base) ** (np.float32(-2.0) * ids / np.float32(width))
        table[p, at : at + width] = np.repeat(rates.astype(np.float32), 2)
        at += width
    return table


def prep_body(
    qkv_hbm, frame_hbm, row_hbm, col_hbm, rate_hbm, out_ref,
    qkv_ref, frame_ref, row_ref, col_ref, rate_ref, sems,
):
    copies = [
        pltpu.make_async_copy(src, dst, sems.at[i])
        for i, (src, dst) in enumerate(
            (
                (frame_hbm, frame_ref), (row_hbm, row_ref), (col_hbm, col_ref),
                (rate_hbm, rate_ref), (qkv_hbm, qkv_ref),
            )
        )
    ]
    for c in copies:
        c.start()
    for c in copies[:4]:
        c.wait()
    tokens = qkv_ref.shape[1]
    sub = lax.broadcasted_iota(jnp.int32, (8, tokens), 0)
    pos = jnp.where(
        sub == 0, frame_ref[...], jnp.where(sub == 1, row_ref[...], jnp.where(sub == 2, col_ref[...], 0))
    ).astype(f32)
    angles = lax.dot_general(
        pos, rate_ref[...], (((0,), (0,)), ((), ())), precision=lax.Precision.HIGHEST,
        preferred_element_type=f32,
    )
    lane = lax.broadcasted_iota(jnp.int32, (tokens, HD), 1)
    even = (lane % 2) == 0
    cosine = jnp.cos(angles)
    sine = jnp.sin(angles)
    sine = jnp.where(even, -sine, sine)
    copies[4].wait()

    def rotate(v):
        v = v.astype(f32)
        partner = jnp.where(even, pltpu.roll(v, HD - 1, 1), pltpu.roll(v, 1, 1))
        return (v * cosine + partner * sine).astype(bf16)

    for head in range(8):
        cols = slice(head * HD, (head + 1) * HD)
        out_ref[head, 0:32, :] = rotate(qkv_ref[0, :, cols])
        out_ref[head, 32:64, :] = rotate(qkv_ref[1, :, cols])
        out_ref[head, 64:96, :] = qkv_ref[2, :, cols]


def softmax_block(q, keys, values, live):
    scale = LOG2E / math.sqrt(HD)
    scores = lax.dot_general(q, keys, (((1,), (1,)), ((), ())), preferred_element_type=f32)
    n_img = keys.shape[0] - 128
    s_img = scores[:, :n_img]
    s_txt = jnp.where(live, scores[:, n_img:], neg_large)
    peak = jnp.maximum(
        jnp.max(s_img, axis=1, keepdims=True), jnp.max(s_txt, axis=1, keepdims=True)
    )
    w_img = jnp.exp2((s_img - peak) * scale)
    w_txt = jnp.exp2((s_txt - peak) * scale)
    total = jnp.sum(w_img, axis=1, keepdims=True) + jnp.sum(w_txt, axis=1, keepdims=True)
    weights = jnp.concatenate([w_img.astype(bf16), w_txt.astype(bf16)], axis=1)
    out = jnp.dot(weights, values, preferred_element_type=f32)
    return out / total, peak * scale + jnp.log2(total)


def three_parts(v):
    high = v.astype(bf16).astype(f32)
    rest = v - high
    mid = rest.astype(bf16).astype(f32)
    return high, mid, rest - mid


def live_mask(j, length):
    lane = lax.broadcasted_iota(jnp.int32, (1, 128), 1)
    index = lane + (j // 2) * 128
    return jnp.logical_and(index // 64 == j, index < length)


SCALE = LOG2E / math.sqrt(HD)


def text_queries(txt_ref, j):
    return jnp.concatenate(
        [txt_ref[0, pl.ds(pl.multiple_of((j ^ s) * 64, 64), 64), :] for s in range(4)], axis=0
    )


def early_body(where_ref, len_ref, recv_ref, kv_ref, txt_ref, acc_ref, stat_ref):
    j = where_ref[0]
    start = pl.multiple_of((j // 2) * 128, 128)
    keys = jnp.concatenate(
        [
            recv_ref[:, 32:64, :].reshape(256, HD), kv_ref[:, 0:32, :].reshape(256, HD),
            txt_ref[1, pl.ds(start, 128), :],
        ],
        axis=0,
    )
    values = jnp.concatenate(
        [
            recv_ref[:, 64:96, :].reshape(256, HD), kv_ref[:, 32:64, :].reshape(256, HD),
            txt_ref[2, pl.ds(start, 128), :],
        ],
        axis=0,
    )
    q = text_queries(txt_ref, j)
    scores = lax.dot_general(q, keys, (((1,), (1,)), ((), ())), preferred_element_type=f32)
    s_txt = jnp.where(live_mask(j, len_ref[0]), scores[:, 512:], neg_large)
    peak = jnp.maximum(
        jnp.max(scores[:, :512], axis=1, keepdims=True), jnp.max(s_txt, axis=1, keepdims=True)
    )
    w_img = jnp.exp2((scores[:, :512] - peak) * SCALE)
    w_txt = jnp.exp2((s_txt - peak) * SCALE)
    total = jnp.sum(w_img, axis=1, keepdims=True) + jnp.sum(w_txt, axis=1, keepdims=True)
    weights = jnp.concatenate([w_img.astype(bf16), w_txt.astype(bf16)], axis=1)
    acc_ref[...] = jnp.dot(weights, values, preferred_element_type=f32)
    stat_ref[0] = jnp.broadcast_to(peak, (256, 128))
    stat_ref[1] = jnp.broadcast_to(total, (256, 128))


def text_body(
    where_ref, kv0_ref, kv1_ref, txt_ref, acc_ref, stat_ref, p0_ref, p1_ref, p2_ref, p3_ref
):
    keys = jnp.concatenate([r[:, 0:32, :].reshape(256, HD) for r in (kv0_ref, kv1_ref)], axis=0)
    values = jnp.concatenate([r[:, 32:64, :].reshape(256, HD) for r in (kv0_ref, kv1_ref)], axis=0)
    q = text_queries(txt_ref, where_ref[0])
    scores = lax.dot_general(q, keys, (((1,), (1,)), ((), ())), preferred_element_type=f32)
    before = stat_ref[0][:, 0:1]
    peak = jnp.maximum(before, jnp.max(scores, axis=1, keepdims=True))
    shrink = jnp.exp2((before - peak) * SCALE)
    weights = jnp.exp2((scores - peak) * SCALE)
    total = stat_ref[1][:, 0:1] * shrink + jnp.sum(weights, axis=1, keepdims=True)
    out = acc_ref[...] * shrink + jnp.dot(weights.astype(bf16), values, preferred_element_type=f32)
    out = out / total
    lse = peak * SCALE + jnp.log2(total)
    out = out.astype(bf16)
    row = lax.broadcasted_iota(jnp.int32, (64, 128), 0)
    lane = lax.broadcasted_iota(jnp.int32, (64, 128), 1)
    for s, ref in enumerate((p0_ref, p1_ref, p2_ref, p3_ref)):
        ref[0:64, :] = out[64 * s : 64 * s + 64]
        high, mid, low = three_parts(jnp.broadcast_to(lse[64 * s : 64 * s + 64], (64, 128)))
        first = jnp.where(row == lane % 64, jnp.where(lane < 64, high, mid), 0.0)
        second = jnp.where(row == lane, low, 0.0)
        first = jnp.broadcast_to(jnp.sum(first, axis=0, keepdims=True), (8, 128))
        second = jnp.broadcast_to(jnp.sum(second, axis=0, keepdims=True), (8, 128))
        ref[64:80, :] = jnp.concatenate([first, second], axis=0).astype(bf16)


def image_body(
    where_ref, len_ref, recv_ref, kv1_ref, kv2_ref, kv3_ref, q1_ref, q2_ref, q3_ref, txt_ref,
    out_ref, keys_ref, values_ref,
):
    j = where_ref[0]
    keys_ref[0:256, :] = recv_ref[:, 32:64, :].reshape(256, HD)
    values_ref[0:256, :] = recv_ref[:, 64:96, :].reshape(256, HD)
    for b, ref in ((1, kv1_ref), (2, kv2_ref), (3, kv3_ref)):
        keys_ref[256 * b : 256 * b + 256, :] = ref[:, 0:32, :].reshape(256, HD)
        values_ref[256 * b : 256 * b + 256, :] = ref[:, 32:64, :].reshape(256, HD)
    start = pl.multiple_of((j // 2) * 128, 128)
    keys_ref[1024:1152, :] = txt_ref[1, pl.ds(start, 128), :]
    values_ref[1024:1152, :] = txt_ref[2, pl.ds(start, 128), :]
    live = live_mask(j, len_ref[0])
    keys = keys_ref[...]
    values = values_ref[...]
    row = lax.broadcasted_iota(jnp.int32, (8, 32, 128), 1)
    lane = lax.broadcasted_iota(jnp.int32, (8, 32, 128), 2)
    for s in range(4):
        q = recv_ref[:, 0:32, :] if s == 0 else (q1_ref, q2_ref, q3_ref)[s - 1][...]
        out, lse = softmax_block(q.reshape(256, HD), keys, values, live)
        at = slice(8 * s, 8 * s + 8)
        out_ref[at, 0:32, :] = out.astype(bf16).reshape(8, 32, HD)
        high, mid, low = three_parts(jnp.broadcast_to(lse, (256, 128)).reshape(8, 32, 128))
        parts = jnp.where(lane < 32, high, jnp.where(lane < 64, mid, low))
        packed = jnp.where(jnp.logical_and(row == lane % 32, lane < 96), parts, 0.0)
        packed = jnp.sum(packed, axis=1, keepdims=True)
        out_ref[at, 32:40, :] = jnp.broadcast_to(packed, (8, 8, 128)).astype(bf16)


def weights_body(w_hbm, w_out, sems):
    share = w_hbm.shape[0] // 8
    copies = [
        pltpu.make_async_copy(
            w_hbm.at[pl.ds(share * i, share)], w_out.at[pl.ds(share * i, share)], sems.at[i]
        )
        for i in range(8)
    ]
    for c in copies:
        c.start()
    for c in copies:
        c.wait()


def blend(outs, lses):
    peak = lses[0]
    for v in lses[1:]:
        peak = jnp.maximum(peak, v)
    weights = [jnp.exp2(v - peak) for v in lses]
    total = weights[0]
    for w in weights[1:]:
        total = total + w
    mixed = outs[0] * weights[0]
    for o, w in zip(outs[1:], weights[1:]):
        mixed = mixed + o * w
    return mixed / total


def fill_body(where_ref, len_ref, img_ref, p0_ref, p1_ref, p2_ref, p3_ref, out_ref):
    row = lax.broadcasted_iota(jnp.int32, (64, 128), 0)
    lane = lax.broadcasted_iota(jnp.int32, (64, 128), 1)
    outs, lses = [], []
    for ref in (p0_ref, p1_ref, p2_ref, p3_ref):
        outs.append(ref[0:64, :].astype(f32))
        stats = ref[64:80, :].astype(f32)
        picked = jnp.where(row == lane % 64, stats[0:1], 0.0) + jnp.where(row == lane, stats[8:9], 0.0)
        lses.append(jnp.sum(picked, axis=1, keepdims=True))
    text = blend(outs, lses)
    text = jnp.where(where_ref[0] * 64 + row < len_ref[0], text, 0.0).astype(bf16)
    for s in range(4):
        for i in range(8):
            d = 4 * i + (where_ref[0] ^ s)
            out_ref[d, 0:32, :] = img_ref[8 * s + i, 0:32]
            out_ref[d, 32:96, :] = text
            out_ref[d, 96:104, :] = img_ref[8 * s + i, 32:40]


def tail_body(core_ref, recv_ref, w_ref, mine_ref, other_ref, txt_out, txt_ref, sem):
    row = lax.broadcasted_iota(jnp.int32, (32, 128), 0)
    lane = lax.broadcasted_iota(jnp.int32, (32, 128), 1)
    pick = jnp.logical_and(row == lane % 32, lane < 96)
    heads = []
    for head in range(8):
        outs, lses = [], []
        for j in range(4):
            s = head * 4 + j
            outs.append(recv_ref[s, 0:32, :].astype(f32))
            stats = recv_ref[s, 96:104, :].astype(f32)[0:1]
            lses.append(jnp.sum(jnp.where(pick, stats, 0.0), axis=1, keepdims=True))
            txt_ref[64 * j : 64 * j + 64, head * HD : (head + 1) * HD] = recv_ref[s, 32:96, :]
        heads.append(blend(outs, lses))
    leave = pltpu.make_async_copy(txt_ref, txt_out, sem)
    leave.start()
    rows = jnp.concatenate(heads, axis=1)
    flipped = jnp.concatenate([rows[16:32], rows[0:16]], axis=0)
    rows = jnp.where(core_ref[0] == 0, rows, flipped).astype(bf16)
    projected = jnp.dot(rows, w_ref[...], preferred_element_type=f32)
    mine_ref[...] = projected[0:16]
    other_ref[...] = projected[16:32].astype(bf16)
    leave.wait()


def shards(
    img_qkv, txt_qkv, frame_index, row_index, column_index, txt_len, residual, w_proj, proj_bias, gate
):
    tokens = img_qkv.shape[1]
    width = img_qkv.shape[3]
    d_model = w_proj.shape[1]
    j = lax.axis_index("y").astype(jnp.int32).reshape(1)
    head = lax.axis_index("zl") * 4 + lax.axis_index("x")
    core = lax.axis_index("tp").astype(jnp.int32).reshape(1)
    j, core, head, frame_index = lax.optimization_barrier((j, core, head, frame_index))
    qkv = img_qkv.reshape(tokens, 3, width).transpose(1, 0, 2)
    txt = lax.dynamic_slice_in_dim(txt_qkv[0], head * HD, HD, 2).transpose(1, 0, 2)

    send = call(
        prep_body,
        jax.ShapeDtypeStruct((8, 96, HD), bf16),
        5, hbm=(0, 1, 2, 3, 4),
        scratch=(
            pltpu.VMEM((3, tokens, width), bf16),
            pltpu.VMEM((1, tokens), jnp.int32),
            pltpu.VMEM((1, tokens), jnp.int32),
            pltpu.VMEM((1, tokens), jnp.int32),
            pltpu.VMEM((8, HD), f32),
            pltpu.SemaphoreType.DMA((5,)),
        ),
    )(qkv, frame_index, row_index, column_index, jnp.asarray(rate_table()))
    recv = lax.all_to_all(send, HEAD, 0, 0, tiled=True)
    kv = recv[:, 32:96]
    q = recv[:, 0:32]
    others = {}
    for s in (3, 2, 1):
        others[s] = lax.ppermute(kv, "zh", [(i, i ^ s) for i in range(4)])
    queries = [lax.ppermute(q, "y", [(i, i ^ s) for i in range(4)]) for s in (1, 2, 3)]
    w_near = call(
        weights_body, pltpu.VMEM(w_proj.shape, bf16), 1, hbm=(0,),
        scratch=(pltpu.SemaphoreType.DMA((8,)),),
    )(w_proj)
    piece = jax.ShapeDtypeStruct((80, HD), bf16)
    got = {}
    acc, stat = call(
        early_body,
        [jax.ShapeDtypeStruct((256, HD), f32), jax.ShapeDtypeStruct((2, 256, 128), f32)],
        5, smem=(0, 1),
    )(j, txt_len, recv, others[3], txt)
    pieces = call(text_body, [piece] * 4, 6, smem=(0,))(j, others[2], others[1], txt, acc, stat)
    for s in (2, 3, 1):
        got[s] = lax.ppermute(pieces[s], "y", [(i, i ^ s) for i in range(4)])
    img = call(
        image_body, jax.ShapeDtypeStruct((32, 40, HD), bf16), 10, smem=(0, 1),
        scratch=(pltpu.VMEM((1152, HD), bf16), pltpu.VMEM((1152, HD), bf16)),
    )(j, txt_len, recv, others[1], others[2], others[3], *queries, txt)
    back = call(fill_body, jax.ShapeDtypeStruct((32, 104, HD), bf16), 7, smem=(0, 1))(
        j, txt_len, img, pieces[0], got[1], got[2], got[3]
    )
    home = lax.all_to_all(back, CUBE, 0, 0, tiled=True)
    half = tokens // 2
    mine, other, txt_out = call(
        tail_body,
        [
            jax.ShapeDtypeStruct((half, d_model), f32),
            jax.ShapeDtypeStruct((half, d_model), bf16),
            pltpu.HBM((256, width), bf16),
        ],
        3, smem=(0,), near=(2,), far_outs=(2,),
        scratch=(pltpu.VMEM((256, width), bf16), pltpu.SemaphoreType.DMA),
    )(core, home, w_near)
    theirs = lax.ppermute(other, "tp", [(0, 1), (1, 0)])
    projected = mine + theirs.astype(f32)
    img_out = residual[0].astype(f32) + gate[None, :] * (projected + proj_bias[None, :])
    return img_out.astype(bf16)[None], txt_out[None]


def solution(mesh):
    split = Mesh(
        mesh.devices.reshape(4, 2, 4, 4, mesh.shape["tp"]), ("zh", "zl", "x", "y", "tp")
    )
    placed = (
        P(None, SEQ, None, "tp"),
        P(None, None, None, "tp"),
        P(None, SEQ),
        P(None, SEQ),
        P(None, SEQ),
        P(),
        P(None, SEQ + ("tp",), None),
        P("tp", None),
        P(),
        P(),
    )
    return jax.shard_map(
        shards,
        mesh=split,
        in_specs=placed,
        out_specs=(P(None, SEQ + ("tp",), None), P(None, None, "tp")),
        check_vma=False,
    )
```

```python
import math

import jax
import jax.numpy as jnp
import numpy as np
from jax import lax
from jax.experimental import pallas as pl
from jax.experimental.pallas import tpu as pltpu
from jax.sharding import Mesh
from jax.sharding import PartitionSpec as P


HD = 128
SEQ = ("zh", "zl", "x", "y")
CUBE = ("zl", "x", "y")
HEAD = ("zl", "x")
rope_base = 256.0
neg_large = -1e30
LOG2E = 1.4426950408889634
bf16 = jnp.bfloat16
f32 = jnp.float32


def vmem_spec():
    return pl.BlockSpec(memory_space=pltpu.VMEM)


def smem_spec():
    return pl.BlockSpec(memory_space=pltpu.SMEM)


def any_spec():
    return pl.BlockSpec(memory_space=pltpu.HBM)


def call(
    body, out_shape, n_in, smem=(), hbm=(), near=(), far_outs=(), limit=40 * 1024 * 1024, scratch=(), alias=None
):
    single = not isinstance(out_shape, (tuple, list))
    outs = out_shape if not single else [out_shape]
    specs = [any_spec() if i in far_outs else vmem_spec() for i in range(len(outs))]
    kernel = pl.pallas_call(
        body,
        out_shape=out_shape,
        in_specs=[
            smem_spec() if i in smem else any_spec() if i in hbm else vmem_spec() for i in range(n_in)
        ],
        out_specs=specs[0] if single else specs,
        scratch_shapes=list(scratch),
        input_output_aliases=alias or {},
        compiler_params=pltpu.CompilerParams(vmem_limit_bytes=limit),
    )

    def run(*operands):
        held = [
            pltpu.with_memory_space_constraint(v, pltpu.HBM if i in hbm else pltpu.VMEM)
            if i in hbm or i in near
            else v
            for i, v in enumerate(operands)
        ]
        return kernel(*held)

    return run


def rate_table():
    table = np.zeros((8, HD), np.float32)
    frame_part = HD // 8
    second = (HD - frame_part) // 2
    at = 0
    for p, width in enumerate((frame_part, second, second)):
        ids = np.arange(width // 2, dtype=np.float32)
        rates = np.float32(rope_base) ** (np.float32(-2.0) * ids / np.float32(width))
        table[p, at : at + width] = np.repeat(rates.astype(np.float32), 2)
        at += width
    return table


def prep_body(
    qkv_hbm, frame_hbm, row_hbm, col_hbm, rate_hbm, out_ref,
    qkv_ref, frame_ref, row_ref, col_ref, rate_ref, sems,
):
    copies = [
        pltpu.make_async_copy(src, dst, sems.at[i])
        for i, (src, dst) in enumerate(
            (
                (frame_hbm, frame_ref), (row_hbm, row_ref), (col_hbm, col_ref),
                (rate_hbm, rate_ref), (qkv_hbm, qkv_ref),
            )
        )
    ]
    for c in copies:
        c.start()
    for c in copies[:4]:
        c.wait()
    tokens = qkv_ref.shape[1]
    sub = lax.broadcasted_iota(jnp.int32, (8, tokens), 0)
    pos = jnp.where(
        sub == 0, frame_ref[...], jnp.where(sub == 1, row_ref[...], jnp.where(sub == 2, col_ref[...], 0))
    ).astype(f32)
    angles = lax.dot_general(
        pos, rate_ref[...], (((0,), (0,)), ((), ())), precision=lax.Precision.HIGHEST,
        preferred_element_type=f32,
    )
    lane = lax.broadcasted_iota(jnp.int32, (tokens, HD), 1)
    even = (lane % 2) == 0
    cosine = jnp.cos(angles)
    sine = jnp.sin(angles)
    sine = jnp.where(even, -sine, sine)
    copies[4].wait()

    def rotate(v):
        v = v.astype(f32)
        partner = jnp.where(even, pltpu.roll(v, HD - 1, 1), pltpu.roll(v, 1, 1))
        return (v * cosine + partner * sine).astype(bf16)

    for head in range(8):
        cols = slice(head * HD, (head + 1) * HD)
        out_ref[head, 0:32, :] = rotate(qkv_ref[0, :, cols])
        out_ref[head, 32:64, :] = rotate(qkv_ref[1, :, cols])
        out_ref[head, 64:96, :] = qkv_ref[2, :, cols]


def softmax_block(q, keys, values, live):
    scale = LOG2E / math.sqrt(HD)
    scores = lax.dot_general(q, keys, (((1,), (1,)), ((), ())), preferred_element_type=f32)
    n_img = keys.shape[0] - 128
    s_img = scores[:, :n_img]
    s_txt = jnp.where(live, scores[:, n_img:], neg_large)
    peak = jnp.maximum(
        jnp.max(s_img, axis=1, keepdims=True), jnp.max(s_txt, axis=1, keepdims=True)
    )
    w_img = jnp.exp2((s_img - peak) * scale)
    w_txt = jnp.exp2((s_txt - peak) * scale)
    total = jnp.sum(w_img, axis=1, keepdims=True) + jnp.sum(w_txt, axis=1, keepdims=True)
    weights = jnp.concatenate([w_img.astype(bf16), w_txt.astype(bf16)], axis=1)
    out = jnp.dot(weights, values, preferred_element_type=f32)
    return out / total, peak * scale + jnp.log2(total)


def three_parts(v):
    high = v.astype(bf16).astype(f32)
    rest = v - high
    mid = rest.astype(bf16).astype(f32)
    return high, mid, rest - mid


def live_mask(j, length):
    lane = lax.broadcasted_iota(jnp.int32, (1, 128), 1)
    index = lane + (j // 2) * 128
    return jnp.logical_and(index // 64 == j, index < length)


SCALE = LOG2E / math.sqrt(HD)


def text_queries(txt_ref, j):
    return jnp.concatenate(
        [txt_ref[0, pl.ds(pl.multiple_of((j ^ s) * 64, 64), 64), :] for s in range(4)], axis=0
    )


def early_body(where_ref, len_ref, recv_ref, kv_ref, txt_ref, acc_ref, stat_ref):
    j = where_ref[0]
    start = pl.multiple_of((j // 2) * 128, 128)
    keys = jnp.concatenate(
        [
            recv_ref[:, 32:64, :].reshape(256, HD), kv_ref[:, 0:32, :].reshape(256, HD),
            txt_ref[1, pl.ds(start, 128), :],
        ],
        axis=0,
    )
    values = jnp.concatenate(
        [
            recv_ref[:, 64:96, :].reshape(256, HD), kv_ref[:, 32:64, :].reshape(256, HD),
            txt_ref[2, pl.ds(start, 128), :],
        ],
        axis=0,
    )
    q = text_queries(txt_ref, j)
    scores = lax.dot_general(q, keys, (((1,), (1,)), ((), ())), preferred_element_type=f32)
    s_txt = jnp.where(live_mask(j, len_ref[0]), scores[:, 512:], neg_large)
    peak = jnp.maximum(
        jnp.max(scores[:, :512], axis=1, keepdims=True), jnp.max(s_txt, axis=1, keepdims=True)
    )
    w_img = jnp.exp2((scores[:, :512] - peak) * SCALE)
    w_txt = jnp.exp2((s_txt - peak) * SCALE)
    total = jnp.sum(w_img, axis=1, keepdims=True) + jnp.sum(w_txt, axis=1, keepdims=True)
    weights = jnp.concatenate([w_img.astype(bf16), w_txt.astype(bf16)], axis=1)
    acc_ref[...] = jnp.dot(weights, values, preferred_element_type=f32)
    stat_ref[0] = jnp.broadcast_to(peak, (256, 128))
    stat_ref[1] = jnp.broadcast_to(total, (256, 128))


def text_body(
    where_ref, kv0_ref, kv1_ref, txt_ref, acc_ref, stat_ref, p0_ref, p1_ref, p2_ref, p3_ref
):
    keys = jnp.concatenate([r[:, 0:32, :].reshape(256, HD) for r in (kv0_ref, kv1_ref)], axis=0)
    values = jnp.concatenate([r[:, 32:64, :].reshape(256, HD) for r in (kv0_ref, kv1_ref)], axis=0)
    q = text_queries(txt_ref, where_ref[0])
    scores = lax.dot_general(q, keys, (((1,), (1,)), ((), ())), preferred_element_type=f32)
    before = stat_ref[0][:, 0:1]
    peak = jnp.maximum(before, jnp.max(scores, axis=1, keepdims=True))
    shrink = jnp.exp2((before - peak) * SCALE)
    weights = jnp.exp2((scores - peak) * SCALE)
    total = stat_ref[1][:, 0:1] * shrink + jnp.sum(weights, axis=1, keepdims=True)
    out = acc_ref[...] * shrink + jnp.dot(weights.astype(bf16), values, preferred_element_type=f32)
    out = out / total
    lse = peak * SCALE + jnp.log2(total)
    out = out.astype(bf16)
    row = lax.broadcasted_iota(jnp.int32, (64, 128), 0)
    lane = lax.broadcasted_iota(jnp.int32, (64, 128), 1)
    for s, ref in enumerate((p0_ref, p1_ref, p2_ref, p3_ref)):
        ref[0:64, :] = out[64 * s : 64 * s + 64]
        high, mid, low = three_parts(jnp.broadcast_to(lse[64 * s : 64 * s + 64], (64, 128)))
        first = jnp.where(row == lane % 64, jnp.where(lane < 64, high, mid), 0.0)
        second = jnp.where(row == lane, low, 0.0)
        first = jnp.broadcast_to(jnp.sum(first, axis=0, keepdims=True), (8, 128))
        second = jnp.broadcast_to(jnp.sum(second, axis=0, keepdims=True), (8, 128))
        ref[64:80, :] = jnp.concatenate([first, second], axis=0).astype(bf16)


def image_body(
    where_ref, len_ref, recv_ref, kv1_ref, kv2_ref, kv3_ref, q1_ref, q2_ref, q3_ref, txt_ref, w_hbm,
    out_ref, w_out, keys_ref, values_ref, sems,
):
    share = w_hbm.shape[0] // 8
    fetches = [
        pltpu.make_async_copy(
            w_hbm.at[pl.ds(share * i, share)], w_out.at[pl.ds(share * i, share)], sems.at[i]
        )
        for i in range(8)
    ]
    for c in fetches:
        c.start()
    j = where_ref[0]
    keys_ref[0:256, :] = recv_ref[:, 32:64, :].reshape(256, HD)
    values_ref[0:256, :] = recv_ref[:, 64:96, :].reshape(256, HD)
    for b, ref in ((1, kv1_ref), (2, kv2_ref), (3, kv3_ref)):
        keys_ref[256 * b : 256 * b + 256, :] = ref[:, 0:32, :].reshape(256, HD)
        values_ref[256 * b : 256 * b + 256, :] = ref[:, 32:64, :].reshape(256, HD)
    start = pl.multiple_of((j // 2) * 128, 128)
    keys_ref[1024:1152, :] = txt_ref[1, pl.ds(start, 128), :]
    values_ref[1024:1152, :] = txt_ref[2, pl.ds(start, 128), :]
    live = live_mask(j, len_ref[0])
    keys = keys_ref[...]
    values = values_ref[...]
    row = lax.broadcasted_iota(jnp.int32, (8, 32, 128), 1)
    lane = lax.broadcasted_iota(jnp.int32, (8, 32, 128), 2)
    for s in range(4):
        q = recv_ref[:, 0:32, :] if s == 0 else (q1_ref, q2_ref, q3_ref)[s - 1][...]
        out, lse = softmax_block(q.reshape(256, HD), keys, values, live)
        at = slice(8 * s, 8 * s + 8)
        out_ref[at, 0:32, :] = out.astype(bf16).reshape(8, 32, HD)
        high, mid, low = three_parts(jnp.broadcast_to(lse, (256, 128)).reshape(8, 32, 128))
        parts = jnp.where(lane < 32, high, jnp.where(lane < 64, mid, low))
        packed = jnp.where(jnp.logical_and(row == lane % 32, lane < 96), parts, 0.0)
        packed = jnp.sum(packed, axis=1, keepdims=True)
        out_ref[at, 32:40, :] = jnp.broadcast_to(packed, (8, 8, 128)).astype(bf16)
    for c in fetches:
        c.wait()


def blend(outs, lses):
    peak = lses[0]
    for v in lses[1:]:
        peak = jnp.maximum(peak, v)
    weights = [jnp.exp2(v - peak) for v in lses]
    total = weights[0]
    for w in weights[1:]:
        total = total + w
    mixed = outs[0] * weights[0]
    for o, w in zip(outs[1:], weights[1:]):
        mixed = mixed + o * w
    return mixed / total


def fill_body(where_ref, len_ref, img_ref, p0_ref, p1_ref, p2_ref, p3_ref, out_ref):
    row = lax.broadcasted_iota(jnp.int32, (64, 128), 0)
    lane = lax.broadcasted_iota(jnp.int32, (64, 128), 1)
    outs, lses = [], []
    for ref in (p0_ref, p1_ref, p2_ref, p3_ref):
        outs.append(ref[0:64, :].astype(f32))
        stats = ref[64:80, :].astype(f32)
        picked = jnp.where(row == lane % 64, stats[0:1], 0.0) + jnp.where(row == lane, stats[8:9], 0.0)
        lses.append(jnp.sum(picked, axis=1, keepdims=True))
    text = blend(outs, lses)
    text = jnp.where(where_ref[0] * 64 + row < len_ref[0], text, 0.0).astype(bf16)
    for s in range(4):
        for i in range(8):
            d = 4 * i + (where_ref[0] ^ s)
            out_ref[d, 0:32, :] = img_ref[8 * s + i, 0:32]
            out_ref[d, 32:96, :] = text
            out_ref[d, 96:104, :] = img_ref[8 * s + i, 32:40]


def tail_body(core_ref, recv_ref, w_ref, mine_ref, other_ref, txt_out, txt_ref, sem):
    row = lax.broadcasted_iota(jnp.int32, (32, 128), 0)
    lane = lax.broadcasted_iota(jnp.int32, (32, 128), 1)
    pick = jnp.logical_and(row == lane % 32, lane < 96)
    for head in range(8):
        for j in range(4):
            txt_ref[64 * j : 64 * j + 64, head * HD : (head + 1) * HD] = recv_ref[head * 4 + j, 32:96, :]
    leave = pltpu.make_async_copy(txt_ref, txt_out, sem)
    leave.start()
    projected = None
    for pair in range(4):
        heads = []
        for head in (2 * pair, 2 * pair + 1):
            outs, lses = [], []
            for j in range(4):
                s = head * 4 + j
                outs.append(recv_ref[s, 0:32, :].astype(f32))
                stats = recv_ref[s, 96:104, :].astype(f32)[0:1]
                lses.append(jnp.sum(jnp.where(pick, stats, 0.0), axis=1, keepdims=True))
            heads.append(blend(outs, lses))
        rows = jnp.concatenate(heads, axis=1)
        flipped = jnp.concatenate([rows[16:32], rows[0:16]], axis=0)
        rows = jnp.where(core_ref[0] == 0, rows, flipped).astype(bf16)
        part = jnp.dot(
            rows, w_ref[256 * pair : 256 * pair + 256, :], preferred_element_type=f32
        )
        projected = part if projected is None else projected + part
    mine_ref[...] = projected[0:16]
    other_ref[...] = projected[16:32].astype(bf16)
    leave.wait()


def shards(
    img_qkv, txt_qkv, frame_index, row_index, column_index, txt_len, residual, w_proj, proj_bias, gate
):
    tokens = img_qkv.shape[1]
    width = img_qkv.shape[3]
    d_model = w_proj.shape[1]
    j = lax.axis_index("y").astype(jnp.int32).reshape(1)
    head = lax.axis_index("zl") * 4 + lax.axis_index("x")
    core = lax.axis_index("tp").astype(jnp.int32).reshape(1)
    j, core, head, frame_index = lax.optimization_barrier((j, core, head, frame_index))
    qkv = img_qkv.reshape(tokens, 3, width).transpose(1, 0, 2)
    txt = lax.dynamic_slice_in_dim(txt_qkv[0], head * HD, HD, 2).transpose(1, 0, 2)

    send = call(
        prep_body,
        jax.ShapeDtypeStruct((8, 96, HD), bf16),
        5, hbm=(0, 1, 2, 3, 4),
        scratch=(
            pltpu.VMEM((3, tokens, width), bf16),
            pltpu.VMEM((1, tokens), jnp.int32),
            pltpu.VMEM((1, tokens), jnp.int32),
            pltpu.VMEM((1, tokens), jnp.int32),
            pltpu.VMEM((8, HD), f32),
            pltpu.SemaphoreType.DMA((5,)),
        ),
    )(qkv, frame_index, row_index, column_index, jnp.asarray(rate_table()))
    recv = lax.all_to_all(send, HEAD, 0, 0, tiled=True)
    kv = recv[:, 32:96]
    q = recv[:, 0:32]
    others = {}
    for s in (2, 3, 1):
        others[s] = lax.ppermute(kv, "zh", [(i, i ^ s) for i in range(4)])
    queries = [lax.ppermute(q, "y", [(i, i ^ s) for i in range(4)]) for s in (1, 2, 3)]

    piece = jax.ShapeDtypeStruct((80, HD), bf16)
    got = {}
    acc, stat = call(
        early_body,
        [jax.ShapeDtypeStruct((256, HD), f32), jax.ShapeDtypeStruct((2, 256, 128), f32)],
        5, smem=(0, 1),
    )(j, txt_len, recv, others[2], txt)
    pieces = call(text_body, [piece] * 4, 6, smem=(0,))(j, others[3], others[1], txt, acc, stat)
    for s in (2, 3, 1):
        got[s] = lax.ppermute(pieces[s], "y", [(i, i ^ s) for i in range(4)])
    img, w_near = call(
        image_body,
        [jax.ShapeDtypeStruct((32, 40, HD), bf16), pltpu.VMEM(w_proj.shape, bf16)],
        11, smem=(0, 1), hbm=(10,),
        scratch=(
            pltpu.VMEM((1152, HD), bf16), pltpu.VMEM((1152, HD), bf16), pltpu.SemaphoreType.DMA((8,)),
        ),
    )(j, txt_len, recv, others[1], others[2], others[3], *queries, txt, w_proj)
    back = call(fill_body, jax.ShapeDtypeStruct((32, 104, HD), bf16), 7, smem=(0, 1))(
        j, txt_len, img, pieces[0], got[1], got[2], got[3]
    )
    home = lax.all_to_all(back, CUBE, 0, 0, tiled=True)
    half = tokens // 2
    mine, other, txt_out = call(
        tail_body,
        [
            jax.ShapeDtypeStruct((half, d_model), f32),
            jax.ShapeDtypeStruct((half, d_model), bf16),
            pltpu.HBM((256, width), bf16),
        ],
        3, smem=(0,), near=(2,), far_outs=(2,),
        scratch=(pltpu.VMEM((256, width), bf16), pltpu.SemaphoreType.DMA),
    )(core, home, w_near)
    theirs = lax.ppermute(other, "tp", [(0, 1), (1, 0)])
    projected = mine + theirs.astype(f32)
    img_out = residual[0].astype(f32) + gate[None, :] * (projected + proj_bias[None, :])
    return img_out.astype(bf16)[None], txt_out[None]


def solution(mesh):
    split = Mesh(
        mesh.devices.reshape(4, 2, 4, 4, mesh.shape["tp"]), ("zh", "zl", "x", "y", "tp")
    )
    placed = (
        P(None, SEQ, None, "tp"),
        P(None, None, None, "tp"),
        P(None, SEQ),
        P(None, SEQ),
        P(None, SEQ),
        P(),
        P(None, SEQ + ("tp",), None),
        P("tp", None),
        P(),
        P(),
    )
    return jax.shard_map(
        shards,
        mesh=split,
        in_specs=placed,
        out_specs=(P(None, SEQ + ("tp",), None), P(None, None, "tp")),
        check_vma=False,
    )
```

```python
import math

import jax
import jax.numpy as jnp
import numpy as np
from jax import lax
from jax.experimental import pallas as pl
from jax.experimental.pallas import tpu as pltpu
from jax.sharding import Mesh
from jax.sharding import PartitionSpec as P


HD = 128
SEQ = ("zh", "zl", "x", "y")
HEAD = ("zl", "x")
rope_base = 256.0
neg_large = -1e30
LOG2E = 1.4426950408889634
bf16 = jnp.bfloat16
f32 = jnp.float32


def vmem_spec():
    return pl.BlockSpec(memory_space=pltpu.VMEM)


def smem_spec():
    return pl.BlockSpec(memory_space=pltpu.SMEM)


def any_spec():
    return pl.BlockSpec(memory_space=pltpu.HBM)


def call(
    body, out_shape, n_in, smem=(), hbm=(), near=(), far_outs=(), limit=40 * 1024 * 1024, scratch=(), alias=None
):
    single = not isinstance(out_shape, (tuple, list))
    outs = out_shape if not single else [out_shape]
    specs = [any_spec() if i in far_outs else vmem_spec() for i in range(len(outs))]
    kernel = pl.pallas_call(
        body,
        out_shape=out_shape,
        in_specs=[
            smem_spec() if i in smem else any_spec() if i in hbm else vmem_spec() for i in range(n_in)
        ],
        out_specs=specs[0] if single else specs,
        scratch_shapes=list(scratch),
        input_output_aliases=alias or {},
        compiler_params=pltpu.CompilerParams(vmem_limit_bytes=limit),
    )

    def run(*operands):
        held = [
            pltpu.with_memory_space_constraint(v, pltpu.HBM if i in hbm else pltpu.VMEM)
            if i in hbm or i in near
            else v
            for i, v in enumerate(operands)
        ]
        return kernel(*held)

    return run


def rate_table():
    table = np.zeros((8, HD), np.float32)
    frame_part = HD // 8
    second = (HD - frame_part) // 2
    at = 0
    for p, width in enumerate((frame_part, second, second)):
        ids = np.arange(width // 2, dtype=np.float32)
        rates = np.float32(rope_base) ** (np.float32(-2.0) * ids / np.float32(width))
        table[p, at : at + width] = np.repeat(rates.astype(np.float32), 2)
        at += width
    return table


def prep_body(
    qkv_hbm, frame_hbm, row_hbm, col_hbm, rate_hbm, out_ref,
    qkv_ref, frame_ref, row_ref, col_ref, rate_ref, sems,
):
    copies = [
        pltpu.make_async_copy(src, dst, sems.at[i])
        for i, (src, dst) in enumerate(
            (
                (frame_hbm, frame_ref), (row_hbm, row_ref), (col_hbm, col_ref),
                (rate_hbm, rate_ref), (qkv_hbm, qkv_ref),
            )
        )
    ]
    for c in copies:
        c.start()
    for c in copies[:4]:
        c.wait()
    tokens = qkv_ref.shape[1]
    sub = lax.broadcasted_iota(jnp.int32, (8, tokens), 0)
    pos = jnp.where(
        sub == 0, frame_ref[...], jnp.where(sub == 1, row_ref[...], jnp.where(sub == 2, col_ref[...], 0))
    ).astype(f32)
    angles = lax.dot_general(
        pos, rate_ref[...], (((0,), (0,)), ((), ())), precision=lax.Precision.HIGHEST,
        preferred_element_type=f32,
    )
    lane = lax.broadcasted_iota(jnp.int32, (tokens, HD), 1)
    even = (lane % 2) == 0
    cosine = jnp.cos(angles)
    sine = jnp.sin(angles)
    sine = jnp.where(even, -sine, sine)
    copies[4].wait()

    def rotate(v):
        v = v.astype(f32)
        partner = jnp.where(even, pltpu.roll(v, HD - 1, 1), pltpu.roll(v, 1, 1))
        return (v * cosine + partner * sine).astype(bf16)

    for head in range(8):
        cols = slice(head * HD, (head + 1) * HD)
        out_ref[head, 0:32, :] = rotate(qkv_ref[0, :, cols])
        out_ref[head, 32:64, :] = rotate(qkv_ref[1, :, cols])
        out_ref[head, 64:96, :] = qkv_ref[2, :, cols]


def three_parts(v):
    high = v.astype(bf16).astype(f32)
    rest = v - high
    mid = rest.astype(bf16).astype(f32)
    return high, mid, rest - mid


def live_mask(j, length):
    lane = lax.broadcasted_iota(jnp.int32, (1, 128), 1)
    index = lane + (j // 2) * 128
    return jnp.logical_and(index // 64 == j, index < length)


SCALE = LOG2E / math.sqrt(HD)


def stat_rows(lse):
    row = lax.broadcasted_iota(jnp.int32, (128, 128), 0)
    lane = lax.broadcasted_iota(jnp.int32, (128, 128), 1)
    sub = lax.broadcasted_iota(jnp.int32, (8, 128), 0)
    packed = jnp.zeros((8, 128), f32)
    for half in range(2):
        column = jnp.broadcast_to(lse[128 * half : 128 * half + 128], (128, 128))
        for p, part in enumerate(three_parts(column)):
            line = jnp.sum(jnp.where(row == lane, part, 0.0), axis=0, keepdims=True)
            packed = jnp.where(sub == 2 * p + half, line, packed)
    return packed.astype(bf16)


def stat_column(packed):
    packed = packed.astype(f32)
    row = lax.broadcasted_iota(jnp.int32, (128, 128), 0)
    lane = lax.broadcasted_iota(jnp.int32, (128, 128), 1)
    halves = []
    for half in range(2):
        line = packed[half : half + 1] + packed[2 + half : 3 + half] + packed[4 + half : 5 + half]
        halves.append(jnp.sum(jnp.where(row == lane, line, 0.0), axis=1, keepdims=True))
    return jnp.concatenate(halves, axis=0)


def query_block(b, recv_ref, q_refs, txt_ref):
    if b == 4:
        return txt_ref[0]
    q = recv_ref[:, 0:32, :] if b == 0 else q_refs[b - 1][...]
    return q.reshape(256, HD)


def early_body(
    where_ref, len_ref, recv_ref, kv_ref, q1_ref, q2_ref, q3_ref, txt_ref, acc_ref, stat_ref
):
    j = where_ref[0]
    start = pl.multiple_of((j // 2) * 128, 128)
    keys = jnp.concatenate(
        [
            recv_ref[:, 32:64, :].reshape(256, HD), kv_ref[:, 0:32, :].reshape(256, HD),
            txt_ref[1, pl.ds(start, 128), :],
        ],
        axis=0,
    )
    values = jnp.concatenate(
        [
            recv_ref[:, 64:96, :].reshape(256, HD), kv_ref[:, 32:64, :].reshape(256, HD),
            txt_ref[2, pl.ds(start, 128), :],
        ],
        axis=0,
    )
    live = live_mask(j, len_ref[0])
    for b in range(5):
        q = query_block(b, recv_ref, (q1_ref, q2_ref, q3_ref), txt_ref)
        scores = lax.dot_general(q, keys, (((1,), (1,)), ((), ())), preferred_element_type=f32)
        s_txt = jnp.where(live, scores[:, 512:], neg_large)
        peak = jnp.maximum(
            jnp.max(scores[:, :512], axis=1, keepdims=True), jnp.max(s_txt, axis=1, keepdims=True)
        )
        w_img = jnp.exp2((scores[:, :512] - peak) * SCALE)
        w_txt = jnp.exp2((s_txt - peak) * SCALE)
        total = jnp.sum(w_img, axis=1, keepdims=True) + jnp.sum(w_txt, axis=1, keepdims=True)
        weights = jnp.concatenate([w_img.astype(bf16), w_txt.astype(bf16)], axis=1)
        at = slice(256 * b, 256 * b + 256)
        acc_ref[at, :] = jnp.dot(weights, values, preferred_element_type=f32)
        stat_ref[0, at, :] = jnp.broadcast_to(peak, (256, 128))
        stat_ref[1, at, :] = jnp.broadcast_to(total, (256, 128))


def late_body(
    recv_ref, kv0_ref, kv1_ref, q1_ref, q2_ref, q3_ref, txt_ref, acc_ref, stat_ref,
    m1_ref, m2_ref, m3_ref, keep_ref,
):
    keys = jnp.concatenate([r[:, 0:32, :].reshape(256, HD) for r in (kv0_ref, kv1_ref)], axis=0)
    values = jnp.concatenate([r[:, 32:64, :].reshape(256, HD) for r in (kv0_ref, kv1_ref)], axis=0)
    messages = (m1_ref, m2_ref, m3_ref)
    for b in range(5):
        q = query_block(b, recv_ref, (q1_ref, q2_ref, q3_ref), txt_ref)
        at = slice(256 * b, 256 * b + 256)
        scores = lax.dot_general(q, keys, (((1,), (1,)), ((), ())), preferred_element_type=f32)
        before = stat_ref[0, at, 0:1]
        peak = jnp.maximum(before, jnp.max(scores, axis=1, keepdims=True))
        shrink = jnp.exp2((before - peak) * SCALE)
        weights = jnp.exp2((scores - peak) * SCALE)
        total = stat_ref[1, at, 0:1] * shrink + jnp.sum(weights, axis=1, keepdims=True)
        out = acc_ref[at, :] * shrink + jnp.dot(
            weights.astype(bf16), values, preferred_element_type=f32
        )
        out = out / total
        lse = peak * SCALE + jnp.log2(total)
        if b in (0, 4):
            rows = slice(0, 256) if b == 0 else slice(256, 512)
            keep_ref[0, rows, :] = out
            keep_ref[1, rows, :] = jnp.broadcast_to(lse, (256, 128))
        if b in (1, 2, 3):
            messages[b - 1][0:256, :] = out.astype(bf16)
            messages[b - 1][512:520, :] = stat_rows(lse)
        if b == 4:
            stats = stat_rows(lse)
            for m in messages:
                m[256:512, :] = out.astype(bf16)
                m[520:528, :] = stats


def weights_body(w_hbm, w_out, sems):
    share = w_hbm.shape[0] // 8
    copies = [
        pltpu.make_async_copy(
            w_hbm.at[pl.ds(share * i, share)], w_out.at[pl.ds(share * i, share)], sems.at[i]
        )
        for i in range(8)
    ]
    for c in copies:
        c.start()
    for c in copies:
        c.wait()


def blend(outs, lses):
    peak = lses[0]
    for v in lses[1:]:
        peak = jnp.maximum(peak, v)
    weights = [jnp.exp2(v - peak) for v in lses]
    total = weights[0]
    for w in weights[1:]:
        total = total + w
    mixed = outs[0] * weights[0]
    for o, w in zip(outs[1:], weights[1:]):
        mixed = mixed + o * w
    return mixed / total


def mix_body(len_ref, keep_ref, g1_ref, g2_ref, g3_ref, out_ref):
    got = (g1_ref, g2_ref, g3_ref)
    for part in range(2):
        rows = slice(256 * part, 256 * part + 256)
        outs = [keep_ref[0, rows, :]] + [g[rows, :].astype(f32) for g in got]
        lses = [keep_ref[1, rows, 0:1]]
        lses += [stat_column(g[512 + 8 * part : 520 + 8 * part, :]) for g in got]
        mixed = blend(outs, lses)
        if part == 0:
            out_ref[:, 0:32, :] = mixed.astype(bf16).reshape(8, 32, HD)
        else:
            row = lax.broadcasted_iota(jnp.int32, (256, 128), 0)
            text = jnp.where(row < len_ref[0], mixed, 0.0).astype(bf16)
            for d in range(8):
                out_ref[d, 32:288, :] = text


def tail_body(core_ref, recv_ref, w_ref, mine_ref, other_ref, txt_out, sems):
    leave = [
        pltpu.make_async_copy(
            recv_ref.at[h, pl.ds(32, 256)], txt_out.at[:, pl.ds(h * HD, HD)], sems.at[h]
        )
        for h in range(8)
    ]
    for c in leave:
        c.start()
    rows = jnp.concatenate([recv_ref[h, 0:32, :] for h in range(8)], axis=1).astype(f32)
    flipped = jnp.concatenate([rows[16:32], rows[0:16]], axis=0)
    rows = jnp.where(core_ref[0] == 0, rows, flipped).astype(bf16)
    projected = jnp.dot(rows, w_ref[...], preferred_element_type=f32)
    mine_ref[...] = projected[0:16]
    other_ref[...] = projected[16:32].astype(bf16)
    for c in leave:
        c.wait()


def shards(
    img_qkv, txt_qkv, frame_index, row_index, column_index, txt_len, residual, w_proj, proj_bias, gate
):
    tokens = img_qkv.shape[1]
    width = img_qkv.shape[3]
    d_model = w_proj.shape[1]
    j = lax.axis_index("y").astype(jnp.int32).reshape(1)
    head = lax.axis_index("zl") * 4 + lax.axis_index("x")
    core = lax.axis_index("tp").astype(jnp.int32).reshape(1)
    j, core, head, frame_index = lax.optimization_barrier((j, core, head, frame_index))
    qkv = img_qkv.reshape(tokens, 3, width).transpose(1, 0, 2)
    txt = lax.dynamic_slice_in_dim(txt_qkv[0], head * HD, HD, 2).transpose(1, 0, 2)

    send = call(
        prep_body,
        jax.ShapeDtypeStruct((8, 96, HD), bf16),
        5, hbm=(0, 1, 2, 3, 4),
        scratch=(
            pltpu.VMEM((3, tokens, width), bf16),
            pltpu.VMEM((1, tokens), jnp.int32),
            pltpu.VMEM((1, tokens), jnp.int32),
            pltpu.VMEM((1, tokens), jnp.int32),
            pltpu.VMEM((8, HD), f32),
            pltpu.SemaphoreType.DMA((5,)),
        ),
    )(qkv, frame_index, row_index, column_index, jnp.asarray(rate_table()))
    recv = lax.all_to_all(send, HEAD, 0, 0, tiled=True)
    kv = recv[:, 32:96]
    q = recv[:, 0:32]
    others = {}
    for s in (2, 3, 1):
        others[s] = lax.ppermute(kv, "zh", [(i, i ^ s) for i in range(4)])
    queries = [lax.ppermute(q, "y", [(i, i ^ s) for i in range(4)]) for s in (1, 2, 3)]
    w_near = call(
        weights_body, pltpu.VMEM(w_proj.shape, bf16), 1, hbm=(0,),
        scratch=(pltpu.SemaphoreType.DMA((8,)),),
    )(w_proj)
    acc, stat = call(
        early_body,
        [jax.ShapeDtypeStruct((1280, HD), f32), jax.ShapeDtypeStruct((2, 1280, 128), f32)],
        8, smem=(0, 1),
    )(j, txt_len, recv, others[2], *queries, txt)
    *messages, keep = call(
        late_body,
        [jax.ShapeDtypeStruct((528, HD), bf16)] * 3 + [jax.ShapeDtypeStruct((2, 512, 128), f32)],
        9,
    )(recv, others[3], others[1], *queries, txt, acc, stat)
    got = {}
    for s in (2, 3, 1):
        got[s] = lax.ppermute(messages[s - 1], "y", [(i, i ^ s) for i in range(4)])
    back = call(mix_body, jax.ShapeDtypeStruct((8, 288, HD), bf16), 5, smem=(0,))(
        txt_len, keep, got[1], got[2], got[3]
    )
    home = lax.all_to_all(back, HEAD, 0, 0, tiled=True)
    half = tokens // 2
    mine, other, txt_out = call(
        tail_body,
        [
            jax.ShapeDtypeStruct((half, d_model), f32),
            jax.ShapeDtypeStruct((half, d_model), bf16),
            pltpu.HBM((256, width), bf16),
        ],
        3, smem=(0,), near=(2,), far_outs=(2,),
        scratch=(pltpu.SemaphoreType.DMA((8,)),),
    )(core, home, w_near)
    theirs = lax.ppermute(other, "tp", [(0, 1), (1, 0)])
    projected = mine + theirs.astype(f32)
    img_out = residual[0].astype(f32) + gate[None, :] * (projected + proj_bias[None, :])
    return img_out.astype(bf16)[None], txt_out[None]


def solution(mesh):
    split = Mesh(
        mesh.devices.reshape(4, 2, 4, 4, mesh.shape["tp"]), ("zh", "zl", "x", "y", "tp")
    )
    placed = (
        P(None, SEQ, None, "tp"),
        P(None, None, None, "tp"),
        P(None, SEQ),
        P(None, SEQ),
        P(None, SEQ),
        P(),
        P(None, SEQ + ("tp",), None),
        P("tp", None),
        P(),
        P(),
    )
    return jax.shard_map(
        shards,
        mesh=split,
        in_specs=placed,
        out_specs=(P(None, SEQ + ("tp",), None), P(None, None, "tp")),
        check_vma=False,
    )
```

```python
import math

import jax
import jax.numpy as jnp
import numpy as np
from jax import lax
from jax.experimental import pallas as pl
from jax.experimental.pallas import tpu as pltpu
from jax.sharding import Mesh
from jax.sharding import PartitionSpec as P


HD = 128
SEQ = ("zh", "zl", "x", "y")
HEAD = ("zl", "x")
rope_base = 256.0
neg_large = -1e30
LOG2E = 1.4426950408889634
bf16 = jnp.bfloat16
f32 = jnp.float32


def vmem_spec():
    return pl.BlockSpec(memory_space=pltpu.VMEM)


def smem_spec():
    return pl.BlockSpec(memory_space=pltpu.SMEM)


def any_spec():
    return pl.BlockSpec(memory_space=pltpu.HBM)


def call(
    body, out_shape, n_in, smem=(), hbm=(), near=(), far_outs=(), limit=40 * 1024 * 1024, scratch=(), alias=None
):
    single = not isinstance(out_shape, (tuple, list))
    outs = out_shape if not single else [out_shape]
    specs = [any_spec() if i in far_outs else vmem_spec() for i in range(len(outs))]
    kernel = pl.pallas_call(
        body,
        out_shape=out_shape,
        in_specs=[
            smem_spec() if i in smem else any_spec() if i in hbm else vmem_spec() for i in range(n_in)
        ],
        out_specs=specs[0] if single else specs,
        scratch_shapes=list(scratch),
        input_output_aliases=alias or {},
        compiler_params=pltpu.CompilerParams(vmem_limit_bytes=limit),
    )

    def run(*operands):
        held = [
            pltpu.with_memory_space_constraint(v, pltpu.HBM if i in hbm else pltpu.VMEM)
            if i in hbm or i in near
            else v
            for i, v in enumerate(operands)
        ]
        return kernel(*held)

    return run


def rate_table():
    table = np.zeros((8, HD), np.float32)
    frame_part = HD // 8
    second = (HD - frame_part) // 2
    at = 0
    for p, width in enumerate((frame_part, second, second)):
        ids = np.arange(width // 2, dtype=np.float32)
        rates = np.float32(rope_base) ** (np.float32(-2.0) * ids / np.float32(width))
        table[p, at : at + width] = np.repeat(rates.astype(np.float32), 2)
        at += width
    return table


def prep_body(
    qkv_hbm, frame_hbm, row_hbm, col_hbm, rate_hbm, out_ref,
    qkv_ref, frame_ref, row_ref, col_ref, rate_ref, sems,
):
    copies = [
        pltpu.make_async_copy(src, dst, sems.at[i])
        for i, (src, dst) in enumerate(
            (
                (frame_hbm, frame_ref), (row_hbm, row_ref), (col_hbm, col_ref),
                (rate_hbm, rate_ref), (qkv_hbm, qkv_ref),
            )
        )
    ]
    for c in copies:
        c.start()
    for c in copies[:4]:
        c.wait()
    tokens = qkv_ref.shape[1]
    sub = lax.broadcasted_iota(jnp.int32, (8, tokens), 0)
    pos = jnp.where(
        sub == 0, frame_ref[...], jnp.where(sub == 1, row_ref[...], jnp.where(sub == 2, col_ref[...], 0))
    ).astype(f32)
    angles = lax.dot_general(
        pos, rate_ref[...], (((0,), (0,)), ((), ())), precision=lax.Precision.HIGHEST,
        preferred_element_type=f32,
    )
    lane = lax.broadcasted_iota(jnp.int32, (tokens, HD), 1)
    even = (lane % 2) == 0
    cosine = jnp.cos(angles)
    sine = jnp.sin(angles)
    sine = jnp.where(even, -sine, sine)
    copies[4].wait()

    def rotate(v):
        v = v.astype(f32)
        partner = jnp.where(even, pltpu.roll(v, HD - 1, 1), pltpu.roll(v, 1, 1))
        return (v * cosine + partner * sine).astype(bf16)

    for head in range(8):
        cols = slice(head * HD, (head + 1) * HD)
        out_ref[head, 0:32, :] = rotate(qkv_ref[0, :, cols])
        out_ref[head, 32:64, :] = rotate(qkv_ref[1, :, cols])
        out_ref[head, 64:96, :] = qkv_ref[2, :, cols]


def three_parts(v):
    high = v.astype(bf16).astype(f32)
    rest = v - high
    mid = rest.astype(bf16).astype(f32)
    return high, mid, rest - mid


def live_mask(j, length):
    lane = lax.broadcasted_iota(jnp.int32, (1, 128), 1)
    index = lane + (j // 2) * 128
    return jnp.logical_and(index // 64 == j, index < length)


SCALE = LOG2E / math.sqrt(HD)


def stat_rows(lse):
    row = lax.broadcasted_iota(jnp.int32, (128, 128), 0)
    lane = lax.broadcasted_iota(jnp.int32, (128, 128), 1)
    sub = lax.broadcasted_iota(jnp.int32, (8, 128), 0)
    packed = jnp.zeros((8, 128), f32)
    for half in range(2):
        column = jnp.broadcast_to(lse[128 * half : 128 * half + 128], (128, 128))
        for p, part in enumerate(three_parts(column)):
            line = jnp.sum(jnp.where(row == lane, part, 0.0), axis=0, keepdims=True)
            packed = jnp.where(sub == 2 * p + half, line, packed)
    return packed.astype(bf16)


def stat_column(packed):
    packed = packed.astype(f32)
    row = lax.broadcasted_iota(jnp.int32, (128, 128), 0)
    lane = lax.broadcasted_iota(jnp.int32, (128, 128), 1)
    halves = []
    for half in range(2):
        line = packed[half : half + 1] + packed[2 + half : 3 + half] + packed[4 + half : 5 + half]
        halves.append(jnp.sum(jnp.where(row == lane, line, 0.0), axis=1, keepdims=True))
    return jnp.concatenate(halves, axis=0)


def query_block(b, recv_ref, q_refs, txt_ref):
    if b == 4:
        return txt_ref[0]
    q = recv_ref[:, 0:32, :] if b == 0 else q_refs[b - 1][...]
    return q.reshape(256, HD)


def early_body(
    where_ref, len_ref, recv_ref, kv_ref, q1_ref, q2_ref, q3_ref, txt_ref, acc_ref, stat_ref
):
    j = where_ref[0]
    start = pl.multiple_of((j // 2) * 128, 128)
    keys = jnp.concatenate(
        [
            recv_ref[:, 32:64, :].reshape(256, HD), kv_ref[:, 0:32, :].reshape(256, HD),
            txt_ref[1, pl.ds(start, 128), :],
        ],
        axis=0,
    )
    values = jnp.concatenate(
        [
            recv_ref[:, 64:96, :].reshape(256, HD), kv_ref[:, 32:64, :].reshape(256, HD),
            txt_ref[2, pl.ds(start, 128), :],
        ],
        axis=0,
    )
    live = live_mask(j, len_ref[0])
    for b in range(5):
        q = query_block(b, recv_ref, (q1_ref, q2_ref, q3_ref), txt_ref)
        scores = lax.dot_general(q, keys, (((1,), (1,)), ((), ())), preferred_element_type=f32)
        s_txt = jnp.where(live, scores[:, 512:], neg_large)
        peak = jnp.maximum(
            jnp.max(scores[:, :512], axis=1, keepdims=True), jnp.max(s_txt, axis=1, keepdims=True)
        )
        w_img = jnp.exp2((scores[:, :512] - peak) * SCALE)
        w_txt = jnp.exp2((s_txt - peak) * SCALE)
        total = jnp.sum(w_img, axis=1, keepdims=True) + jnp.sum(w_txt, axis=1, keepdims=True)
        weights = jnp.concatenate([w_img.astype(bf16), w_txt.astype(bf16)], axis=1)
        at = slice(256 * b, 256 * b + 256)
        acc_ref[at, :] = jnp.dot(weights, values, preferred_element_type=f32)
        stat_ref[0, at, :] = jnp.broadcast_to(peak, (256, 128))
        stat_ref[1, at, :] = jnp.broadcast_to(total, (256, 128))


def late_keys(kv0_ref, kv1_ref):
    both = (kv0_ref, kv1_ref)
    keys = jnp.concatenate([r[:, 0:32, :].reshape(256, HD) for r in both], axis=0)
    values = jnp.concatenate([r[:, 32:64, :].reshape(256, HD) for r in both], axis=0)
    return keys, values


def late_block(b, q, keys, values, acc_ref, stat_ref):
    at = slice(256 * b, 256 * b + 256)
    scores = lax.dot_general(q, keys, (((1,), (1,)), ((), ())), preferred_element_type=f32)
    before = stat_ref[0, at, 0:1]
    peak = jnp.maximum(before, jnp.max(scores, axis=1, keepdims=True))
    shrink = jnp.exp2((before - peak) * SCALE)
    weights = jnp.exp2((scores - peak) * SCALE)
    total = stat_ref[1, at, 0:1] * shrink + jnp.sum(weights, axis=1, keepdims=True)
    out = acc_ref[at, :] * shrink + jnp.dot(
        weights.astype(bf16), values, preferred_element_type=f32
    )
    return out / total, peak * SCALE + jnp.log2(total)


def late_first_body(
    kv0_ref, kv1_ref, q2_ref, txt_ref, acc_ref, stat_ref, m2_ref, keep_ref
):
    keys, values = late_keys(kv0_ref, kv1_ref)
    out, lse = late_block(4, txt_ref[0], keys, values, acc_ref, stat_ref)
    keep_ref[0] = out
    keep_ref[1] = jnp.broadcast_to(lse, (256, 128))
    m2_ref[256:512, :] = out.astype(bf16)
    m2_ref[520:528, :] = stat_rows(lse)
    out, lse = late_block(2, q2_ref[...].reshape(256, HD), keys, values, acc_ref, stat_ref)
    m2_ref[0:256, :] = out.astype(bf16)
    m2_ref[512:520, :] = stat_rows(lse)


def late_second_body(
    kv0_ref, kv1_ref, q3_ref, q1_ref, acc_ref, stat_ref, m2_ref, m3_ref, m1_ref
):
    keys, values = late_keys(kv0_ref, kv1_ref)
    for b, q_ref, m_ref in ((3, q3_ref, m3_ref), (1, q1_ref, m1_ref)):
        out, lse = late_block(b, q_ref[...].reshape(256, HD), keys, values, acc_ref, stat_ref)
        m_ref[0:256, :] = out.astype(bf16)
        m_ref[256:512, :] = m2_ref[256:512, :]
        m_ref[512:520, :] = stat_rows(lse)
        m_ref[520:528, :] = m2_ref[520:528, :]


def late_own_body(kv0_ref, kv1_ref, recv_ref, acc_ref, stat_ref, keep_ref):
    keys, values = late_keys(kv0_ref, kv1_ref)
    q = recv_ref[:, 0:32, :].reshape(256, HD)
    out, lse = late_block(0, q, keys, values, acc_ref, stat_ref)
    keep_ref[0] = out
    keep_ref[1] = jnp.broadcast_to(lse, (256, 128))


def weights_body(w_hbm, w_out, sems):
    share = w_hbm.shape[0] // 8
    copies = [
        pltpu.make_async_copy(
            w_hbm.at[pl.ds(share * i, share)], w_out.at[pl.ds(share * i, share)], sems.at[i]
        )
        for i in range(8)
    ]
    for c in copies:
        c.start()
    for c in copies:
        c.wait()


def blend(outs, lses):
    peak = lses[0]
    for v in lses[1:]:
        peak = jnp.maximum(peak, v)
    weights = [jnp.exp2(v - peak) for v in lses]
    total = weights[0]
    for w in weights[1:]:
        total = total + w
    mixed = outs[0] * weights[0]
    for o, w in zip(outs[1:], weights[1:]):
        mixed = mixed + o * w
    return mixed / total


def mix_body(len_ref, own_ref, keep_ref, g1_ref, g2_ref, g3_ref, out_ref):
    got = (g1_ref, g2_ref, g3_ref)
    for part in range(2):
        rows = slice(256 * part, 256 * part + 256)
        kept = (own_ref, keep_ref)[part]
        outs = [kept[0]] + [g[rows, :].astype(f32) for g in got]
        lses = [kept[1, :, 0:1]]
        lses += [stat_column(g[512 + 8 * part : 520 + 8 * part, :]) for g in got]
        mixed = blend(outs, lses)
        if part == 0:
            out_ref[:, 0:32, :] = mixed.astype(bf16).reshape(8, 32, HD)
        else:
            row = lax.broadcasted_iota(jnp.int32, (256, 128), 0)
            text = jnp.where(row < len_ref[0], mixed, 0.0).astype(bf16)
            for d in range(8):
                out_ref[d, 32:288, :] = text


def tail_body(core_ref, recv_ref, w_ref, mine_ref, other_ref, txt_out, sems):
    leave = [
        pltpu.make_async_copy(
            recv_ref.at[h, pl.ds(32, 256)], txt_out.at[:, pl.ds(h * HD, HD)], sems.at[h]
        )
        for h in range(8)
    ]
    for c in leave:
        c.start()
    rows = jnp.concatenate([recv_ref[h, 0:32, :] for h in range(8)], axis=1).astype(f32)
    flipped = jnp.concatenate([rows[16:32], rows[0:16]], axis=0)
    rows = jnp.where(core_ref[0] == 0, rows, flipped).astype(bf16)
    projected = jnp.dot(rows, w_ref[...], preferred_element_type=f32)
    mine_ref[...] = projected[0:16]
    other_ref[...] = projected[16:32].astype(bf16)
    for c in leave:
        c.wait()


def shards(
    img_qkv, txt_qkv, frame_index, row_index, column_index, txt_len, residual, w_proj, proj_bias, gate
):
    tokens = img_qkv.shape[1]
    width = img_qkv.shape[3]
    d_model = w_proj.shape[1]
    j = lax.axis_index("y").astype(jnp.int32).reshape(1)
    head = lax.axis_index("zl") * 4 + lax.axis_index("x")
    core = lax.axis_index("tp").astype(jnp.int32).reshape(1)
    j, core, head, frame_index = lax.optimization_barrier((j, core, head, frame_index))
    qkv = img_qkv.reshape(tokens, 3, width).transpose(1, 0, 2)
    txt = lax.dynamic_slice_in_dim(txt_qkv[0], head * HD, HD, 2).transpose(1, 0, 2)

    send = call(
        prep_body,
        jax.ShapeDtypeStruct((8, 96, HD), bf16),
        5, hbm=(0, 1, 2, 3, 4),
        scratch=(
            pltpu.VMEM((3, tokens, width), bf16),
            pltpu.VMEM((1, tokens), jnp.int32),
            pltpu.VMEM((1, tokens), jnp.int32),
            pltpu.VMEM((1, tokens), jnp.int32),
            pltpu.VMEM((8, HD), f32),
            pltpu.SemaphoreType.DMA((5,)),
        ),
    )(qkv, frame_index, row_index, column_index, jnp.asarray(rate_table()))
    recv = lax.all_to_all(send, HEAD, 0, 0, tiled=True)
    kv = recv[:, 32:96]
    q = recv[:, 0:32]
    others = {}
    for s in (2, 3, 1):
        others[s] = lax.ppermute(kv, "zh", [(i, i ^ s) for i in range(4)])
    queries = [lax.ppermute(q, "y", [(i, i ^ s) for i in range(4)]) for s in (1, 2, 3)]

    acc, stat = call(
        early_body,
        [jax.ShapeDtypeStruct((1280, HD), f32), jax.ShapeDtypeStruct((2, 1280, 128), f32)],
        8, smem=(0, 1),
    )(j, txt_len, recv, others[2], *queries, txt)
    late = (others[3], others[1])
    message = jax.ShapeDtypeStruct((528, HD), bf16)
    kept = jax.ShapeDtypeStruct((2, 256, 128), f32)
    got = {}

    def pass_on(m, s):
        got[s] = lax.ppermute(m, "y", [(i, i ^ s) for i in range(4)])

    m2, keep = call(late_first_body, [message, kept], 6)(*late, queries[1], txt, acc, stat)
    pass_on(m2, 2)
    m3, m1 = call(late_second_body, [message] * 2, 7)(*late, queries[2], queries[0], acc, stat, m2)
    pass_on(m3, 3)
    pass_on(m1, 1)
    own = call(late_own_body, kept, 5)(*late, recv, acc, stat)
    w_near = call(
        weights_body, pltpu.VMEM(w_proj.shape, bf16), 1, hbm=(0,),
        scratch=(pltpu.SemaphoreType.DMA((8,)),),
    )(w_proj)
    back = call(mix_body, jax.ShapeDtypeStruct((8, 288, HD), bf16), 6, smem=(0,))(
        txt_len, own, keep, got[1], got[2], got[3]
    )
    home = lax.all_to_all(back, HEAD, 0, 0, tiled=True)
    half = tokens // 2
    mine, other, txt_out = call(
        tail_body,
        [
            jax.ShapeDtypeStruct((half, d_model), f32),
            jax.ShapeDtypeStruct((half, d_model), bf16),
            pltpu.HBM((256, width), bf16),
        ],
        3, smem=(0,), near=(2,), far_outs=(2,),
        scratch=(pltpu.SemaphoreType.DMA((8,)),),
    )(core, home, w_near)
    theirs = lax.ppermute(other, "tp", [(0, 1), (1, 0)])
    projected = mine + theirs.astype(f32)
    img_out = residual[0].astype(f32) + gate[None, :] * (projected + proj_bias[None, :])
    return img_out.astype(bf16)[None], txt_out[None]


def solution(mesh):
    split = Mesh(
        mesh.devices.reshape(4, 2, 4, 4, mesh.shape["tp"]), ("zh", "zl", "x", "y", "tp")
    )
    placed = (
        P(None, SEQ, None, "tp"),
        P(None, None, None, "tp"),
        P(None, SEQ),
        P(None, SEQ),
        P(None, SEQ),
        P(),
        P(None, SEQ + ("tp",), None),
        P("tp", None),
        P(),
        P(),
    )
    return jax.shard_map(
        shards,
        mesh=split,
        in_specs=placed,
        out_specs=(P(None, SEQ + ("tp",), None), P(None, None, "tp")),
        check_vma=False,
    )
```

```python
import math

import jax
import jax.numpy as jnp
import numpy as np
from jax import lax
from jax.experimental import pallas as pl
from jax.experimental.pallas import tpu as pltpu
from jax.sharding import Mesh
from jax.sharding import PartitionSpec as P


HD = 128
SEQ = ("zh", "zl", "x", "y")
HEAD = ("zl", "x")
rope_base = 256.0
neg_large = -1e30
LOG2E = 1.4426950408889634
bf16 = jnp.bfloat16
f32 = jnp.float32


def vmem_spec():
    return pl.BlockSpec(memory_space=pltpu.VMEM)


def smem_spec():
    return pl.BlockSpec(memory_space=pltpu.SMEM)


def any_spec():
    return pl.BlockSpec(memory_space=pltpu.HBM)


def call(
    body, out_shape, n_in, smem=(), hbm=(), near=(), far_outs=(), limit=40 * 1024 * 1024, scratch=(), alias=None
):
    single = not isinstance(out_shape, (tuple, list))
    outs = out_shape if not single else [out_shape]
    specs = [any_spec() if i in far_outs else vmem_spec() for i in range(len(outs))]
    kernel = pl.pallas_call(
        body,
        out_shape=out_shape,
        in_specs=[
            smem_spec() if i in smem else any_spec() if i in hbm else vmem_spec() for i in range(n_in)
        ],
        out_specs=specs[0] if single else specs,
        scratch_shapes=list(scratch),
        input_output_aliases=alias or {},
        compiler_params=pltpu.CompilerParams(vmem_limit_bytes=limit),
    )

    def run(*operands):
        held = [
            pltpu.with_memory_space_constraint(v, pltpu.HBM if i in hbm else pltpu.VMEM)
            if i in hbm or i in near
            else v
            for i, v in enumerate(operands)
        ]
        return kernel(*held)

    return run


def rate_table():
    table = np.zeros((8, HD), np.float32)
    frame_part = HD // 8
    second = (HD - frame_part) // 2
    at = 0
    for p, width in enumerate((frame_part, second, second)):
        ids = np.arange(width // 2, dtype=np.float32)
        rates = np.float32(rope_base) ** (np.float32(-2.0) * ids / np.float32(width))
        table[p, at : at + width] = np.repeat(rates.astype(np.float32), 2)
        at += width
    return table


def prep_body(
    qkv_hbm, frame_hbm, row_hbm, col_hbm, rate_hbm, out_ref,
    qkv_ref, frame_ref, row_ref, col_ref, rate_ref, sems,
):
    copies = [
        pltpu.make_async_copy(src, dst, sems.at[i])
        for i, (src, dst) in enumerate(
            (
                (frame_hbm, frame_ref), (row_hbm, row_ref), (col_hbm, col_ref),
                (rate_hbm, rate_ref), (qkv_hbm, qkv_ref),
            )
        )
    ]
    for c in copies:
        c.start()
    for c in copies[:4]:
        c.wait()
    tokens = qkv_ref.shape[1]
    sub = lax.broadcasted_iota(jnp.int32, (8, tokens), 0)
    pos = jnp.where(
        sub == 0, frame_ref[...], jnp.where(sub == 1, row_ref[...], jnp.where(sub == 2, col_ref[...], 0))
    ).astype(f32)
    angles = lax.dot_general(
        pos, rate_ref[...], (((0,), (0,)), ((), ())), precision=lax.Precision.HIGHEST,
        preferred_element_type=f32,
    )
    lane = lax.broadcasted_iota(jnp.int32, (tokens, HD), 1)
    even = (lane % 2) == 0
    cosine = jnp.cos(angles)
    sine = jnp.sin(angles)
    sine = jnp.where(even, -sine, sine)
    copies[4].wait()

    def rotate(v):
        v = v.astype(f32)
        partner = jnp.where(even, pltpu.roll(v, HD - 1, 1), pltpu.roll(v, 1, 1))
        return (v * cosine + partner * sine).astype(bf16)

    for head in range(8):
        cols = slice(head * HD, (head + 1) * HD)
        out_ref[head, 0:32, :] = rotate(qkv_ref[0, :, cols])
        out_ref[head, 32:64, :] = rotate(qkv_ref[1, :, cols])
        out_ref[head, 64:96, :] = qkv_ref[2, :, cols]


def three_parts(v):
    high = v.astype(bf16).astype(f32)
    rest = v - high
    mid = rest.astype(bf16).astype(f32)
    return high, mid, rest - mid


def live_mask(j, length):
    lane = lax.broadcasted_iota(jnp.int32, (1, 128), 1)
    index = lane + (j // 2) * 128
    return jnp.logical_and(index // 64 == j, index < length)


SCALE = LOG2E / math.sqrt(HD)


def stat_rows(lse):
    row = lax.broadcasted_iota(jnp.int32, (128, 128), 0)
    lane = lax.broadcasted_iota(jnp.int32, (128, 128), 1)
    sub = lax.broadcasted_iota(jnp.int32, (8, 128), 0)
    packed = jnp.zeros((8, 128), f32)
    for half in range(2):
        column = jnp.broadcast_to(lse[128 * half : 128 * half + 128], (128, 128))
        for p, part in enumerate(three_parts(column)):
            line = jnp.sum(jnp.where(row == lane, part, 0.0), axis=0, keepdims=True)
            packed = jnp.where(sub == 2 * p + half, line, packed)
    return packed.astype(bf16)


def stat_column(packed):
    packed = packed.astype(f32)
    row = lax.broadcasted_iota(jnp.int32, (128, 128), 0)
    lane = lax.broadcasted_iota(jnp.int32, (128, 128), 1)
    halves = []
    for half in range(2):
        line = packed[half : half + 1] + packed[2 + half : 3 + half] + packed[4 + half : 5 + half]
        halves.append(jnp.sum(jnp.where(row == lane, line, 0.0), axis=1, keepdims=True))
    return jnp.concatenate(halves, axis=0)


def early_rows(where_ref, len_ref, recv_ref, kv_ref, txt_ref, blocks, acc_ref, stat_ref):
    j = where_ref[0]
    start = pl.multiple_of((j // 2) * 128, 128)
    keys = jnp.concatenate(
        [
            recv_ref[:, 32:64, :].reshape(256, HD), kv_ref[:, 0:32, :].reshape(256, HD),
            txt_ref[1, pl.ds(start, 128), :],
        ],
        axis=0,
    )
    values = jnp.concatenate(
        [
            recv_ref[:, 64:96, :].reshape(256, HD), kv_ref[:, 32:64, :].reshape(256, HD),
            txt_ref[2, pl.ds(start, 128), :],
        ],
        axis=0,
    )
    live = live_mask(j, len_ref[0])
    for slot, q in enumerate(blocks):
        scores = lax.dot_general(q, keys, (((1,), (1,)), ((), ())), preferred_element_type=f32)
        s_txt = jnp.where(live, scores[:, 512:], neg_large)
        peak = jnp.maximum(
            jnp.max(scores[:, :512], axis=1, keepdims=True), jnp.max(s_txt, axis=1, keepdims=True)
        )
        w_img = jnp.exp2((scores[:, :512] - peak) * SCALE)
        w_txt = jnp.exp2((s_txt - peak) * SCALE)
        total = jnp.sum(w_img, axis=1, keepdims=True) + jnp.sum(w_txt, axis=1, keepdims=True)
        weights = jnp.concatenate([w_img.astype(bf16), w_txt.astype(bf16)], axis=1)
        at = slice(256 * slot, 256 * slot + 256)
        acc_ref[at, :] = jnp.dot(weights, values, preferred_element_type=f32)
        stat_ref[0, at, :] = jnp.broadcast_to(peak, (256, 128))
        stat_ref[1, at, :] = jnp.broadcast_to(total, (256, 128))


def early_near_body(where_ref, len_ref, recv_ref, kv_ref, txt_ref, acc_ref, stat_ref):
    blocks = (txt_ref[0], recv_ref[:, 0:32, :].reshape(256, HD))
    early_rows(where_ref, len_ref, recv_ref, kv_ref, txt_ref, blocks, acc_ref, stat_ref)


def early_far_body(
    where_ref, len_ref, recv_ref, kv_ref, txt_ref, q1_ref, q2_ref, q3_ref, acc_ref, stat_ref
):
    blocks = [q[...].reshape(256, HD) for q in (q1_ref, q2_ref, q3_ref)]
    early_rows(where_ref, len_ref, recv_ref, kv_ref, txt_ref, blocks, acc_ref, stat_ref)


def late_keys(kv0_ref, kv1_ref):
    both = (kv0_ref, kv1_ref)
    keys = jnp.concatenate([r[:, 0:32, :].reshape(256, HD) for r in both], axis=0)
    values = jnp.concatenate([r[:, 32:64, :].reshape(256, HD) for r in both], axis=0)
    return keys, values


def late_block(slot, q, keys, values, acc_ref, stat_ref):
    at = slice(256 * slot, 256 * slot + 256)
    scores = lax.dot_general(q, keys, (((1,), (1,)), ((), ())), preferred_element_type=f32)
    before = stat_ref[0, at, 0:1]
    peak = jnp.maximum(before, jnp.max(scores, axis=1, keepdims=True))
    shrink = jnp.exp2((before - peak) * SCALE)
    weights = jnp.exp2((scores - peak) * SCALE)
    total = stat_ref[1, at, 0:1] * shrink + jnp.sum(weights, axis=1, keepdims=True)
    out = acc_ref[at, :] * shrink + jnp.dot(
        weights.astype(bf16), values, preferred_element_type=f32
    )
    return out / total, peak * SCALE + jnp.log2(total)


def late_first_body(
    kv0_ref, kv1_ref, q2_ref, txt_ref, acc_ref, stat_ref, facc_ref, fstat_ref, m2_ref, keep_ref
):
    keys, values = late_keys(kv0_ref, kv1_ref)
    out, lse = late_block(0, txt_ref[0], keys, values, acc_ref, stat_ref)
    keep_ref[0] = out
    keep_ref[1] = jnp.broadcast_to(lse, (256, 128))
    m2_ref[256:512, :] = out.astype(bf16)
    m2_ref[520:528, :] = stat_rows(lse)
    out, lse = late_block(1, q2_ref[...].reshape(256, HD), keys, values, facc_ref, fstat_ref)
    m2_ref[0:256, :] = out.astype(bf16)
    m2_ref[512:520, :] = stat_rows(lse)


def late_second_body(
    kv0_ref, kv1_ref, q3_ref, q1_ref, acc_ref, stat_ref, m2_ref, m3_ref, m1_ref
):
    keys, values = late_keys(kv0_ref, kv1_ref)
    for slot, q_ref, m_ref in ((2, q3_ref, m3_ref), (0, q1_ref, m1_ref)):
        out, lse = late_block(slot, q_ref[...].reshape(256, HD), keys, values, acc_ref, stat_ref)
        m_ref[0:256, :] = out.astype(bf16)
        m_ref[256:512, :] = m2_ref[256:512, :]
        m_ref[512:520, :] = stat_rows(lse)
        m_ref[520:528, :] = m2_ref[520:528, :]


def late_own_body(kv0_ref, kv1_ref, recv_ref, acc_ref, stat_ref, keep_ref):
    keys, values = late_keys(kv0_ref, kv1_ref)
    q = recv_ref[:, 0:32, :].reshape(256, HD)
    out, lse = late_block(1, q, keys, values, acc_ref, stat_ref)
    keep_ref[0] = out
    keep_ref[1] = jnp.broadcast_to(lse, (256, 128))


def weights_body(w_hbm, w_out, sems):
    share = w_hbm.shape[0] // 8
    copies = [
        pltpu.make_async_copy(
            w_hbm.at[pl.ds(share * i, share)], w_out.at[pl.ds(share * i, share)], sems.at[i]
        )
        for i in range(8)
    ]
    for c in copies:
        c.start()
    for c in copies:
        c.wait()


def blend(outs, lses):
    peak = lses[0]
    for v in lses[1:]:
        peak = jnp.maximum(peak, v)
    weights = [jnp.exp2(v - peak) for v in lses]
    total = weights[0]
    for w in weights[1:]:
        total = total + w
    mixed = outs[0] * weights[0]
    for o, w in zip(outs[1:], weights[1:]):
        mixed = mixed + o * w
    return mixed / total


def mix_body(len_ref, own_ref, keep_ref, g1_ref, g2_ref, g3_ref, out_ref):
    got = (g1_ref, g2_ref, g3_ref)
    for part in range(2):
        rows = slice(256 * part, 256 * part + 256)
        kept = (own_ref, keep_ref)[part]
        outs = [kept[0]] + [g[rows, :].astype(f32) for g in got]
        lses = [kept[1, :, 0:1]]
        lses += [stat_column(g[512 + 8 * part : 520 + 8 * part, :]) for g in got]
        mixed = blend(outs, lses)
        if part == 0:
            out_ref[:, 0:32, :] = mixed.astype(bf16).reshape(8, 32, HD)
        else:
            row = lax.broadcasted_iota(jnp.int32, (256, 128), 0)
            text = jnp.where(row < len_ref[0], mixed, 0.0).astype(bf16)
            for d in range(8):
                out_ref[d, 32:288, :] = text


def tail_body(core_ref, recv_ref, w_ref, mine_ref, other_ref, txt_out, sems):
    leave = [
        pltpu.make_async_copy(
            recv_ref.at[h, pl.ds(32, 256)], txt_out.at[:, pl.ds(h * HD, HD)], sems.at[h]
        )
        for h in range(8)
    ]
    for c in leave:
        c.start()
    rows = jnp.concatenate([recv_ref[h, 0:32, :] for h in range(8)], axis=1).astype(f32)
    flipped = jnp.concatenate([rows[16:32], rows[0:16]], axis=0)
    rows = jnp.where(core_ref[0] == 0, rows, flipped).astype(bf16)
    projected = jnp.dot(rows, w_ref[...], preferred_element_type=f32)
    mine_ref[...] = projected[0:16]
    other_ref[...] = projected[16:32].astype(bf16)
    for c in leave:
        c.wait()


def shards(
    img_qkv, txt_qkv, frame_index, row_index, column_index, txt_len, residual, w_proj, proj_bias, gate
):
    tokens = img_qkv.shape[1]
    width = img_qkv.shape[3]
    d_model = w_proj.shape[1]
    j = lax.axis_index("y").astype(jnp.int32).reshape(1)
    head = lax.axis_index("zl") * 4 + lax.axis_index("x")
    core = lax.axis_index("tp").astype(jnp.int32).reshape(1)
    j, core, head, frame_index = lax.optimization_barrier((j, core, head, frame_index))
    qkv = img_qkv.reshape(tokens, 3, width).transpose(1, 0, 2)
    txt = lax.dynamic_slice_in_dim(txt_qkv[0], head * HD, HD, 2).transpose(1, 0, 2)

    send = call(
        prep_body,
        jax.ShapeDtypeStruct((8, 96, HD), bf16),
        5, hbm=(0, 1, 2, 3, 4),
        scratch=(
            pltpu.VMEM((3, tokens, width), bf16),
            pltpu.VMEM((1, tokens), jnp.int32),
            pltpu.VMEM((1, tokens), jnp.int32),
            pltpu.VMEM((1, tokens), jnp.int32),
            pltpu.VMEM((8, HD), f32),
            pltpu.SemaphoreType.DMA((5,)),
        ),
    )(qkv, frame_index, row_index, column_index, jnp.asarray(rate_table()))
    recv = lax.all_to_all(send, HEAD, 0, 0, tiled=True)
    kv = recv[:, 32:96]
    q = recv[:, 0:32]
    others = {}
    for s in (2, 3, 1):
        others[s] = lax.ppermute(kv, "zh", [(i, i ^ s) for i in range(4)])
    queries = {}
    for s in (2, 3, 1):
        queries[s] = lax.ppermute(q, "y", [(i, i ^ s) for i in range(4)])

    here = (j, txt_len, recv, others[2], txt)
    acc, stat = call(
        early_near_body,
        [jax.ShapeDtypeStruct((512, HD), f32), jax.ShapeDtypeStruct((2, 512, 128), f32)],
        5, smem=(0, 1),
    )(*here)
    far = call(
        early_far_body,
        [jax.ShapeDtypeStruct((768, HD), f32), jax.ShapeDtypeStruct((2, 768, 128), f32)],
        8, smem=(0, 1),
    )(*here, queries[1], queries[2], queries[3])
    late = (others[3], others[1])
    message = jax.ShapeDtypeStruct((528, HD), bf16)
    kept = jax.ShapeDtypeStruct((2, 256, 128), f32)
    got = {}

    def pass_on(m, s):
        got[s] = lax.ppermute(m, "y", [(i, i ^ s) for i in range(4)])

    m2, keep = call(late_first_body, [message, kept], 8)(*late, queries[2], txt, acc, stat, *far)
    pass_on(m2, 2)
    m3, m1 = call(late_second_body, [message] * 2, 7)(*late, queries[3], queries[1], *far, m2)
    pass_on(m3, 3)
    pass_on(m1, 1)
    own = call(late_own_body, kept, 5)(*late, recv, acc, stat)
    w_near = call(
        weights_body, pltpu.VMEM(w_proj.shape, bf16), 1, hbm=(0,),
        scratch=(pltpu.SemaphoreType.DMA((8,)),),
    )(w_proj)
    back = call(mix_body, jax.ShapeDtypeStruct((8, 288, HD), bf16), 6, smem=(0,))(
        txt_len, own, keep, got[1], got[2], got[3]
    )
    home = lax.all_to_all(back, HEAD, 0, 0, tiled=True)
    half = tokens // 2
    mine, other, txt_out = call(
        tail_body,
        [
            jax.ShapeDtypeStruct((half, d_model), f32),
            jax.ShapeDtypeStruct((half, d_model), bf16),
            pltpu.HBM((256, width), bf16),
        ],
        3, smem=(0,), near=(2,), far_outs=(2,),
        scratch=(pltpu.SemaphoreType.DMA((8,)),),
    )(core, home, w_near)
    theirs = lax.ppermute(other, "tp", [(0, 1), (1, 0)])
    projected = mine + theirs.astype(f32)
    img_out = residual[0].astype(f32) + gate[None, :] * (projected + proj_bias[None, :])
    return img_out.astype(bf16)[None], txt_out[None]


def solution(mesh):
    split = Mesh(
        mesh.devices.reshape(4, 2, 4, 4, mesh.shape["tp"]), ("zh", "zl", "x", "y", "tp")
    )
    placed = (
        P(None, SEQ, None, "tp"),
        P(None, None, None, "tp"),
        P(None, SEQ),
        P(None, SEQ),
        P(None, SEQ),
        P(),
        P(None, SEQ + ("tp",), None),
        P("tp", None),
        P(),
        P(),
    )
    return jax.shard_map(
        shards,
        mesh=split,
        in_specs=placed,
        out_specs=(P(None, SEQ + ("tp",), None), P(None, None, "tp")),
        check_vma=False,
    )
```

```python
import math

import jax
import jax.numpy as jnp
import numpy as np
from jax import lax
from jax.experimental import pallas as pl
from jax.experimental.pallas import tpu as pltpu
from jax.sharding import Mesh
from jax.sharding import PartitionSpec as P


HD = 128
SEQ = ("zh", "zl", "xh", "xl", "yh", "yl")
BLOCK = ("xh", "yh")
HEAD = ("zl", "xl", "yl")
rope_base = 256.0
neg_large = -1e30
LOG2E = 1.4426950408889634
bf16 = jnp.bfloat16
f32 = jnp.float32


def vmem_spec():
    return pl.BlockSpec(memory_space=pltpu.VMEM)


def smem_spec():
    return pl.BlockSpec(memory_space=pltpu.SMEM)


def any_spec():
    return pl.BlockSpec(memory_space=pltpu.HBM)


def call(
    body, out_shape, n_in, smem=(), hbm=(), near=(), far_outs=(), limit=40 * 1024 * 1024, scratch=(), alias=None
):
    single = not isinstance(out_shape, (tuple, list))
    outs = out_shape if not single else [out_shape]
    specs = [any_spec() if i in far_outs else vmem_spec() for i in range(len(outs))]
    kernel = pl.pallas_call(
        body,
        out_shape=out_shape,
        in_specs=[
            smem_spec() if i in smem else any_spec() if i in hbm else vmem_spec() for i in range(n_in)
        ],
        out_specs=specs[0] if single else specs,
        scratch_shapes=list(scratch),
        input_output_aliases=alias or {},
        compiler_params=pltpu.CompilerParams(vmem_limit_bytes=limit),
    )

    def run(*operands):
        held = [
            pltpu.with_memory_space_constraint(v, pltpu.HBM if i in hbm else pltpu.VMEM)
            if i in hbm or i in near
            else v
            for i, v in enumerate(operands)
        ]
        return kernel(*held)

    return run


def rate_table():
    table = np.zeros((8, HD), np.float32)
    frame_part = HD // 8
    second = (HD - frame_part) // 2
    at = 0
    for p, width in enumerate((frame_part, second, second)):
        ids = np.arange(width // 2, dtype=np.float32)
        rates = np.float32(rope_base) ** (np.float32(-2.0) * ids / np.float32(width))
        table[p, at : at + width] = np.repeat(rates.astype(np.float32), 2)
        at += width
    return table


def prep_body(
    qkv_hbm, frame_hbm, row_hbm, col_hbm, rate_hbm, out_ref,
    qkv_ref, frame_ref, row_ref, col_ref, rate_ref, sems,
):
    copies = [
        pltpu.make_async_copy(src, dst, sems.at[i])
        for i, (src, dst) in enumerate(
            (
                (frame_hbm, frame_ref), (row_hbm, row_ref), (col_hbm, col_ref),
                (rate_hbm, rate_ref), (qkv_hbm, qkv_ref),
            )
        )
    ]
    for c in copies:
        c.start()
    for c in copies[:4]:
        c.wait()
    tokens = qkv_ref.shape[1]
    sub = lax.broadcasted_iota(jnp.int32, (8, tokens), 0)
    pos = jnp.where(
        sub == 0, frame_ref[...], jnp.where(sub == 1, row_ref[...], jnp.where(sub == 2, col_ref[...], 0))
    ).astype(f32)
    angles = lax.dot_general(
        pos, rate_ref[...], (((0,), (0,)), ((), ())), precision=lax.Precision.HIGHEST,
        preferred_element_type=f32,
    )
    lane = lax.broadcasted_iota(jnp.int32, (tokens, HD), 1)
    even = (lane % 2) == 0
    cosine = jnp.cos(angles)
    sine = jnp.sin(angles)
    sine = jnp.where(even, -sine, sine)
    copies[4].wait()

    def rotate(v):
        v = v.astype(f32)
        partner = jnp.where(even, pltpu.roll(v, HD - 1, 1), pltpu.roll(v, 1, 1))
        return (v * cosine + partner * sine).astype(bf16)

    for head in range(8):
        cols = slice(head * HD, (head + 1) * HD)
        out_ref[head, 0:32, :] = rotate(qkv_ref[0, :, cols])
        out_ref[head, 32:64, :] = rotate(qkv_ref[1, :, cols])
        out_ref[head, 64:96, :] = qkv_ref[2, :, cols]


def three_parts(v):
    high = v.astype(bf16).astype(f32)
    rest = v - high
    mid = rest.astype(bf16).astype(f32)
    return high, mid, rest - mid


def live_mask(j, length):
    lane = lax.broadcasted_iota(jnp.int32, (1, 128), 1)
    index = lane + (j // 2) * 128
    return jnp.logical_and(index // 64 == j, index < length)


SCALE = LOG2E / math.sqrt(HD)


def stat_rows(lse):
    row = lax.broadcasted_iota(jnp.int32, (128, 128), 0)
    lane = lax.broadcasted_iota(jnp.int32, (128, 128), 1)
    sub = lax.broadcasted_iota(jnp.int32, (8, 128), 0)
    packed = jnp.zeros((8, 128), f32)
    for half in range(2):
        column = jnp.broadcast_to(lse[128 * half : 128 * half + 128], (128, 128))
        for p, part in enumerate(three_parts(column)):
            line = jnp.sum(jnp.where(row == lane, part, 0.0), axis=0, keepdims=True)
            packed = jnp.where(sub == 2 * p + half, line, packed)
    return packed.astype(bf16)


def stat_column(packed):
    packed = packed.astype(f32)
    row = lax.broadcasted_iota(jnp.int32, (128, 128), 0)
    lane = lax.broadcasted_iota(jnp.int32, (128, 128), 1)
    halves = []
    for half in range(2):
        line = packed[half : half + 1] + packed[2 + half : 3 + half] + packed[4 + half : 5 + half]
        halves.append(jnp.sum(jnp.where(row == lane, line, 0.0), axis=1, keepdims=True))
    return jnp.concatenate(halves, axis=0)


def early_rows(where_ref, len_ref, recv_ref, kv_ref, txt_ref, blocks, acc_ref, stat_ref):
    j = where_ref[0]
    start = pl.multiple_of((j // 2) * 128, 128)
    keys = jnp.concatenate(
        [
            recv_ref[:, 32:64, :].reshape(256, HD), kv_ref[:, 0:32, :].reshape(256, HD),
            txt_ref[1, pl.ds(start, 128), :],
        ],
        axis=0,
    )
    values = jnp.concatenate(
        [
            recv_ref[:, 64:96, :].reshape(256, HD), kv_ref[:, 32:64, :].reshape(256, HD),
            txt_ref[2, pl.ds(start, 128), :],
        ],
        axis=0,
    )
    live = live_mask(j, len_ref[0])
    for slot, q in enumerate(blocks):
        scores = lax.dot_general(q, keys, (((1,), (1,)), ((), ())), preferred_element_type=f32)
        s_txt = jnp.where(live, scores[:, 512:], neg_large)
        peak = jnp.maximum(
            jnp.max(scores[:, :512], axis=1, keepdims=True), jnp.max(s_txt, axis=1, keepdims=True)
        )
        w_img = jnp.exp2((scores[:, :512] - peak) * SCALE)
        w_txt = jnp.exp2((s_txt - peak) * SCALE)
        total = jnp.sum(w_img, axis=1, keepdims=True) + jnp.sum(w_txt, axis=1, keepdims=True)
        weights = jnp.concatenate([w_img.astype(bf16), w_txt.astype(bf16)], axis=1)
        at = slice(256 * slot, 256 * slot + 256)
        acc_ref[at, :] = jnp.dot(weights, values, preferred_element_type=f32)
        stat_ref[0, at, :] = jnp.broadcast_to(peak, (256, 128))
        stat_ref[1, at, :] = jnp.broadcast_to(total, (256, 128))


def early_near_body(where_ref, len_ref, recv_ref, kv_ref, txt_ref, acc_ref, stat_ref):
    blocks = (txt_ref[0], recv_ref[:, 0:32, :].reshape(256, HD))
    early_rows(where_ref, len_ref, recv_ref, kv_ref, txt_ref, blocks, acc_ref, stat_ref)


def early_far_body(
    where_ref, len_ref, recv_ref, kv_ref, txt_ref, q1_ref, q2_ref, q3_ref, acc_ref, stat_ref
):
    blocks = [q[...].reshape(256, HD) for q in (q1_ref, q2_ref, q3_ref)]
    early_rows(where_ref, len_ref, recv_ref, kv_ref, txt_ref, blocks, acc_ref, stat_ref)


def late_keys(kv0_ref, kv1_ref):
    both = (kv0_ref, kv1_ref)
    keys = jnp.concatenate([r[:, 0:32, :].reshape(256, HD) for r in both], axis=0)
    values = jnp.concatenate([r[:, 32:64, :].reshape(256, HD) for r in both], axis=0)
    return keys, values


def late_block(slot, q, keys, values, acc_ref, stat_ref):
    at = slice(256 * slot, 256 * slot + 256)
    scores = lax.dot_general(q, keys, (((1,), (1,)), ((), ())), preferred_element_type=f32)
    before = stat_ref[0, at, 0:1]
    peak = jnp.maximum(before, jnp.max(scores, axis=1, keepdims=True))
    shrink = jnp.exp2((before - peak) * SCALE)
    weights = jnp.exp2((scores - peak) * SCALE)
    total = stat_ref[1, at, 0:1] * shrink + jnp.sum(weights, axis=1, keepdims=True)
    out = acc_ref[at, :] * shrink + jnp.dot(
        weights.astype(bf16), values, preferred_element_type=f32
    )
    return out / total, peak * SCALE + jnp.log2(total)


def late_first_body(
    kv0_ref, kv1_ref, q2_ref, txt_ref, acc_ref, stat_ref, facc_ref, fstat_ref, m2_ref, keep_ref
):
    keys, values = late_keys(kv0_ref, kv1_ref)
    out, lse = late_block(0, txt_ref[0], keys, values, acc_ref, stat_ref)
    keep_ref[0] = out
    keep_ref[1] = jnp.broadcast_to(lse, (256, 128))
    m2_ref[256:512, :] = out.astype(bf16)
    m2_ref[520:528, :] = stat_rows(lse)
    out, lse = late_block(1, q2_ref[...].reshape(256, HD), keys, values, facc_ref, fstat_ref)
    m2_ref[0:256, :] = out.astype(bf16)
    m2_ref[512:520, :] = stat_rows(lse)


def late_second_body(
    kv0_ref, kv1_ref, q3_ref, q1_ref, acc_ref, stat_ref, m2_ref, m3_ref, m1_ref
):
    keys, values = late_keys(kv0_ref, kv1_ref)
    for slot, q_ref, m_ref in ((2, q3_ref, m3_ref), (0, q1_ref, m1_ref)):
        out, lse = late_block(slot, q_ref[...].reshape(256, HD), keys, values, acc_ref, stat_ref)
        m_ref[0:256, :] = out.astype(bf16)
        m_ref[256:512, :] = m2_ref[256:512, :]
        m_ref[512:520, :] = stat_rows(lse)
        m_ref[520:528, :] = m2_ref[520:528, :]


def late_own_body(kv0_ref, kv1_ref, recv_ref, acc_ref, stat_ref, keep_ref):
    keys, values = late_keys(kv0_ref, kv1_ref)
    q = recv_ref[:, 0:32, :].reshape(256, HD)
    out, lse = late_block(1, q, keys, values, acc_ref, stat_ref)
    keep_ref[0] = out
    keep_ref[1] = jnp.broadcast_to(lse, (256, 128))


def weights_body(w_hbm, w_out, sems):
    share = w_hbm.shape[0] // 8
    copies = [
        pltpu.make_async_copy(
            w_hbm.at[pl.ds(share * i, share)], w_out.at[pl.ds(share * i, share)], sems.at[i]
        )
        for i in range(8)
    ]
    for c in copies:
        c.start()
    for c in copies:
        c.wait()


def blend(outs, lses):
    peak = lses[0]
    for v in lses[1:]:
        peak = jnp.maximum(peak, v)
    weights = [jnp.exp2(v - peak) for v in lses]
    total = weights[0]
    for w in weights[1:]:
        total = total + w
    mixed = outs[0] * weights[0]
    for o, w in zip(outs[1:], weights[1:]):
        mixed = mixed + o * w
    return mixed / total


def mix_body(len_ref, own_ref, keep_ref, g1_ref, g2_ref, g3_ref, out_ref):
    got = (g1_ref, g2_ref, g3_ref)
    for part in range(2):
        rows = slice(256 * part, 256 * part + 256)
        kept = (own_ref, keep_ref)[part]
        outs = [kept[0]] + [g[rows, :].astype(f32) for g in got]
        lses = [kept[1, :, 0:1]]
        lses += [stat_column(g[512 + 8 * part : 520 + 8 * part, :]) for g in got]
        mixed = blend(outs, lses)
        if part == 0:
            out_ref[:, 0:32, :] = mixed.astype(bf16).reshape(8, 32, HD)
        else:
            row = lax.broadcasted_iota(jnp.int32, (256, 128), 0)
            text = jnp.where(row < len_ref[0], mixed, 0.0).astype(bf16)
            for d in range(8):
                out_ref[d, 32:288, :] = text


def tail_body(core_ref, recv_ref, w_ref, mine_ref, other_ref, txt_out, sems):
    leave = [
        pltpu.make_async_copy(
            recv_ref.at[h, pl.ds(32, 256)], txt_out.at[:, pl.ds(h * HD, HD)], sems.at[h]
        )
        for h in range(8)
    ]
    for c in leave:
        c.start()
    rows = jnp.concatenate([recv_ref[h, 0:32, :] for h in range(8)], axis=1).astype(f32)
    flipped = jnp.concatenate([rows[16:32], rows[0:16]], axis=0)
    rows = jnp.where(core_ref[0] == 0, rows, flipped).astype(bf16)
    projected = jnp.dot(rows, w_ref[...], preferred_element_type=f32)
    mine_ref[...] = projected[0:16]
    other_ref[...] = projected[16:32].astype(bf16)
    for c in leave:
        c.wait()


def shards(
    img_qkv, txt_qkv, frame_index, row_index, column_index, txt_len, residual, w_proj, proj_bias, gate
):
    tokens = img_qkv.shape[1]
    width = img_qkv.shape[3]
    d_model = w_proj.shape[1]
    j = lax.axis_index(BLOCK).astype(jnp.int32).reshape(1)
    head = lax.axis_index(HEAD)
    core = lax.axis_index("tp").astype(jnp.int32).reshape(1)
    j, core, head, frame_index = lax.optimization_barrier((j, core, head, frame_index))
    qkv = img_qkv.reshape(tokens, 3, width).transpose(1, 0, 2)
    txt = lax.dynamic_slice_in_dim(txt_qkv[0], head * HD, HD, 2).transpose(1, 0, 2)

    send = call(
        prep_body,
        jax.ShapeDtypeStruct((8, 96, HD), bf16),
        5, hbm=(0, 1, 2, 3, 4),
        scratch=(
            pltpu.VMEM((3, tokens, width), bf16),
            pltpu.VMEM((1, tokens), jnp.int32),
            pltpu.VMEM((1, tokens), jnp.int32),
            pltpu.VMEM((1, tokens), jnp.int32),
            pltpu.VMEM((8, HD), f32),
            pltpu.SemaphoreType.DMA((5,)),
        ),
    )(qkv, frame_index, row_index, column_index, jnp.asarray(rate_table()))
    recv = lax.all_to_all(send, HEAD, 0, 0, tiled=True)
    kv = recv[:, 32:96]
    q = recv[:, 0:32]
    others = {}
    for s in (2, 3, 1):
        others[s] = lax.ppermute(kv, "zh", [(i, i ^ s) for i in range(4)])
    queries = {}
    for s in (2, 3, 1):
        queries[s] = lax.ppermute(q, BLOCK, [(i, i ^ s) for i in range(4)])

    here = (j, txt_len, recv, others[2], txt)
    acc, stat = call(
        early_near_body,
        [jax.ShapeDtypeStruct((512, HD), f32), jax.ShapeDtypeStruct((2, 512, 128), f32)],
        5, smem=(0, 1),
    )(*here)
    far = call(
        early_far_body,
        [jax.ShapeDtypeStruct((768, HD), f32), jax.ShapeDtypeStruct((2, 768, 128), f32)],
        8, smem=(0, 1),
    )(*here, queries[1], queries[2], queries[3])
    late = (others[3], others[1])
    message = jax.ShapeDtypeStruct((528, HD), bf16)
    kept = jax.ShapeDtypeStruct((2, 256, 128), f32)
    got = {}

    def pass_on(m, s):
        got[s] = lax.ppermute(m, BLOCK, [(i, i ^ s) for i in range(4)])

    m2, keep = call(late_first_body, [message, kept], 8)(*late, queries[2], txt, acc, stat, *far)
    pass_on(m2, 2)
    m3, m1 = call(late_second_body, [message] * 2, 7)(*late, queries[3], queries[1], *far, m2)
    pass_on(m3, 3)
    pass_on(m1, 1)
    own = call(late_own_body, kept, 5)(*late, recv, acc, stat)
    w_near = call(
        weights_body, pltpu.VMEM(w_proj.shape, bf16), 1, hbm=(0,),
        scratch=(pltpu.SemaphoreType.DMA((8,)),),
    )(w_proj)
    back = call(mix_body, jax.ShapeDtypeStruct((8, 288, HD), bf16), 6, smem=(0,))(
        txt_len, own, keep, got[1], got[2], got[3]
    )
    home = lax.all_to_all(back, HEAD, 0, 0, tiled=True)
    half = tokens // 2
    mine, other, txt_out = call(
        tail_body,
        [
            jax.ShapeDtypeStruct((half, d_model), f32),
            jax.ShapeDtypeStruct((half, d_model), bf16),
            pltpu.HBM((256, width), bf16),
        ],
        3, smem=(0,), near=(2,), far_outs=(2,),
        scratch=(pltpu.SemaphoreType.DMA((8,)),),
    )(core, home, w_near)
    theirs = lax.ppermute(other, "tp", [(0, 1), (1, 0)])
    projected = mine + theirs.astype(f32)
    img_out = residual[0].astype(f32) + gate[None, :] * (projected + proj_bias[None, :])
    return img_out.astype(bf16)[None], txt_out[None]


def solution(mesh):
    split = Mesh(
        mesh.devices.reshape(4, 2, 2, 2, 2, 2, mesh.shape["tp"]), SEQ + ("tp",)
    )
    placed = (
        P(None, SEQ, None, "tp"),
        P(None, None, None, "tp"),
        P(None, SEQ),
        P(None, SEQ),
        P(None, SEQ),
        P(),
        P(None, SEQ + ("tp",), None),
        P("tp", None),
        P(),
        P(),
    )
    return jax.shard_map(
        shards,
        mesh=split,
        in_specs=placed,
        out_specs=(P(None, SEQ + ("tp",), None), P(None, None, "tp")),
        check_vma=False,
    )
```
